128 devices in a mesh: dom: 128 (over y, z, x, core).
Axes of the slice: x: 4, y: 4, z: 4, core: 2. Of those that a mesh axis runs over, the one named last changes fastest.
Arguments:
- features: bfloat16 [65536, 512], P('dom'), may hold values from -6 to 6
- weights: bfloat16 [3, 512, 512], replicated, may hold values from -0.078125 to 0.078125
- halo_send: int32 [128, 128, 4], P('dom'), may hold values from 0 to 511
- nbr_index: int32 [65536, 2, 8], P('dom'), may hold values from 0 to 1023
- tile_count: int32 [128], P('dom'), may hold values from 1 to 16, as said below
- edge_ends: int32 [2048, 2, 256], P('dom'), may hold values from 0 to 511
- neg_ids: int32 [1024], P('dom'), may hold values from 0 to 511
Outputs:
- weight_grad: float32 [3, 512, 512], replicated
- mean_loss: float32 [], replicated
- pre_grad: bfloat16 [65536, 512], P('dom')
The draws below stay inside these ranges and needn't reach their ends.
Inputs may be any that keep to these rules, and one draw needn't show every extreme that they name: `nbr_index`: an entry below 512 names a row of the node's own partition; an entry 512 + q * 4 + k names slot k of the halo from partition q. `tile_count`: partition 128 - 1 holds 16 tiles; every other partition holds at most 8. `edge_ends`: tile slots at or past a partition's tile_count hold no edges. `neg_ids`: entry j names a row of partition j // 8.
All inputs are finite; a program needn't handle non-finite values.
Results may differ from the reference program's by a relative error of at most 0.0012.
The reference program's roundings to bfloat16 on the way count: a program that leaves them out, or rounds other values in their place, can miss the bound.
Values may be sent and summed in bfloat16 or wider, within the bound.
No kernel may reach another device: no remote copies, remote signals or barrier semaphores. Data moves between devices by JAX's collectives and lax.ppermute only.
A program may use at most 64 MiB of HBM per device.

```python
import jax
import jax.numpy as jnp
from jax import lax

H = 512
RELS = 2
FAN = 8
TILE = 256
NODE_DEV = 512
HALO_PEER = 4
MAX_TILES = 16
NEG_DEV = 8
NODES = 65536
NEG = 1024
SLOTS = 1024
N_DOM = 128


def draw_tile_count(key, part):
    first = jax.random.randint(jax.random.fold_in(key, 11), (N_DOM,), 0, MAX_TILES)
    second = jax.random.randint(jax.random.fold_in(key, 12), (N_DOM,), 0, MAX_TILES)
    counts = 1 + first * second // (2 * MAX_TILES)
    return jnp.where(jnp.arange(N_DOM) == N_DOM - 1, MAX_TILES, counts).astype(jnp.int32)


def touch_ends(values, own_key, low, top_value):
    longest = values.shape.index(max(values.shape))
    spots = []
    for shift in (0, 1):
        where = [jax.random.randint(jax.random.fold_in(own_key, axis), (), 0, length) for axis, length in enumerate(values.shape)]
        where[longest] = (where[longest] + shift) % values.shape[longest]
        spots.append(tuple(where))
    return values.at[spots[0]].set(low).at[spots[1]].set(top_value)


def levels(key, dims, split, low, largest):
    def one(axis_at, blocks):
        steps = jax.random.uniform(jax.random.fold_in(jax.random.fold_in(key, 6), axis_at), (blocks,), jnp.float32, low / len(split), largest / len(split))
        return jnp.repeat(jnp.exp(steps), dims[axis_at] // blocks).reshape((-1,) + (1,) * (len(dims) - axis_at - 1))

    factor_of = one(*split[0])
    for cut in split[1:]:
        factor_of = factor_of * one(*cut)
    return factor_of


def centred(key, extent, scale, limit, split=(), kind=jnp.bfloat16):
    entries = jax.random.normal(key, extent, jnp.float32) * scale
    if len(split) > 0:
        entries = levels(key, extent, split, -0.22, 0.18) * entries
    return jnp.clip(entries, min=-limit, max=limit).astype(kind)


def setup_inputs(seed: int = 0) -> dict:
    seeds = jax.random.split(jax.random.key(seed), 8)
    return {
        "features": centred(seeds[0], (NODES, H), 1.0, 6.0, ((0, 128),)),
        "weights": centred(seeds[1], (RELS + 1, H, H), (12 * H) ** -0.5, 0.078125),
        "halo_send": touch_ends(jax.random.randint(seeds[2], (N_DOM, N_DOM, HALO_PEER), 0, NODE_DEV), jax.random.fold_in(seeds[2], 1), 0, NODE_DEV - 1).astype(jnp.int32),
        "nbr_index": touch_ends(jax.random.randint(seeds[3], (NODES, RELS, FAN), 0, SLOTS), jax.random.fold_in(seeds[3], 1), 0, SLOTS - 1).astype(jnp.int32),
        "tile_count": draw_tile_count(jax.random.fold_in(seeds[7], 71), 0),
        "edge_ends": touch_ends(jax.random.randint(seeds[5], (N_DOM * MAX_TILES, 2, TILE), 0, NODE_DEV), jax.random.fold_in(seeds[5], 1), 0, NODE_DEV - 1).astype(jnp.int32),
        "neg_ids": touch_ends(jax.random.randint(seeds[6], (NEG,), 0, NODE_DEV), jax.random.fold_in(seeds[6], 1), 0, NODE_DEV - 1).astype(jnp.int32),
    }


def neighbour_mean(lookup, neighbours):
    running_sum = jnp.zeros((neighbours.shape[0], lookup.shape[1]), jnp.float32)
    for column in range(neighbours.shape[1]):
        running_sum = running_sum + lookup[neighbours[:, column]].astype(jnp.float32)
    return (running_sum / neighbours.shape[1]).astype(jnp.bfloat16)


def score_tile(source, target, negatives):
    source_wide = source.astype(jnp.float32)
    target_wide = target.astype(jnp.float32)
    positive = jnp.sum(source_wide * target_wide, axis=1)
    negative = lax.dot_general(source, negatives, (((1,), (1,)), ((), ())), preferred_element_type=jnp.float32)
    count_neg = negatives.shape[0]
    tile_loss = jnp.sum(jnp.logaddexp(0.0, -positive)) + jnp.sum(jnp.logaddexp(0.0, negative)) / count_neg
    grad_positive = -jax.nn.sigmoid(-positive)
    grad_negative = (jax.nn.sigmoid(negative) / count_neg).astype(jnp.bfloat16)
    source_grad = grad_positive[:, None] * target_wide + jnp.dot(grad_negative, negatives, preferred_element_type=jnp.float32)
    target_grad = grad_positive[:, None] * source_wide
    negative_grad = lax.dot_general(grad_negative, source, (((0,), (0,)), ((), ())), preferred_element_type=jnp.float32)
    return tile_loss, source_grad, target_grad, negative_grad


def reference(features, weights, halo_send, nbr_index, tile_count, edge_ends, neg_ids):
    def layer_part(partition):
        own_rows = lax.dynamic_slice_in_dim(features, partition * NODE_DEV, NODE_DEV, 0)
        sender = jnp.arange(N_DOM, dtype=jnp.int32)[:, None] * NODE_DEV
        halo_index = (sender + halo_send[:, partition, :]).reshape(-1).astype(jnp.int32)
        lookup = jnp.concatenate([own_rows, features[halo_index]], 0)
        neighbours = lax.dynamic_slice_in_dim(nbr_index, partition * NODE_DEV, NODE_DEV, 0)
        preact = jnp.dot(own_rows, weights[0], preferred_element_type=jnp.float32)
        means = []
        for relation in range(RELS):
            mean_rows = neighbour_mean(lookup, neighbours[:, relation, :])
            means.append(mean_rows)
            preact = preact + jnp.dot(mean_rows, weights[relation + 1], preferred_element_type=jnp.float32)
        return preact, jnp.stack(means)

    parts = jnp.arange(N_DOM, dtype=jnp.int32)
    preact, means = lax.map(layer_part, parts)
    embedding = preact.astype(jnp.bfloat16)
    flat_rows = embedding.reshape(-1, H)
    neg_rows = (jnp.arange(NEG, dtype=jnp.int32) // NEG_DEV) * NODE_DEV + neg_ids
    negatives = flat_rows[neg_rows]

    def per_part(state_now, partition):
        loss_sum, negative_total = state_now
        own_embed = embedding[partition]
        tile_ends = lax.dynamic_slice_in_dim(edge_ends, partition * MAX_TILES, MAX_TILES, 0)

        def tile_step(tile_index, running):
            tile_loss_sum, node_grad, neg_grad = running
            pair_ends = lax.dynamic_index_in_dim(tile_ends, tile_index, 0, keepdims=False)
            tile_loss, source_grad, target_grad, negative_grad = score_tile(own_embed[pair_ends[0]], own_embed[pair_ends[1]], negatives)
            node_grad = node_grad.at[pair_ends[0]].add(source_grad).at[pair_ends[1]].add(target_grad)
            return tile_loss_sum + tile_loss, node_grad, neg_grad + negative_grad

        initial = (jnp.zeros((), jnp.float32), jnp.zeros((NODE_DEV, H), jnp.float32), negative_total)
        tile_loss_sum, node_grad, negative_total = lax.fori_loop(0, tile_count[partition], tile_step, initial)
        return (loss_sum + tile_loss_sum, negative_total), node_grad

    start_state = (jnp.zeros((), jnp.float32), jnp.zeros((NEG, H), jnp.float32))
    (loss_sum, negative_total), node_grad = lax.scan(per_part, start_state, parts)
    node_grad = node_grad.reshape(-1, H).at[neg_rows].add(negative_total).reshape(N_DOM, NODE_DEV, H)
    pre_grad = node_grad.astype(jnp.bfloat16)
    feature_parts = features.reshape(N_DOM, NODE_DEV, H)

    def grad_part(running, items):
        own_rows, mean_rows, grad_rows = items
        terms = [lax.dot_general(own_rows, grad_rows, (((0,), (0,)), ((), ())), preferred_element_type=jnp.float32)]
        for relation in range(RELS):
            terms.append(lax.dot_general(mean_rows[relation], grad_rows, (((0,), (0,)), ((), ())), preferred_element_type=jnp.float32))
        return running + jnp.stack(terms), None

    weight_sum, unused = lax.scan(grad_part, jnp.zeros((RELS + 1, H, H), jnp.float32), (feature_parts, means, pre_grad))
    edge_total = jnp.sum(tile_count).astype(jnp.float32) * TILE
    return weight_sum / edge_total, loss_sum / edge_total, pre_grad.reshape(-1, H)
```

```python
import jax
import jax.numpy as jnp
from jax import lax
from jax.experimental import pallas as pl
from jax.experimental.pallas import tpu as pltpu
from jax.sharding import Mesh
from jax.sharding import PartitionSpec as P

DOM = ("dom_0", "dom_1", "dom_2", "dom_3")
FAR = ("dom_0", "dom_1", "dom_2")
NEAR = ("dom_3",)
H = 512
RELS = 2
FAN = 8
TILE = 256
NODE_DEV = 512
NEG = 1024
NEG_DEV = 8
F32 = jnp.float32
BF16 = jnp.bfloat16
NT = (((1,), (1,)), ((), ()))
TN = (((0,), (0,)), ((), ()))


def swap(x, axes):
    return lax.all_to_all(x, axes, split_axis=0, concat_axis=0, tiled=True)


def sent_to_all(x, axes):
    return swap(jnp.broadcast_to(x, (lax.axis_size(axes), *x.shape)), axes)


def dot(a, b):
    return jnp.dot(a, b, preferred_element_type=F32)


def split_two(x):
    high = x.astype(BF16)
    return high, (x - high.astype(F32)).astype(BF16)


def vmem():
    return pl.BlockSpec(memory_space=pltpu.VMEM)


def smem():
    return pl.BlockSpec(memory_space=pltpu.SMEM)


def call(body, outs, specs, scratch=(), flops=0):
    return pl.pallas_call(
        body,
        out_shape=[jax.ShapeDtypeStruct(s, d) for s, d in outs],
        in_specs=specs,
        out_specs=[vmem() for _ in outs],
        scratch_shapes=list(scratch),
        cost_estimate=pl.CostEstimate(flops=flops, transcendentals=0, bytes_accessed=0) if flops else None,
    )


def counts_body(count_ref, features_ref, w_ref, nbr_ref, ends_ref, halo_count_ref, own_sum_ref, pre_ref, pairs_ref, sources_ref, own_count_ref, edge_ref):
    rows = 32
    lanes = lax.broadcasted_iota(jnp.int32, (rows, NODE_DEV), 1)

    def chunk(step, _):
        at = pl.ds(pl.multiple_of(step * rows, rows), rows)
        for r in range(RELS):
            index = nbr_ref[at, r * FAN : (r + 1) * FAN]
            for half in range(2):
                total = jnp.zeros((rows, NODE_DEV), F32)
                for k in range(FAN):
                    hit = lanes == (index[:, k : k + 1] - half * NODE_DEV)
                    total = total + jnp.where(hit, 1.0, 0.0)
                if half == 0:
                    own_count_ref[r, at, :] = total.astype(BF16)
                else:
                    halo_count_ref[r, at, :] = total.astype(BF16)
        return 0

    lax.fori_loop(0, NODE_DEV // rows, chunk, 0)
    own = features_ref[...]
    for r in range(RELS):
        own_sum_ref[r] = dot(own_count_ref[r], own)
    pre_ref[...] = dot(own, w_ref[0])
    pairs_ref[...] = jnp.zeros((NODE_DEV, NODE_DEV), F32)
    edge_ref[...] = jnp.zeros((NODE_DEV, TILE), F32)
    node = lax.broadcasted_iota(jnp.int32, (NODE_DEV, TILE), 0)

    def tile(t, _):
        source = jnp.where(node == ends_ref[t, 0:1, :], 1.0, 0.0)
        target = jnp.where(node == ends_ref[t, 1:2, :], 1.0, 0.0)
        edge_ref[...] += source
        source = source.astype(BF16)
        target = target.astype(BF16)
        both = jnp.concatenate([source, target], axis=1)
        other = jnp.concatenate([target, source], axis=1)
        pairs_ref[...] += lax.dot_general(both, other, NT, preferred_element_type=F32)
        return 0

    lax.fori_loop(0, count_ref[0], tile, 0)
    sources_ref[...] = jnp.broadcast_to(jnp.sum(edge_ref[...], axis=1, keepdims=True), (NODE_DEV, 128))


def layer_body(neg_ids_ref, halo_count_ref, halo_ref, own_sum_ref, pre_ref, w_ref, means_ref, embed_ref, picked_ref):
    halo = halo_ref[...]
    preact = pre_ref[...]
    for r in range(RELS):
        total = own_sum_ref[r] + dot(halo_count_ref[r], halo)
        mean = (total * (1.0 / FAN)).astype(BF16)
        means_ref[r] = mean
        preact = preact + dot(mean, w_ref[r + 1])
    embed = preact.astype(BF16)
    embed_ref[...] = embed
    row = lax.broadcasted_iota(jnp.int32, (16, NODE_DEV), 0)
    lane = lax.broadcasted_iota(jnp.int32, (16, NODE_DEV), 1)
    chosen = jnp.zeros((16, NODE_DEV), F32)
    for i in range(NEG_DEV):
        chosen = jnp.where((row == i) & (lane == neg_ids_ref[i]), 1.0, chosen)
    picked_ref[...] = dot(chosen.astype(BF16), embed)[:NEG_DEV].astype(BF16)


def soft_parts(x):
    small = jnp.exp(-jnp.abs(x))
    bottom = 1.0 / (1.0 + small)
    sigmoid = jnp.where(x >= 0, bottom, small * bottom)
    log_one = jnp.where(small < 1e-3, small * (1.0 - 0.5 * small), jnp.log(1.0 + small))
    return sigmoid, jnp.maximum(x, 0.0) + log_one


def positive_body(embed_ref, pairs_ref, features_ref, means_ref, grad_ref, loss_ref, turned_ref):
    embed = embed_ref[...]
    scores = lax.dot_general(embed, embed, NT, preferred_element_type=F32)
    sigmoid, softplus = soft_parts(-scores)
    pairs = pairs_ref[...]
    loss_ref[...] = jnp.broadcast_to(0.5 * jnp.sum(pairs * softplus, keepdims=True), (8, 128))
    high, low = split_two(-(pairs * sigmoid))
    grad_ref[...] = dot(high, embed) + dot(low, embed)
    turned_ref[0:H, :] = features_ref[...].T
    for r in range(RELS):
        turned_ref[(r + 1) * H : (r + 2) * H, :] = means_ref[r].T


def negative_body(count_ref, embed_ref, neg_ref, base_ref, sources_ref, loss_ref, grad_ref, send_ref):
    embed = embed_ref[...]
    sources = sources_ref[:, 0:1]
    loss = loss_ref[0:1, 0:1]
    grad = jnp.zeros((NODE_DEV, H), F32)
    spread_high, spread_low = split_two(embed.astype(F32) * sources)
    spread = jnp.concatenate([spread_high, spread_low], axis=1)
    for core in range(2):
        negatives = neg_ref[core]
        scores = lax.dot_general(embed, negatives, NT, preferred_element_type=F32)
        sigmoid, softplus = soft_parts(scores)
        per_source = jnp.sum(softplus, axis=1, keepdims=True)
        loss = loss + jnp.sum(per_source * sources, axis=0, keepdims=True) * (1.0 / NEG)
        weight = (sigmoid * (1.0 / NEG)).astype(BF16)
        grad = grad + dot(weight, negatives)
        parts = lax.dot_general(weight, spread, TN, preferred_element_type=F32)
        total = parts[:, :H] + parts[:, H:]
        send_ref[:, core, :, 0:H] = total.reshape(NEG // 16, NEG_DEV, H).astype(BF16)
    grad_ref[...] = base_ref[...] + sources * grad
    first = loss.astype(BF16).astype(F32)
    second = (loss - first).astype(BF16).astype(F32)
    third = (loss - first) - second
    lane = lax.broadcasted_iota(jnp.int32, (NEG_DEV, 128), 1)
    tiles = jnp.zeros((NEG_DEV, 128), F32) + count_ref[0].astype(F32)
    notes = jnp.where(lane == 0, first, jnp.where(lane == 1, second, jnp.where(lane == 2, third, tiles)))
    notes = jnp.broadcast_to(notes[None], (NEG // 16, NEG_DEV, 128)).astype(BF16)
    for core in range(2):
        send_ref[:, core, :, H:] = notes


def outer_body(neg_ids_ref, arrived_ref, grad_ref, turned_ref, pre_ref, weight_ref, note_ref, sum_ref):
    total = jnp.sum(arrived_ref[...].astype(F32), axis=0)
    note_ref[...] = total[:, H:]
    sum_ref[...] = grad_ref[...]
    for i in range(NEG_DEV):
        at = pl.ds(neg_ids_ref[i], 1)
        sum_ref[at, :] += total[i : i + 1, 0:H]
    pre = sum_ref[...].astype(BF16)
    pre_ref[...] = pre
    turned = turned_ref[...]
    for half in range(2):
        weight_ref[half] = dot(turned, pre[:, half * 256 : (half + 1) * 256])


def finish_body(whole_ref, note_ref, weight_ref, loss_ref):
    note = note_ref[0:1, :]
    loss = note[:, 0:1] + note[:, 1:2] + note[:, 2:3]
    edges = note[:, 3:4] * TILE
    loss_ref[...] = loss / edges
    for half in range(2):
        for r in range(RELS + 1):
            weight_ref[r, :, half * 256 : (half + 1) * 256] = whole_ref[half, r * H : (r + 1) * H, :] / edges


def on_device(features, weights, halo_send, nbr_index, tile_count, edge_ends, neg_ids):
    square = (NODE_DEV, H)
    outgoing = features[halo_send[0]]
    incoming = swap(outgoing, DOM)
    halo_count, own_sum, pre, pairs, sources = call(
        counts_body,
        [((RELS, NODE_DEV, 512), BF16), ((RELS, *square), F32), (square, F32), ((NODE_DEV, NODE_DEV), F32), ((NODE_DEV, 128), F32)],
        [smem(), vmem(), vmem(), vmem(), vmem()],
        [pltpu.VMEM((RELS, NODE_DEV, NODE_DEV), BF16), pltpu.VMEM((NODE_DEV, TILE), F32)],
    )(tile_count, features, weights, nbr_index.reshape(NODE_DEV, RELS * FAN), edge_ends)
    means, embed, picked = call(
        layer_body,
        [((RELS, *square), BF16), (square, BF16), ((NEG_DEV, H), BF16)],
        [smem(), vmem(), vmem(), vmem(), vmem(), vmem()],
    )(neg_ids, halo_count, incoming.reshape(512, H), own_sum, pre, weights)
    far_rows = sent_to_all(picked, FAR)
    negatives = sent_to_all(far_rows.reshape(NEG // 2, H), NEAR)
    base, loss, turned = call(
        positive_body,
        [(square, F32), ((8, 128), F32), (((RELS + 1) * H, NODE_DEV), BF16)],
        [vmem(), vmem(), vmem(), vmem()],
    )(embed, pairs, features, means)
    grad, outgoing_grad = call(
        negative_body,
        [(square, F32), ((NEG // 16, 2, NEG_DEV, H + 128), BF16)],
        [smem(), vmem(), vmem(), vmem(), vmem(), vmem()],
    )(tile_count, embed, negatives.reshape(2, NEG // 2, H), base, sources, loss)
    arrived = swap(outgoing_grad.reshape(NEG // NEG_DEV, NEG_DEV, H + 128), DOM)
    pre_grad, partial, note = call(
        outer_body,
        [(square, BF16), ((2, (RELS + 1) * H, 256), F32), ((NEG_DEV, 128), F32)],
        [smem(), vmem(), vmem(), vmem()],
        [pltpu.VMEM(square, F32)],
    )(neg_ids, arrived, grad, turned)
    paired = jnp.sum(swap(partial, NEAR), axis=0)
    mine = jnp.sum(swap(paired.reshape(64, 24, 256), FAR), axis=0)
    half = sent_to_all(mine, FAR).reshape((RELS + 1) * H, 256)
    whole = sent_to_all(half, NEAR)
    weight_grad, mean_loss = call(
        finish_body,
        [((RELS + 1, H, H), F32), ((1, 1), F32)],
        [vmem(), vmem()],
    )(whole, note)
    return weight_grad, mean_loss.reshape(()), pre_grad


def solution(mesh):
    torus = Mesh(mesh.devices.reshape(4, 4, 4, 2), DOM)
    in_specs = (
        P(DOM, None),
        P(),
        P(DOM, None, None),
        P(DOM, None, None),
        P(DOM),
        P(DOM, None, None),
        P(DOM),
    )
    out_specs = (P(), P(), P(DOM, None))
    return jax.shard_map(on_device, mesh=torus, in_specs=in_specs, out_specs=out_specs, check_vma=False)
```

```python
import jax
import jax.numpy as jnp
from jax import lax
from jax.experimental import pallas as pl
from jax.experimental.pallas import tpu as pltpu
from jax.sharding import Mesh
from jax.sharding import PartitionSpec as P

DOM = ("dom_0", "dom_1", "dom_2", "dom_3")
FAR = ("dom_0", "dom_1", "dom_2")
NEAR = ("dom_3",)
H = 512
RELS = 2
FAN = 8
TILE = 256
NODE_DEV = 512
NEG = 1024
NEG_DEV = 8
CHIPS = 64
GROUP = 4
HALF = 256
F32 = jnp.float32
BF16 = jnp.bfloat16
NT = (((1,), (1,)), ((), ()))
TN = (((0,), (0,)), ((), ()))


def swap(x, axes):
    return lax.all_to_all(x, axes, split_axis=0, concat_axis=0, tiled=True)


def core_swap(x):
    return lax.ppermute(x, "dom_3", [(0, 1), (1, 0)])


def dot(a, b):
    return jnp.dot(a, b, preferred_element_type=F32)


def split_two(x):
    high = x.astype(BF16)
    return high, (x - high.astype(F32)).astype(BF16)


def vmem():
    return pl.BlockSpec(memory_space=pltpu.VMEM)


def weight_at(k):
    return pl.BlockSpec((1, H, H), lambda i: (k, 0, 0))


def smem():
    return pl.BlockSpec(memory_space=pltpu.SMEM)


def call(body, outs, specs, scratch=(), flops=0):
    return pl.pallas_call(
        body,
        out_shape=[jax.ShapeDtypeStruct(s, d) for s, d in outs],
        grid=(1,),
        in_specs=specs,
        out_specs=[vmem() for _ in outs],
        scratch_shapes=list(scratch),
        cost_estimate=pl.CostEstimate(flops=flops, transcendentals=0, bytes_accessed=0) if flops else None,
    )


def counts_body(features_ref, w_ref, nbr_ref, halo_count_ref, own_sum_ref, pre_ref, own_count_ref):
    rows = 32
    lanes = lax.broadcasted_iota(jnp.int32, (rows, NODE_DEV), 1)

    def chunk(step, _):
        at = pl.ds(pl.multiple_of(step * rows, rows), rows)
        for r in range(RELS):
            index = nbr_ref[at, r * FAN : (r + 1) * FAN]
            for half in range(2):
                total = jnp.zeros((rows, NODE_DEV), F32)
                for k in range(FAN):
                    hit = lanes == (index[:, k : k + 1] - half * NODE_DEV)
                    total = total + jnp.where(hit, 1.0, 0.0)
                if half == 0:
                    own_count_ref[r, at, :] = total.astype(BF16)
                else:
                    halo_count_ref[r, at, :] = total.astype(BF16)
        return 0

    lax.fori_loop(0, NODE_DEV // rows, chunk, 0)
    own = features_ref[...]
    for r in range(RELS):
        own_sum_ref[r] = dot(own_count_ref[r], own)
    pre_ref[...] = dot(own, w_ref[0])


def layer_body(neg_ids_ref, halo_count_ref, halo_ref, own_sum_ref, pre_ref, first_ref, second_ref, means_ref, embed_ref, picked_ref):
    halo = halo_ref[...]
    preact = pre_ref[...]
    for r, w_ref in enumerate((first_ref, second_ref)):
        total = own_sum_ref[r] + dot(halo_count_ref[r], halo)
        mean = (total * (1.0 / FAN)).astype(BF16)
        means_ref[r] = mean
        preact = preact + dot(mean, w_ref[0])
    embed = preact.astype(BF16)
    embed_ref[...] = embed
    row = lax.broadcasted_iota(jnp.int32, (16, NODE_DEV), 0)
    lane = lax.broadcasted_iota(jnp.int32, (16, NODE_DEV), 1)
    chosen = jnp.zeros((16, NODE_DEV), F32)
    for i in range(NEG_DEV):
        chosen = jnp.where((row == i) & (lane == neg_ids_ref[i]), 1.0, chosen)
    picked = dot(chosen.astype(BF16), embed)[:NEG_DEV]
    picked_ref[...] = jnp.broadcast_to(picked[None], (CHIPS, NEG_DEV, H)).astype(BF16)


def soft_parts(x):
    small = jnp.exp(-jnp.abs(x))
    bottom = 1.0 / (1.0 + small)
    sigmoid = jnp.where(x >= 0, bottom, small * bottom)
    log_one = jnp.where(small < 1e-3, small * (1.0 - 0.5 * small), jnp.log(1.0 + small))
    return sigmoid, jnp.maximum(x, 0.0) + log_one


def positive_body(count_ref, embed_ref, ends_ref, features_ref, means_ref, grad_ref, loss_ref, turned_ref, sources_ref, spread_ref, pairs_ref):
    tiles = count_ref[0]
    pairs_ref[...] = jnp.zeros((NODE_DEV, NODE_DEV), F32)
    node = lax.broadcasted_iota(jnp.int32, (NODE_DEV, TILE), 0)

    def group(step, _):
        sources, targets = [], []
        for j in range(GROUP):
            t = step * GROUP + j
            source = jnp.where(t < tiles, ends_ref[t, 0:1, :], -1)
            sources.append(jnp.where(node == source, 1.0, 0.0).astype(BF16))
            targets.append(jnp.where(node == ends_ref[t, 1:2, :], 1.0, 0.0).astype(BF16))
        pairs_ref[...] += lax.dot_general(
            jnp.concatenate(sources, axis=1), jnp.concatenate(targets, axis=1), NT, preferred_element_type=F32
        )
        return 0

    lax.fori_loop(0, (tiles + (GROUP - 1)) // GROUP, group, 0)
    embed = embed_ref[...]
    pairs = pairs_ref[...]
    sources = jnp.sum(pairs, axis=1, keepdims=True)
    sources_ref[...] = jnp.broadcast_to(sources, (NODE_DEV, 128))
    high, low = split_two(embed.astype(F32) * sources)
    spread_ref[:, 0:H] = high
    spread_ref[:, H:] = low
    scores = lax.dot_general(embed, embed, NT, preferred_element_type=F32)
    sigmoid, softplus = soft_parts(-scores)
    loss_ref[...] = jnp.broadcast_to(jnp.sum(pairs * softplus, keepdims=True), (8, 128))
    high, low = split_two(-((pairs + pairs.T) * sigmoid))
    grad_ref[...] = dot(high, embed) + dot(low, embed)
    turned_ref[0:H, :] = features_ref[...].T
    for r in range(RELS):
        turned_ref[(r + 1) * H : (r + 2) * H, :] = means_ref[r].T


def scored(embed, rows, sources, spread):
    scores = lax.dot_general(embed, rows, NT, preferred_element_type=F32)
    sigmoid, softplus = soft_parts(scores)
    per_source = jnp.sum(softplus, axis=1, keepdims=True)
    loss = jnp.sum(per_source * sources, axis=0, keepdims=True) * (1.0 / NEG)
    weight = (sigmoid * (1.0 / NEG)).astype(BF16)
    parts = lax.dot_general(weight, spread, TN, preferred_element_type=F32)
    return weight, loss, parts[:, :H] + parts[:, H:]


def near_body(embed_ref, rows_ref, spread_ref, sources_ref, base_ref, loss_in_ref, grad_ref, part_ref, loss_ref):
    rows = rows_ref[...]
    sources = sources_ref[:, 0:1]
    weight, loss, part = scored(embed_ref[...], rows, sources, spread_ref[...])
    part_ref[...] = part
    grad_ref[...] = base_ref[...] + sources * dot(weight, rows)
    loss_ref[...] = loss_in_ref[...] + loss


def other_body(embed_ref, rows_ref, spread_ref, sources_ref, loss_in_ref, weight_ref, part_ref, loss_ref):
    weight, loss, part = scored(embed_ref[...], rows_ref[...], sources_ref[:, 0:1], spread_ref[...])
    weight_ref[...] = weight
    part_ref[...] = part.astype(BF16)
    loss_ref[...] = loss_in_ref[...] + loss


def rest_body(weight_ref, rows_ref, sources_ref, grad_in_ref, grad_ref):
    grad_ref[...] = grad_in_ref[...] + sources_ref[:, 0:1] * dot(weight_ref[...], rows_ref[...])


def merge_body(count_ref, part_ref, arrived_ref, loss_ref, send_ref):
    total = part_ref[...] + arrived_ref[...].astype(F32)
    send_ref[:, :, 0:H] = total.reshape(CHIPS, NEG_DEV, H).astype(BF16)
    loss = loss_ref[...]
    first = loss.astype(BF16).astype(F32)
    second = (loss - first).astype(BF16).astype(F32)
    third = (loss - first) - second
    lane = lax.broadcasted_iota(jnp.int32, (NEG_DEV, 128), 1)
    tiles = jnp.zeros((NEG_DEV, 128), F32) + count_ref[0].astype(F32)
    notes = jnp.where(lane == 0, first, jnp.where(lane == 1, second, jnp.where(lane == 2, third, tiles)))
    send_ref[:, :, H:] = jnp.broadcast_to(notes[None], (CHIPS, NEG_DEV, 128)).astype(BF16)


def half_of(ref, core):
    return ref[:, pl.ds(pl.multiple_of(core * HALF, HALF), HALF)]


def outer_body(neg_ids_ref, core_ref, arrived_ref, grad_ref, turned_ref, pre_ref, weight_ref, note_ref, sum_ref):
    total = jnp.sum(arrived_ref[...].astype(F32), axis=0)
    note_ref[...] = total[:, H:]
    sum_ref[...] = grad_ref[...]
    for i in range(NEG_DEV):
        at = pl.ds(neg_ids_ref[i], 1)
        sum_ref[at, :] += total[i : i + 1, 0:H]
    pre_ref[...] = sum_ref[...].astype(BF16)
    weight_ref[...] = dot(turned_ref[...], half_of(pre_ref, 1 - core_ref[0]))


def inner_body(core_ref, pre_ref, turned_ref, weight_ref):
    weight_ref[...] = dot(turned_ref[...], half_of(pre_ref, core_ref[0]))


def owned_body(arrived_ref, send_ref):
    total = jnp.sum(arrived_ref[...], axis=0)
    send_ref[...] = jnp.broadcast_to(total[None], send_ref.shape)


def first_half_body(core_ref, half_ref, own_note_ref, other_note_ref, weight_ref, loss_ref):
    note = own_note_ref[0:1, :] + other_note_ref[0:1, :]
    loss = note[:, 0:1] + note[:, 1:2] + note[:, 2:3]
    edges = note[:, 3:4] * TILE
    loss_ref[...] = loss / edges
    weight_ref[...] = half_ref[...].reshape(RELS + 1, H, HALF) / edges


def second_half_body(core_ref, half_ref, own_note_ref, other_note_ref, begun_ref, weight_ref):
    edges = (own_note_ref[0:1, 3:4] + other_note_ref[0:1, 3:4]) * TILE
    weight_ref[...] = half_ref[...].reshape(RELS + 1, H, HALF) / edges


def halves(body, which, extra, alias):
    whole = jax.ShapeDtypeStruct((RELS + 1, H, H), F32)
    block = pl.BlockSpec((RELS + 1, H, HALF), lambda i, core: (0, 0, which(core[0])))
    scalar = pl.BlockSpec((1, 1), lambda i, core: (0, 0))
    full = pl.BlockSpec(((RELS + 1) * H, HALF), lambda i, core: (0, 0))
    note = pl.BlockSpec((8, 128), lambda i, core: (0, 0))
    return pl.pallas_call(
        body,
        out_shape=[whole, jax.ShapeDtypeStruct((1, 1), F32)][: 1 + extra],
        grid_spec=pltpu.PrefetchScalarGridSpec(
            num_scalar_prefetch=1,
            grid=(1,),
            in_specs=[full, note, note] + [pl.BlockSpec(memory_space=pl.ANY)] * len(alias),
            out_specs=[block, scalar][: 1 + extra],
        ),
        input_output_aliases=alias,
    )


def on_device(features, weights, halo_send, nbr_index, tile_count, edge_ends, neg_ids):
    square = (NODE_DEV, H)
    core = lax.axis_index(NEAR).astype(jnp.int32).reshape(1)
    outgoing = features[halo_send[0]]
    incoming = swap(outgoing, DOM)
    halo_count, own_sum, pre = call(
        counts_body,
        [((RELS, NODE_DEV, 512), BF16), ((RELS, *square), F32), (square, F32)],
        [vmem(), weight_at(0), vmem()],
        [pltpu.VMEM((RELS, NODE_DEV, NODE_DEV), BF16)],
    )(features, weights, nbr_index.reshape(NODE_DEV, RELS * FAN))
    means, embed, picked = call(
        layer_body,
        [((RELS, *square), BF16), (square, BF16), ((CHIPS, NEG_DEV, H), BF16)],
        [smem(), vmem(), vmem(), vmem(), vmem(), weight_at(1), weight_at(2)],
    )(neg_ids, halo_count, incoming.reshape(512, H), own_sum, pre, weights, weights)
    near_rows = swap(picked, FAR).reshape(square)
    other_rows = core_swap(near_rows)
    base, loss, turned, sources, spread = call(
        positive_body,
        [(square, F32), ((8, 128), F32), (((RELS + 1) * H, NODE_DEV), BF16), ((NODE_DEV, 128), F32), ((NODE_DEV, 2 * H), BF16)],
        [smem(), vmem(), vmem(), vmem(), vmem()],
        [pltpu.VMEM((NODE_DEV, NODE_DEV), F32)],
    )(tile_count, embed, edge_ends, features, means)
    grad, near_part, loss = call(
        near_body,
        [(square, F32), (square, F32), ((8, 128), F32)],
        [vmem()] * 6,
    )(embed, near_rows, spread, sources, base, loss)
    weight, other_part, loss = call(
        other_body,
        [(square, BF16), (square, BF16), ((8, 128), F32)],
        [vmem()] * 5,
    )(embed, other_rows, spread, sources, loss)
    (grad,) = call(rest_body, [(square, F32)], [vmem()] * 4)(weight, other_rows, sources, grad)
    (outgoing_grad,) = call(
        merge_body,
        [((CHIPS, NEG_DEV, H + 128), BF16)],
        [smem(), vmem(), vmem(), vmem()],
    )(tile_count, near_part, core_swap(other_part), loss)
    arrived = swap(outgoing_grad, FAR)
    pre_grad, partial_other, note = call(
        outer_body,
        [(square, BF16), (((RELS + 1) * H, HALF), F32), ((NEG_DEV, 128), F32)],
        [smem(), smem(), vmem(), vmem(), vmem()],
        [pltpu.VMEM(square, F32)],
    )(neg_ids, core, arrived, grad, turned)
    other_note = core_swap(note)
    partial_arrived = core_swap(partial_other)
    (partial_own,) = call(inner_body, [(((RELS + 1) * H, HALF), F32)], [smem(), vmem(), vmem()])(core, pre_grad, turned)
    paired = (partial_own + partial_arrived).reshape(CHIPS, 24, HALF)
    (mine,) = call(owned_body, [((CHIPS, 24, HALF), F32)], [vmem()])(swap(paired, FAR))
    half = swap(mine, FAR).reshape((RELS + 1) * H, HALF)
    other_half = core_swap(half)
    begun, mean_loss = halves(first_half_body, lambda c: c, 1, {})(core, half, note, other_note)
    (weight_grad,) = halves(second_half_body, lambda c: 1 - c, 0, {4: 0})(core, other_half, note, other_note, begun)
    return weight_grad, mean_loss.reshape(()), pre_grad


def solution(mesh):
    torus = Mesh(mesh.devices.reshape(4, 4, 4, 2), DOM)
    in_specs = (
        P(DOM, None),
        P(),
        P(DOM, None, None),
        P(DOM, None, None),
        P(DOM),
        P(DOM, None, None),
        P(DOM),
    )
    out_specs = (P(), P(), P(DOM, None))
    return jax.shard_map(on_device, mesh=torus, in_specs=in_specs, out_specs=out_specs, check_vma=False)
```

```python
import jax
import jax.numpy as jnp
from jax import lax
from jax.experimental import pallas as pl
from jax.experimental.pallas import tpu as pltpu
from jax.sharding import Mesh
from jax.sharding import PartitionSpec as P

DOM = ("dom_0", "dom_1", "dom_2", "dom_3")
FAR = ("dom_0", "dom_1", "dom_2")
NEAR = ("dom_3",)
H = 512
RELS = 2
FAN = 8
TILE = 256
NODE_DEV = 512
NEG = 1024
NEG_DEV = 8
CHIPS = 64
GROUP = 4
HALF = 256
F32 = jnp.float32
BF16 = jnp.bfloat16
NT = (((1,), (1,)), ((), ()))
TN = (((0,), (0,)), ((), ()))


def swap(x, axes):
    return lax.all_to_all(x, axes, split_axis=0, concat_axis=0, tiled=True)


def core_swap(x):
    return lax.ppermute(x, "dom_3", [(0, 1), (1, 0)])


def dot(a, b):
    return jnp.dot(a, b, preferred_element_type=F32)


def split_two(x):
    high = x.astype(BF16)
    return high, (x - high.astype(F32)).astype(BF16)


def vmem():
    return pl.BlockSpec(memory_space=pltpu.VMEM)


def plain(*shape):
    return pl.BlockSpec(shape, lambda i: (0,) * len(shape))


def weight_at(k):
    return pl.BlockSpec((1, H, H), lambda i: (k, 0, 0))


def smem():
    return pl.BlockSpec(memory_space=pltpu.SMEM)


def near_memory(x):
    return pltpu.with_memory_space_constraint(x, pltpu.VMEM)


def call(body, outs, specs, scratch=(), args=()):
    specs = list(specs)
    given = []
    for spec, x in zip(specs, args):
        held = spec.memory_space == pltpu.VMEM and x.dtype != jnp.int32
        given.append(near_memory(x) if held else x)
    return pl.pallas_call(
        body,
        out_shape=[o if isinstance(o, jax.ShapeDtypeStruct) else pltpu.VMEM(*o) for o in outs],
        grid=(1,),
        in_specs=specs,
        out_specs=[vmem() for _ in outs],
        scratch_shapes=list(scratch),
        compiler_params=pltpu.CompilerParams(vmem_limit_bytes=28 << 20),
    )(*given)


def counts_body(features_ref, w_ref, nbr_ref, halo_count_ref, own_sum_ref, pre_ref, own_count_ref):
    rows = 32
    lanes = lax.broadcasted_iota(jnp.int32, (rows, NODE_DEV), 1)

    def chunk(step, _):
        at = pl.ds(pl.multiple_of(step * rows, rows), rows)
        for r in range(RELS):
            index = nbr_ref[at, r * FAN : (r + 1) * FAN]
            for half in range(2):
                total = jnp.zeros((rows, NODE_DEV), F32)
                for k in range(FAN):
                    hit = lanes == (index[:, k : k + 1] - half * NODE_DEV)
                    total = total + jnp.where(hit, 1.0, 0.0)
                if half == 0:
                    own_count_ref[r, at, :] = total.astype(BF16)
                else:
                    halo_count_ref[r, at, :] = total.astype(BF16)
        return 0

    lax.fori_loop(0, NODE_DEV // rows, chunk, 0)
    own = features_ref[...]
    for r in range(RELS):
        own_sum_ref[r] = dot(own_count_ref[r], own)
    pre_ref[...] = dot(own, w_ref[0])


def layer_body(neg_ids_ref, halo_count_ref, halo_ref, own_sum_ref, pre_ref, first_ref, second_ref, means_ref, embed_ref, picked_ref):
    halo = halo_ref[...]
    preact = pre_ref[...]
    for r, w_ref in enumerate((first_ref, second_ref)):
        total = own_sum_ref[r] + dot(halo_count_ref[r], halo)
        mean = (total * (1.0 / FAN)).astype(BF16)
        means_ref[r] = mean
        preact = preact + dot(mean, w_ref[0])
    embed = preact.astype(BF16)
    embed_ref[...] = embed
    row = lax.broadcasted_iota(jnp.int32, (16, NODE_DEV), 0)
    lane = lax.broadcasted_iota(jnp.int32, (16, NODE_DEV), 1)
    chosen = jnp.zeros((16, NODE_DEV), F32)
    for i in range(NEG_DEV):
        chosen = jnp.where((row == i) & (lane == neg_ids_ref[i]), 1.0, chosen)
    picked = dot(chosen.astype(BF16), embed)[:NEG_DEV]
    picked_ref[...] = jnp.broadcast_to(picked[None], (CHIPS, NEG_DEV, H)).astype(BF16)


def soft_parts(x):
    small = jnp.exp(-jnp.abs(x))
    bottom = 1.0 / (1.0 + small)
    sigmoid = jnp.where(x >= 0, bottom, small * bottom)
    log_one = jnp.where(small < 1e-3, small * (1.0 - 0.5 * small), jnp.log(1.0 + small))
    return sigmoid, jnp.maximum(x, 0.0) + log_one


def positive_body(count_ref, embed_ref, ends_ref, features_ref, means_ref, grad_ref, loss_ref, turned_ref, sources_ref, spread_ref, pairs_ref):
    tiles = count_ref[0]
    pairs_ref[...] = jnp.zeros((NODE_DEV, NODE_DEV), F32)
    node = lax.broadcasted_iota(jnp.int32, (NODE_DEV, TILE), 0)

    def group(step, _):
        sources, targets = [], []
        for j in range(GROUP):
            t = step * GROUP + j
            source = jnp.where(t < tiles, ends_ref[t, 0:1, :], -1)
            sources.append(jnp.where(node == source, 1.0, 0.0).astype(BF16))
            targets.append(jnp.where(node == ends_ref[t, 1:2, :], 1.0, 0.0).astype(BF16))
        pairs_ref[...] += lax.dot_general(
            jnp.concatenate(sources, axis=1), jnp.concatenate(targets, axis=1), NT, preferred_element_type=F32
        )
        return 0

    lax.fori_loop(0, (tiles + (GROUP - 1)) // GROUP, group, 0)
    embed = embed_ref[...]
    pairs = pairs_ref[...]
    sources = jnp.sum(pairs, axis=1, keepdims=True)
    sources_ref[...] = jnp.broadcast_to(sources, (NODE_DEV, 128))
    high, low = split_two(embed.astype(F32) * sources)
    spread_ref[:, 0:H] = high
    spread_ref[:, H:] = low
    scores = lax.dot_general(embed, embed, NT, preferred_element_type=F32)
    sigmoid, softplus = soft_parts(-scores)
    loss_ref[...] = jnp.broadcast_to(jnp.sum(pairs * softplus, keepdims=True), (8, 128))
    high, low = split_two(-((pairs + pairs.T) * sigmoid))
    grad_ref[...] = dot(high, embed) + dot(low, embed)
    turned_ref[0:H, :] = features_ref[...].T
    for r in range(RELS):
        turned_ref[(r + 1) * H : (r + 2) * H, :] = means_ref[r].T


def scored(embed, rows, sources, spread):
    scores = lax.dot_general(embed, rows, NT, preferred_element_type=F32)
    sigmoid, softplus = soft_parts(scores)
    per_source = jnp.sum(softplus, axis=1, keepdims=True)
    loss = jnp.sum(per_source * sources, axis=0, keepdims=True) * (1.0 / NEG)
    weight = (sigmoid * (1.0 / NEG)).astype(BF16)
    parts = lax.dot_general(weight, spread, TN, preferred_element_type=F32)
    return weight, loss, parts[:, :H] + parts[:, H:]


def near_body(embed_ref, rows_ref, spread_ref, sources_ref, base_ref, loss_in_ref, grad_ref, part_ref, loss_ref):
    rows = rows_ref[...]
    sources = sources_ref[:, 0:1]
    weight, loss, part = scored(embed_ref[...], rows, sources, spread_ref[...])
    part_ref[...] = part
    grad_ref[...] = base_ref[...] + sources * dot(weight, rows)
    loss_ref[...] = loss_in_ref[...] + loss


def other_body(embed_ref, rows_ref, spread_ref, sources_ref, loss_in_ref, weight_ref, part_ref, loss_ref):
    weight, loss, part = scored(embed_ref[...], rows_ref[...], sources_ref[:, 0:1], spread_ref[...])
    weight_ref[...] = weight
    part_ref[...] = part.astype(BF16)
    loss_ref[...] = loss_in_ref[...] + loss


def rest_body(weight_ref, rows_ref, sources_ref, grad_in_ref, grad_ref):
    grad_ref[...] = grad_in_ref[...] + sources_ref[:, 0:1] * dot(weight_ref[...], rows_ref[...])


def merge_body(count_ref, part_ref, arrived_ref, loss_ref, send_ref):
    total = part_ref[...] + arrived_ref[...].astype(F32)
    send_ref[:, :, 0:H] = total.reshape(CHIPS, NEG_DEV, H).astype(BF16)
    loss = loss_ref[...]
    first = loss.astype(BF16).astype(F32)
    second = (loss - first).astype(BF16).astype(F32)
    third = (loss - first) - second
    lane = lax.broadcasted_iota(jnp.int32, (NEG_DEV, 128), 1)
    tiles = jnp.zeros((NEG_DEV, 128), F32) + count_ref[0].astype(F32)
    notes = jnp.where(lane == 0, first, jnp.where(lane == 1, second, jnp.where(lane == 2, third, tiles)))
    send_ref[:, :, H:] = jnp.broadcast_to(notes[None], (CHIPS, NEG_DEV, 128)).astype(BF16)


def half_of(ref, core):
    return ref[:, pl.ds(pl.multiple_of(core * HALF, HALF), HALF)]


def outer_body(neg_ids_ref, core_ref, arrived_ref, grad_ref, turned_ref, pre_out_ref, pre_ref, weight_ref, note_ref, sum_ref):
    total = jnp.sum(arrived_ref[...].astype(F32), axis=0)
    note_ref[...] = total[:, H:]
    sum_ref[...] = grad_ref[...]
    for i in range(NEG_DEV):
        at = pl.ds(neg_ids_ref[i], 1)
        sum_ref[at, :] += total[i : i + 1, 0:H]
    pre_ref[...] = sum_ref[...].astype(BF16)
    pre_out_ref[...] = pre_ref[...]
    weight_ref[...] = dot(turned_ref[...], half_of(pre_ref, 1 - core_ref[0]))


def inner_body(core_ref, pre_ref, turned_ref, weight_ref):
    weight_ref[...] = dot(turned_ref[...], half_of(pre_ref, core_ref[0]))


def owned_body(arrived_ref, send_ref):
    total = jnp.sum(arrived_ref[...], axis=0)
    send_ref[...] = jnp.broadcast_to(total[None], send_ref.shape)


def first_half_body(core_ref, half_ref, own_note_ref, other_note_ref, weight_ref, loss_ref):
    note = own_note_ref[0:1, :] + other_note_ref[0:1, :]
    loss = note[:, 0:1] + note[:, 1:2] + note[:, 2:3]
    edges = note[:, 3:4] * TILE
    loss_ref[...] = loss / edges
    weight_ref[...] = half_ref[...].reshape(RELS + 1, H, HALF) / edges


def second_half_body(core_ref, half_ref, own_note_ref, other_note_ref, begun_ref, weight_ref):
    edges = (own_note_ref[0:1, 3:4] + other_note_ref[0:1, 3:4]) * TILE
    weight_ref[...] = half_ref[...].reshape(RELS + 1, H, HALF) / edges


def halves(body, which, extra, alias):
    whole = jax.ShapeDtypeStruct((RELS + 1, H, H), F32)
    block = pl.BlockSpec((RELS + 1, H, HALF), lambda i, core: (0, 0, which(core[0])))
    scalar = pl.BlockSpec((1, 1), lambda i, core: (0, 0))
    full = vmem()
    note = pl.BlockSpec((8, 128), lambda i, core: (0, 0))
    return pl.pallas_call(
        body,
        out_shape=[whole, jax.ShapeDtypeStruct((1, 1), F32)][: 1 + extra],
        grid_spec=pltpu.PrefetchScalarGridSpec(
            num_scalar_prefetch=1,
            grid=(1,),
            in_specs=[full, note, note] + [pl.BlockSpec(memory_space=pl.ANY)] * len(alias),
            out_specs=[block, scalar][: 1 + extra],
        ),
        input_output_aliases=alias,
    )


def on_device(features, weights, halo_send, nbr_index, tile_count, edge_ends, neg_ids):
    square = (NODE_DEV, H)
    tall = ((RELS + 1) * H, HALF)
    core = lax.axis_index(NEAR).astype(jnp.int32).reshape(1)
    outgoing = features[halo_send[0]]
    incoming = swap(outgoing, DOM)
    neighbours = nbr_index.reshape(NODE_DEV, RELS * FAN)
    halo_count, own_sum, pre = call(
        counts_body,
        [((RELS, NODE_DEV, 512), BF16), ((RELS, *square), F32), (square, F32)],
        [plain(NODE_DEV, H), weight_at(0), vmem()],
        [pltpu.VMEM((RELS, NODE_DEV, NODE_DEV), BF16)],
        (features, weights, neighbours),
    )
    means, embed, picked = call(
        layer_body,
        [((RELS, *square), BF16), (square, BF16), ((CHIPS, NEG_DEV, H), BF16)],
        [smem(), vmem(), vmem(), vmem(), vmem(), weight_at(1), weight_at(2)],
        (),
        (neg_ids, halo_count, incoming.reshape(512, H), own_sum, pre, weights, weights),
    )
    near_rows = swap(picked, FAR).reshape(square)
    base, loss, turned, sources, spread = call(
        positive_body,
        [(square, F32), ((8, 128), F32), (((RELS + 1) * H, NODE_DEV), BF16), ((NODE_DEV, 128), F32), ((NODE_DEV, 2 * H), BF16)],
        [smem(), vmem(), vmem(), plain(NODE_DEV, H), vmem()],
        [pltpu.VMEM((NODE_DEV, NODE_DEV), F32)],
        (tile_count, embed, edge_ends, features, means),
    )
    near_rows, loss = lax.optimization_barrier((near_rows, loss))
    other_rows = core_swap(near_rows)
    grad, near_part, loss = call(
        near_body,
        [(square, F32), (square, F32), ((8, 128), F32)],
        [vmem()] * 6,
        (),
        (embed, near_rows, spread, sources, base, loss),
    )
    weight, other_part, loss = call(
        other_body,
        [(square, BF16), (square, BF16), ((8, 128), F32)],
        [vmem()] * 5,
        (),
        (embed, other_rows, spread, sources, loss),
    )
    (grad,) = call(rest_body, [(square, F32)], [vmem()] * 4, (), (weight, other_rows, sources, grad))
    (outgoing_grad,) = call(
        merge_body,
        [((CHIPS, NEG_DEV, H + 128), BF16)],
        [smem(), vmem(), vmem(), vmem()],
        (),
        (tile_count, near_part, core_swap(other_part), loss),
    )
    arrived = swap(outgoing_grad, FAR)
    pre_out, pre_grad, partial_other, note = call(
        outer_body,
        [jax.ShapeDtypeStruct(square, BF16), (square, BF16), (tall, F32), ((NEG_DEV, 128), F32)],
        [smem(), smem(), vmem(), vmem(), vmem()],
        [pltpu.VMEM(square, F32)],
        (neg_ids, core, arrived, grad, turned),
    )
    other_note = core_swap(note)
    partial_arrived = core_swap(partial_other)
    (partial_own,) = call(inner_body, [(tall, F32)], [smem(), vmem(), vmem()], (), (core, pre_grad, turned))
    paired = (partial_own + partial_arrived).reshape(CHIPS, 24, HALF)
    (mine,) = call(owned_body, [((CHIPS, 24, HALF), F32)], [vmem()], (), (swap(paired, FAR),))
    half = swap(mine, FAR).reshape(tall)
    other_half = core_swap(half)
    begun, mean_loss = halves(first_half_body, lambda c: c, 1, {})(core, near_memory(half), note, other_note)
    (weight_grad,) = halves(second_half_body, lambda c: 1 - c, 0, {4: 0})(core, near_memory(other_half), note, other_note, begun)
    return weight_grad, mean_loss.reshape(()), pre_out


def solution(mesh):
    torus = Mesh(mesh.devices.reshape(4, 4, 4, 2), DOM)
    in_specs = (
        P(DOM, None),
        P(),
        P(DOM, None, None),
        P(DOM, None, None),
        P(DOM),
        P(DOM, None, None),
        P(DOM),
    )
    out_specs = (P(), P(), P(DOM, None))
    return jax.shard_map(on_device, mesh=torus, in_specs=in_specs, out_specs=out_specs, check_vma=False)
```

```python
import jax
import jax.numpy as jnp
from jax import lax
from jax.experimental import pallas as pl
from jax.experimental.pallas import tpu as pltpu
from jax.sharding import Mesh
from jax.sharding import PartitionSpec as P

DOM = ("dom_0", "dom_1", "dom_2", "dom_3")
FAR = ("dom_0", "dom_1", "dom_2")
NEAR = ("dom_3",)
H = 512
RELS = 2
FAN = 8
TILE = 256
NODE_DEV = 512
NEG = 1024
NEG_DEV = 8
CHIPS = 64
GROUP = 4
HALF = 256
F32 = jnp.float32
BF16 = jnp.bfloat16
NT = (((1,), (1,)), ((), ()))
TN = (((0,), (0,)), ((), ()))
FROM_HBM = "hbm"


def swap(x, axes):
    return lax.all_to_all(x, axes, split_axis=0, concat_axis=0, tiled=True)


def core_swap(x):
    return lax.ppermute(x, "dom_3", [(0, 1), (1, 0)])


def dot(a, b):
    return jnp.dot(a, b, preferred_element_type=F32)


def split_two(x):
    high = x.astype(BF16)
    return high, (x - high.astype(F32)).astype(BF16)


def vmem():
    return pl.BlockSpec(memory_space=pltpu.VMEM)


def whole(shape):
    return pl.BlockSpec(shape, lambda i: (0,) * len(shape))


def weight_at(k):
    return pl.BlockSpec((1, H, H), lambda i: (k, 0, 0))


def smem():
    return pl.BlockSpec(memory_space=pltpu.SMEM)


def near_memory(x):
    return pltpu.with_memory_space_constraint(x, pltpu.VMEM)


def hbm(shape, kind):
    return pltpu.HBM(shape, kind)


def call(body, outs, specs, scratch=(), args=()):
    given = []
    for spec, x in zip(specs, args):
        if spec is FROM_HBM:
            x = pltpu.with_memory_space_constraint(x, pltpu.HBM)
        elif spec.memory_space == pltpu.VMEM and x.dtype != jnp.int32:
            x = near_memory(x)
        given.append(x)
    return pl.pallas_call(
        body,
        out_shape=[pltpu.VMEM(*o) if isinstance(o, tuple) else o for o in outs],
        grid=(1,),
        in_specs=[whole(x.shape) if spec is FROM_HBM else spec for spec, x in zip(specs, args)],
        out_specs=[vmem() if isinstance(o, tuple) else whole(o.shape) for o in outs],
        scratch_shapes=list(scratch),
        compiler_params=pltpu.CompilerParams(vmem_limit_bytes=28 << 20),
    )(*given)


def counts_body(features_ref, w_ref, nbr_ref, halo_count_ref, own_sum_ref, pre_ref, own_count_ref):
    rows = 32
    lanes = lax.broadcasted_iota(jnp.int32, (rows, NODE_DEV), 1)

    def chunk(step, _):
        at = pl.ds(pl.multiple_of(step * rows, rows), rows)
        for r in range(RELS):
            index = nbr_ref[at, r * FAN : (r + 1) * FAN]
            for half in range(2):
                total = jnp.zeros((rows, NODE_DEV), F32)
                for k in range(FAN):
                    hit = lanes == (index[:, k : k + 1] - half * NODE_DEV)
                    total = total + jnp.where(hit, 1.0, 0.0)
                if half == 0:
                    own_count_ref[r, at, :] = total.astype(BF16)
                else:
                    halo_count_ref[r, at, :] = total.astype(BF16)
        return 0

    lax.fori_loop(0, NODE_DEV // rows, chunk, 0)
    own = features_ref[...]
    for r in range(RELS):
        own_sum_ref[r] = dot(own_count_ref[r], own)
    pre_ref[...] = dot(own, w_ref[0])


def layer_body(neg_ids_ref, halo_count_ref, halo_ref, own_sum_ref, pre_ref, first_ref, second_ref, means_ref, embed_ref, picked_ref):
    halo = halo_ref[...]
    preact = pre_ref[...]
    for r, w_ref in enumerate((first_ref, second_ref)):
        total = own_sum_ref[r] + dot(halo_count_ref[r], halo)
        mean = (total * (1.0 / FAN)).astype(BF16)
        means_ref[r] = mean
        preact = preact + dot(mean, w_ref[0])
    embed = preact.astype(BF16)
    embed_ref[...] = embed
    row = lax.broadcasted_iota(jnp.int32, (16, NODE_DEV), 0)
    lane = lax.broadcasted_iota(jnp.int32, (16, NODE_DEV), 1)
    chosen = jnp.zeros((16, NODE_DEV), F32)
    for i in range(NEG_DEV):
        chosen = jnp.where((row == i) & (lane == neg_ids_ref[i]), 1.0, chosen)
    picked = dot(chosen.astype(BF16), embed)[:NEG_DEV]
    picked_ref[...] = jnp.broadcast_to(picked[None], (CHIPS, NEG_DEV, H)).astype(BF16)


def soft_parts(x):
    small = jnp.exp(-jnp.abs(x))
    bottom = 1.0 / (1.0 + small)
    sigmoid = jnp.where(x >= 0, bottom, small * bottom)
    log_one = jnp.where(small < 1e-3, small * (1.0 - 0.5 * small), jnp.log(1.0 + small))
    return sigmoid, jnp.maximum(x, 0.0) + log_one


def positive_body(count_ref, embed_ref, ends_ref, features_ref, means_ref, grad_ref, loss_ref, turned_ref, sources_ref, spread_ref, pairs_ref):
    tiles = count_ref[0]
    pairs_ref[...] = jnp.zeros((NODE_DEV, NODE_DEV), F32)
    node = lax.broadcasted_iota(jnp.int32, (NODE_DEV, TILE), 0)

    def group(step, _):
        sources, targets = [], []
        for j in range(GROUP):
            t = step * GROUP + j
            source = jnp.where(t < tiles, ends_ref[t, 0:1, :], -1)
            sources.append(jnp.where(node == source, 1.0, 0.0).astype(BF16))
            targets.append(jnp.where(node == ends_ref[t, 1:2, :], 1.0, 0.0).astype(BF16))
        pairs_ref[...] += lax.dot_general(
            jnp.concatenate(sources, axis=1), jnp.concatenate(targets, axis=1), NT, preferred_element_type=F32
        )
        return 0

    lax.fori_loop(0, (tiles + (GROUP - 1)) // GROUP, group, 0)
    embed = embed_ref[...]
    pairs = pairs_ref[...]
    sources = jnp.sum(pairs, axis=1, keepdims=True)
    sources_ref[...] = jnp.broadcast_to(sources, (NODE_DEV, 128))
    high, low = split_two(embed.astype(F32) * sources)
    spread_ref[:, 0:H] = high
    spread_ref[:, H:] = low
    scores = lax.dot_general(embed, embed, NT, preferred_element_type=F32)
    sigmoid, softplus = soft_parts(-scores)
    loss_ref[...] = jnp.broadcast_to(jnp.sum(pairs * softplus, keepdims=True), (8, 128))
    high, low = split_two(-((pairs + pairs.T) * sigmoid))
    grad_ref[...] = dot(high, embed) + dot(low, embed)
    turned_ref[0:H, :] = features_ref[...].T
    for r in range(RELS):
        turned_ref[(r + 1) * H : (r + 2) * H, :] = means_ref[r].T


def scored(embed, rows, sources, spread):
    scores = lax.dot_general(embed, rows, NT, preferred_element_type=F32)
    sigmoid, softplus = soft_parts(scores)
    per_source = jnp.sum(softplus, axis=1, keepdims=True)
    loss = jnp.sum(per_source * sources, axis=0, keepdims=True) * (1.0 / NEG)
    weight = (sigmoid * (1.0 / NEG)).astype(BF16)
    parts = lax.dot_general(weight, spread, TN, preferred_element_type=F32)
    return weight, loss, parts[:, :H] + parts[:, H:]


def near_body(embed_ref, rows_ref, spread_ref, sources_ref, loss_in_ref, weight_ref, part_ref, loss_ref):
    weight, loss, part = scored(embed_ref[...], rows_ref[...], sources_ref[:, 0:1], spread_ref[...])
    weight_ref[...] = weight
    part_ref[...] = part.astype(part_ref.dtype)
    loss_ref[...] = loss_in_ref[...] + loss


def rest_body(near_weight_ref, near_rows_ref, weight_ref, rows_ref, sources_ref, base_ref, grad_ref):
    total = dot(near_weight_ref[...], near_rows_ref[...]) + dot(weight_ref[...], rows_ref[...])
    grad_ref[...] = base_ref[...] + sources_ref[:, 0:1] * total


def merge_body(count_ref, part_ref, arrived_ref, loss_ref, send_ref):
    total = part_ref[...] + arrived_ref[...].astype(F32)
    send_ref[:, :, 0:H] = total.reshape(CHIPS, NEG_DEV, H).astype(BF16)
    loss = loss_ref[...]
    first = loss.astype(BF16).astype(F32)
    second = (loss - first).astype(BF16).astype(F32)
    third = (loss - first) - second
    lane = lax.broadcasted_iota(jnp.int32, (NEG_DEV, 128), 1)
    tiles = jnp.zeros((NEG_DEV, 128), F32) + count_ref[0].astype(F32)
    notes = jnp.where(lane == 0, first, jnp.where(lane == 1, second, jnp.where(lane == 2, third, tiles)))
    send_ref[:, :, H:] = jnp.broadcast_to(notes[None], (CHIPS, NEG_DEV, 128)).astype(BF16)


def half_of(ref, core):
    return ref[:, pl.ds(pl.multiple_of(core * HALF, HALF), HALF)]


def outer_body(neg_ids_ref, core_ref, arrived_ref, grad_ref, turned_ref, pre_out_ref, pre_ref, weight_ref, note_ref, sum_ref):
    total = jnp.sum(arrived_ref[...].astype(F32), axis=0)
    note_ref[...] = total[:, H:]
    sum_ref[...] = grad_ref[...]
    for i in range(NEG_DEV):
        at = pl.ds(neg_ids_ref[i], 1)
        sum_ref[at, :] += total[i : i + 1, 0:H]
    pre_ref[...] = sum_ref[...].astype(BF16)
    pre_out_ref[...] = pre_ref[...]
    weight_ref[...] = dot(turned_ref[...], half_of(pre_ref, 1 - core_ref[0]))


def inner_body(core_ref, pre_ref, turned_ref, weight_ref):
    weight_ref[...] = dot(turned_ref[...], half_of(pre_ref, core_ref[0]))


def owned_body(arrived_ref, send_ref):
    total = jnp.sum(arrived_ref[...], axis=0)
    send_ref[...] = jnp.broadcast_to(total[None], send_ref.shape)


def first_half_body(core_ref, half_ref, own_note_ref, other_note_ref, weight_ref, loss_ref):
    note = own_note_ref[0:1, :] + other_note_ref[0:1, :]
    loss = note[:, 0:1] + note[:, 1:2] + note[:, 2:3]
    edges = note[:, 3:4] * TILE
    loss_ref[...] = loss / edges
    weight_ref[...] = half_ref[...].reshape(RELS + 1, H, HALF) / edges


def second_half_body(core_ref, half_ref, own_note_ref, other_note_ref, begun_ref, weight_ref):
    edges = (own_note_ref[0:1, 3:4] + other_note_ref[0:1, 3:4]) * TILE
    weight_ref[...] = half_ref[...].reshape(RELS + 1, H, HALF) / edges


def halves(body, which, extra, alias):
    whole = jax.ShapeDtypeStruct((RELS + 1, H, H), F32)
    block = pl.BlockSpec((RELS + 1, H, HALF), lambda i, core: (0, 0, which(core[0])))
    scalar = pl.BlockSpec((1, 1), lambda i, core: (0, 0))
    full = vmem()
    note = vmem()
    return pl.pallas_call(
        body,
        out_shape=[whole, jax.ShapeDtypeStruct((1, 1), F32)][: 1 + extra],
        grid_spec=pltpu.PrefetchScalarGridSpec(
            num_scalar_prefetch=1,
            grid=(1,),
            in_specs=[full, note, note] + [pl.BlockSpec(memory_space=pl.ANY)] * len(alias),
            out_specs=[block, scalar][: 1 + extra],
        ),
        input_output_aliases=alias,
        compiler_params=pltpu.CompilerParams(vmem_limit_bytes=28 << 20),
    )


def on_device(features, weights, halo_send, nbr_index, tile_count, edge_ends, neg_ids):
    square = (NODE_DEV, H)
    tall = ((RELS + 1) * H, HALF)
    core = lax.axis_index(NEAR).astype(jnp.int32).reshape(1)
    outgoing = features[halo_send[0]]
    incoming = swap(outgoing, DOM)
    neighbours = nbr_index.reshape(NODE_DEV, RELS * FAN)
    halo_count, own_sum, pre = call(
        counts_body,
        [hbm((RELS, NODE_DEV, 512), BF16), hbm((RELS, *square), F32), hbm(square, F32)],
        [FROM_HBM, weight_at(0), vmem()],
        [pltpu.VMEM((RELS, NODE_DEV, NODE_DEV), BF16)],
        (features, weights, neighbours),
    )
    means, embed, picked = call(
        layer_body,
        [hbm((RELS, *square), BF16), (square, BF16), hbm((CHIPS, NEG_DEV, H), BF16)],
        [smem(), FROM_HBM, vmem(), FROM_HBM, FROM_HBM, weight_at(1), weight_at(2)],
        (),
        (neg_ids, halo_count, incoming.reshape(512, H), own_sum, pre, weights, weights),
    )
    near_rows = swap(picked, FAR).reshape(square)
    base, loss, turned, sources, spread = call(
        positive_body,
        [hbm(square, F32), ((8, 128), F32), hbm(((RELS + 1) * H, NODE_DEV), BF16), ((NODE_DEV, 128), F32), ((NODE_DEV, 2 * H), BF16)],
        [smem(), vmem(), vmem(), FROM_HBM, FROM_HBM],
        [pltpu.VMEM((NODE_DEV, NODE_DEV), F32)],
        (tile_count, embed, edge_ends, features, means),
    )
    near_rows, loss = lax.optimization_barrier((near_rows, loss))
    other_rows = core_swap(near_rows)
    near_weight, near_part, loss = call(
        near_body,
        [(square, BF16), (square, F32), ((8, 128), F32)],
        [vmem()] * 5,
        (),
        (embed, near_rows, spread, sources, loss),
    )
    weight, other_part, loss = call(
        near_body,
        [(square, BF16), (square, BF16), ((8, 128), F32)],
        [vmem()] * 5,
        (),
        (embed, other_rows, spread, sources, loss),
    )
    part_arrived = core_swap(other_part)
    (grad,) = call(
        rest_body,
        [(square, F32)],
        [vmem()] * 5 + [FROM_HBM],
        (),
        (near_weight, near_rows, weight, other_rows, sources, base),
    )
    part_arrived, grad = lax.optimization_barrier((part_arrived, grad))
    (outgoing_grad,) = call(
        merge_body,
        [hbm((CHIPS, NEG_DEV, H + 128), BF16)],
        [smem(), vmem(), vmem(), vmem()],
        (),
        (tile_count, near_part, part_arrived, loss),
    )
    arrived = swap(outgoing_grad, FAR)
    pre_out, pre_grad, partial_other, note = call(
        outer_body,
        [hbm(square, BF16), (square, BF16), (tall, F32), ((NEG_DEV, 128), F32)],
        [smem(), smem(), vmem(), vmem(), FROM_HBM],
        [pltpu.VMEM(square, F32)],
        (neg_ids, core, arrived, grad, turned),
    )
    other_note = core_swap(note)
    partial_arrived = core_swap(partial_other)
    (partial_own,) = call(inner_body, [(tall, F32)], [smem(), vmem(), FROM_HBM], (), (core, pre_grad, turned))
    partial_arrived, other_note = lax.optimization_barrier((partial_arrived, other_note))
    paired = (partial_own + partial_arrived).reshape(CHIPS, 24, HALF)
    (mine,) = call(owned_body, [((CHIPS, 24, HALF), F32)], [vmem()], (), (swap(paired, FAR),))
    half = swap(mine, FAR).reshape(tall)
    other_half = core_swap(half)
    notes = near_memory(note), near_memory(other_note)
    begun, mean_loss = halves(first_half_body, lambda c: c, 1, {})(core, near_memory(half), *notes)
    (begun, other_half) = lax.optimization_barrier((begun, other_half))
    (weight_grad,) = halves(second_half_body, lambda c: 1 - c, 0, {4: 0})(core, near_memory(other_half), *notes, begun)
    return weight_grad, mean_loss.reshape(()), pre_out


def solution(mesh):
    torus = Mesh(mesh.devices.reshape(4, 4, 4, 2), DOM)
    in_specs = (
        P(DOM, None),
        P(),
        P(DOM, None, None),
        P(DOM, None, None),
        P(DOM),
        P(DOM, None, None),
        P(DOM),
    )
    out_specs = (P(), P(), P(DOM, None))
    return jax.shard_map(on_device, mesh=torus, in_specs=in_specs, out_specs=out_specs, check_vma=False)
```

```python
import jax
import jax.numpy as jnp
from jax import lax
from jax.experimental import pallas as pl
from jax.experimental.pallas import tpu as pltpu
from jax.sharding import Mesh
from jax.sharding import PartitionSpec as P

DOM = ("dom_0", "dom_1", "dom_2", "dom_3")
FAR = ("dom_0", "dom_1", "dom_2")
NEAR = ("dom_3",)
H = 512
RELS = 2
FAN = 8
TILE = 256
NODE_DEV = 512
NEG = 1024
NEG_DEV = 8
CHIPS = 64
GROUP = 4
HALF = 256
F32 = jnp.float32
BF16 = jnp.bfloat16
F16 = jnp.float16
SPAN = 60000.0
TINY = 1e-30
NT = (((1,), (1,)), ((), ()))
TN = (((0,), (0,)), ((), ()))
FROM_HBM = "hbm"


def swap(x, axes):
    return lax.all_to_all(x, axes, split_axis=0, concat_axis=0, tiled=True)


def core_swap(x):
    return lax.ppermute(x, "dom_3", [(0, 1), (1, 0)])


def dot(a, b):
    return jnp.dot(a, b, preferred_element_type=F32)


def split_two(x):
    high = x.astype(BF16)
    return high, (x - high.astype(F32)).astype(BF16)


def vmem():
    return pl.BlockSpec(memory_space=pltpu.VMEM)


def whole(shape):
    return pl.BlockSpec(shape, lambda i: (0,) * len(shape))


def weight_at(k):
    return pl.BlockSpec((1, H, H), lambda i: (k, 0, 0))


def smem():
    return pl.BlockSpec(memory_space=pltpu.SMEM)


def near_memory(x):
    return pltpu.with_memory_space_constraint(x, pltpu.VMEM)


def hbm(shape, kind):
    return pltpu.HBM(shape, kind)


def call(body, outs, specs, scratch=(), args=()):
    given = []
    for spec, x in zip(specs, args):
        if spec is FROM_HBM:
            x = pltpu.with_memory_space_constraint(x, pltpu.HBM)
        elif spec.memory_space == pltpu.VMEM and x.dtype != jnp.int32:
            x = near_memory(x)
        given.append(x)
    return pl.pallas_call(
        body,
        out_shape=[pltpu.VMEM(*o) if isinstance(o, tuple) else o for o in outs],
        grid=(1,),
        in_specs=[whole(x.shape) if spec is FROM_HBM else spec for spec, x in zip(specs, args)],
        out_specs=[vmem() if isinstance(o, tuple) else whole(o.shape) for o in outs],
        scratch_shapes=list(scratch),
        compiler_params=pltpu.CompilerParams(vmem_limit_bytes=28 << 20),
    )(*given)


def counts_body(features_ref, w_ref, nbr_ref, halo_count_ref, own_sum_ref, pre_ref, own_count_ref):
    rows = 32
    lanes = lax.broadcasted_iota(jnp.int32, (rows, NODE_DEV), 1)

    def chunk(step, _):
        at = pl.ds(pl.multiple_of(step * rows, rows), rows)
        for r in range(RELS):
            index = nbr_ref[at, r * FAN : (r + 1) * FAN]
            for half in range(2):
                total = jnp.zeros((rows, NODE_DEV), F32)
                for k in range(FAN):
                    hit = lanes == (index[:, k : k + 1] - half * NODE_DEV)
                    total = total + jnp.where(hit, 1.0, 0.0)
                if half == 0:
                    own_count_ref[r, at, :] = total.astype(BF16)
                else:
                    halo_count_ref[r, at, :] = total.astype(BF16)
        return 0

    lax.fori_loop(0, NODE_DEV // rows, chunk, 0)
    own = features_ref[...]
    for r in range(RELS):
        own_sum_ref[r] = dot(own_count_ref[r], own)
    pre_ref[...] = dot(own, w_ref[0])


def layer_body(neg_ids_ref, halo_count_ref, halo_ref, own_sum_ref, pre_ref, first_ref, second_ref, means_ref, embed_ref, picked_ref):
    halo = halo_ref[...]
    preact = pre_ref[...]
    for r, w_ref in enumerate((first_ref, second_ref)):
        total = own_sum_ref[r] + dot(halo_count_ref[r], halo)
        mean = (total * (1.0 / FAN)).astype(BF16)
        means_ref[r] = mean
        preact = preact + dot(mean, w_ref[0])
    embed = preact.astype(BF16)
    embed_ref[...] = embed
    row = lax.broadcasted_iota(jnp.int32, (16, NODE_DEV), 0)
    lane = lax.broadcasted_iota(jnp.int32, (16, NODE_DEV), 1)
    chosen = jnp.zeros((16, NODE_DEV), F32)
    for i in range(NEG_DEV):
        chosen = jnp.where((row == i) & (lane == neg_ids_ref[i]), 1.0, chosen)
    picked = dot(chosen.astype(BF16), embed)[:NEG_DEV]
    picked_ref[...] = jnp.broadcast_to(picked[None], (CHIPS, NEG_DEV, H)).astype(BF16)


def soft_parts(x):
    small = jnp.exp(-jnp.abs(x))
    bottom = 1.0 / (1.0 + small)
    sigmoid = jnp.where(x >= 0, bottom, small * bottom)
    log_one = jnp.where(small < 1e-3, small * (1.0 - 0.5 * small), jnp.log(1.0 + small))
    return sigmoid, jnp.maximum(x, 0.0) + log_one


def largest(x):
    return jnp.max(jnp.max(jnp.abs(x), axis=0, keepdims=True), axis=1, keepdims=True)


def positive_body(count_ref, embed_ref, ends_ref, features_ref, means_ref, grad_ref, loss_ref, turned_ref, sources_ref, spread_ref, pairs_ref):
    tiles = count_ref[0]
    pairs_ref[...] = jnp.zeros((NODE_DEV, NODE_DEV), F32)
    node = lax.broadcasted_iota(jnp.int32, (NODE_DEV, TILE), 0)

    def group(step, _):
        sources, targets = [], []
        for j in range(GROUP):
            t = step * GROUP + j
            source = jnp.where(t < tiles, ends_ref[t, 0:1, :], -1)
            sources.append(jnp.where(node == source, 1.0, 0.0).astype(BF16))
            targets.append(jnp.where(node == ends_ref[t, 1:2, :], 1.0, 0.0).astype(BF16))
        pairs_ref[...] += lax.dot_general(
            jnp.concatenate(sources, axis=1), jnp.concatenate(targets, axis=1), NT, preferred_element_type=F32
        )
        return 0

    lax.fori_loop(0, (tiles + (GROUP - 1)) // GROUP, group, 0)
    embed = embed_ref[...]
    pairs = pairs_ref[...]
    sources = jnp.sum(pairs, axis=1, keepdims=True)
    sources_ref[...] = jnp.broadcast_to(sources, (NODE_DEV, 128))
    high, low = split_two(embed.astype(F32) * sources)
    spread_ref[:, 0:H] = high
    spread_ref[:, H:] = low
    scores = lax.dot_general(embed, embed, NT, preferred_element_type=F32)
    sigmoid, softplus = soft_parts(-scores)
    loss = jnp.sum(jnp.sum(pairs * softplus, axis=0, keepdims=True), axis=1, keepdims=True)
    widest = largest(features_ref[...].astype(F32))
    for r in range(RELS):
        widest = jnp.maximum(widest, largest(means_ref[r].astype(F32)))
    lane = lax.broadcasted_iota(jnp.int32, (8, 128), 1)
    loss_ref[...] = jnp.where(lane == 0, loss, widest)
    high, low = split_two(-((pairs + pairs.T) * sigmoid))
    grad_ref[...] = dot(high, embed) + dot(low, embed)
    turned_ref[0:H, :] = features_ref[...].T
    for r in range(RELS):
        turned_ref[(r + 1) * H : (r + 2) * H, :] = means_ref[r].T


def scored(embed, rows, sources, spread):
    scores = lax.dot_general(embed, rows, NT, preferred_element_type=F32)
    sigmoid, softplus = soft_parts(scores)
    per_source = jnp.sum(softplus, axis=1, keepdims=True)
    loss = jnp.sum(per_source * sources, axis=0, keepdims=True) * (1.0 / NEG)
    weight = (sigmoid * (1.0 / NEG)).astype(BF16)
    parts = lax.dot_general(weight, spread, TN, preferred_element_type=F32)
    return weight, loss, parts[:, :H] + parts[:, H:]


def near_body(embed_ref, rows_ref, spread_ref, sources_ref, loss_in_ref, weight_ref, part_ref, loss_ref):
    weight, loss, part = scored(embed_ref[...], rows_ref[...], sources_ref[:, 0:1], spread_ref[...])
    weight_ref[...] = weight
    part_ref[...] = part.astype(part_ref.dtype)
    lane = lax.broadcasted_iota(jnp.int32, (8, 128), 1)
    loss_ref[...] = loss_in_ref[...] + jnp.where(lane == 0, loss, 0.0)


def rest_body(near_weight_ref, near_rows_ref, weight_ref, rows_ref, sources_ref, base_ref, grad_ref):
    total = dot(near_weight_ref[...], near_rows_ref[...]) + dot(weight_ref[...], rows_ref[...])
    grad_ref[...] = base_ref[...] + sources_ref[:, 0:1] * total


def merge_body(count_ref, part_ref, arrived_ref, loss_ref, grad_ref, send_ref):
    total = part_ref[...] + arrived_ref[...].astype(F32)
    send_ref[:, :, 0:H] = total.reshape(CHIPS, NEG_DEV, H).astype(BF16)
    loss = loss_ref[0:1, 0:1]
    widest = loss_ref[0:1, 1:2]
    first = loss.astype(BF16).astype(F32)
    second = (loss - first).astype(BF16).astype(F32)
    third = (loss - first) - second
    lane = lax.broadcasted_iota(jnp.int32, (NEG_DEV, 128), 1)
    notes = jnp.zeros((NEG_DEV, 128), F32) + count_ref[0].astype(F32)
    said = (first, second, third, None, widest * largest(grad_ref[...]) * NODE_DEV, widest * NEG_DEV, largest(total))
    for place, value in enumerate(said):
        if value is not None:
            notes = jnp.where(lane == place, value, notes)
    send_ref[:, :, H:] = jnp.broadcast_to(notes[None], (CHIPS, NEG_DEV, 128)).astype(BF16)


def half_of(ref, core):
    return ref[:, pl.ds(pl.multiple_of(core * HALF, HALF), HALF)]


def outer_body(neg_ids_ref, core_ref, arrived_ref, grad_ref, turned_ref, pre_out_ref, pre_ref, weight_ref, note_ref, sum_ref):
    total = jnp.sum(arrived_ref[...].astype(F32), axis=0)
    note_ref[...] = total[:, H:]
    sum_ref[...] = grad_ref[...]
    for i in range(NEG_DEV):
        at = pl.ds(neg_ids_ref[i], 1)
        sum_ref[at, :] += total[i : i + 1, 0:H]
    pre_ref[...] = sum_ref[...].astype(BF16)
    pre_out_ref[...] = pre_ref[...]
    weight_ref[...] = dot(turned_ref[...], half_of(pre_ref, 1 - core_ref[0]))


def inner_body(core_ref, pre_ref, turned_ref, weight_ref):
    weight_ref[...] = dot(turned_ref[...], half_of(pre_ref, core_ref[0]))


def bound_of(note):
    return note[0:1, 4:5] + note[0:1, 5:6] * note[0:1, 6:7]


def scale_of(own_note, other_note):
    return SPAN / (bound_of(own_note) + bound_of(other_note) + TINY)


def factor_of(own_note_ref, other_note_ref):
    edges = (own_note_ref[0:1, 3:4] + other_note_ref[0:1, 3:4]) * TILE
    return 1.0 / scale_of(own_note_ref[...], other_note_ref[...]) / edges


def first_half_body(core_ref, half_ref, own_note_ref, other_note_ref, weight_ref, loss_ref):
    note = own_note_ref[0:1, :] + other_note_ref[0:1, :]
    loss = note[:, 0:1] + note[:, 1:2] + note[:, 2:3]
    loss_ref[...] = loss / (note[:, 3:4] * TILE)
    half = half_ref[...] * factor_of(own_note_ref, other_note_ref)
    weight_ref[...] = half.reshape(RELS + 1, H, HALF)


def second_half_body(core_ref, half_ref, own_note_ref, other_note_ref, begun_ref, weight_ref):
    half = half_ref[...] * factor_of(own_note_ref, other_note_ref)
    weight_ref[...] = half.reshape(RELS + 1, H, HALF)


def halves(body, which, extra, alias):
    whole = jax.ShapeDtypeStruct((RELS + 1, H, H), F32)
    block = pl.BlockSpec((RELS + 1, H, HALF), lambda i, core: (0, 0, which(core[0])))
    scalar = pl.BlockSpec((1, 1), lambda i, core: (0, 0))
    full = vmem()
    note = vmem()
    return pl.pallas_call(
        body,
        out_shape=[whole, jax.ShapeDtypeStruct((1, 1), F32)][: 1 + extra],
        grid_spec=pltpu.PrefetchScalarGridSpec(
            num_scalar_prefetch=1,
            grid=(1,),
            in_specs=[full, note, note] + [pl.BlockSpec(memory_space=pl.ANY)] * len(alias),
            out_specs=[block, scalar][: 1 + extra],
        ),
        input_output_aliases=alias,
        compiler_params=pltpu.CompilerParams(vmem_limit_bytes=28 << 20),
    )


def on_device(features, weights, halo_send, nbr_index, tile_count, edge_ends, neg_ids):
    square = (NODE_DEV, H)
    tall = ((RELS + 1) * H, HALF)
    core = lax.axis_index(NEAR).astype(jnp.int32).reshape(1)
    outgoing = features[halo_send[0]]
    incoming = swap(outgoing, DOM)
    neighbours = nbr_index.reshape(NODE_DEV, RELS * FAN)
    halo_count, own_sum, pre = call(
        counts_body,
        [hbm((RELS, NODE_DEV, 512), BF16), hbm((RELS, *square), F32), hbm(square, F32)],
        [FROM_HBM, weight_at(0), vmem()],
        [pltpu.VMEM((RELS, NODE_DEV, NODE_DEV), BF16)],
        (features, weights, neighbours),
    )
    means, embed, picked = call(
        layer_body,
        [hbm((RELS, *square), BF16), (square, BF16), hbm((CHIPS, NEG_DEV, H), BF16)],
        [smem(), FROM_HBM, vmem(), FROM_HBM, FROM_HBM, weight_at(1), weight_at(2)],
        (),
        (neg_ids, halo_count, incoming.reshape(512, H), own_sum, pre, weights, weights),
    )
    near_rows = swap(picked, FAR).reshape(square)
    base, loss, turned, sources, spread = call(
        positive_body,
        [hbm(square, F32), ((8, 128), F32), hbm(((RELS + 1) * H, NODE_DEV), BF16), ((NODE_DEV, 128), F32), ((NODE_DEV, 2 * H), BF16)],
        [smem(), vmem(), vmem(), FROM_HBM, FROM_HBM],
        [pltpu.VMEM((NODE_DEV, NODE_DEV), F32)],
        (tile_count, embed, edge_ends, features, means),
    )
    near_rows, loss = lax.optimization_barrier((near_rows, loss))
    other_rows = core_swap(near_rows)
    near_weight, near_part, loss = call(
        near_body,
        [(square, BF16), (square, F32), ((8, 128), F32)],
        [vmem()] * 5,
        (),
        (embed, near_rows, spread, sources, loss),
    )
    weight, other_part, loss = call(
        near_body,
        [(square, BF16), (square, BF16), ((8, 128), F32)],
        [vmem()] * 5,
        (),
        (embed, other_rows, spread, sources, loss),
    )
    part_arrived = core_swap(other_part)
    (grad,) = call(
        rest_body,
        [(square, F32)],
        [vmem()] * 5 + [FROM_HBM],
        (),
        (near_weight, near_rows, weight, other_rows, sources, base),
    )
    part_arrived, grad = lax.optimization_barrier((part_arrived, grad))
    (outgoing_grad,) = call(
        merge_body,
        [hbm((CHIPS, NEG_DEV, H + 128), BF16)],
        [smem(), vmem(), vmem(), vmem(), vmem()],
        (),
        (tile_count, near_part, part_arrived, loss, grad),
    )
    arrived = swap(outgoing_grad, FAR)
    pre_out, pre_grad, partial_other, note = call(
        outer_body,
        [hbm(square, BF16), (square, BF16), (tall, F32), ((NEG_DEV, 128), F32)],
        [smem(), smem(), vmem(), vmem(), FROM_HBM],
        [pltpu.VMEM(square, F32)],
        (neg_ids, core, arrived, grad, turned),
    )
    other_note = core_swap(note)
    partial_arrived = core_swap(partial_other)
    (partial_own,) = call(inner_body, [(tall, F32)], [smem(), vmem(), FROM_HBM], (), (core, pre_grad, turned))
    chunks = (CHIPS, 24, HALF)
    paired = ((partial_own + partial_arrived) * scale_of(note, other_note)).reshape(chunks)
    mine = jnp.sum(swap(paired.astype(F16), FAR).astype(F32), axis=0).astype(F16)
    half = swap(jnp.broadcast_to(mine, chunks), FAR).reshape(tall)
    other_half = core_swap(half).astype(F32)
    half = half.astype(F32)
    notes = near_memory(note), near_memory(other_note)
    begun, mean_loss = halves(first_half_body, lambda c: c, 1, {})(core, near_memory(half), *notes)
    (begun, other_half) = lax.optimization_barrier((begun, other_half))
    (weight_grad,) = halves(second_half_body, lambda c: 1 - c, 0, {4: 0})(core, near_memory(other_half), *notes, begun)
    return weight_grad, mean_loss.reshape(()), pre_out


def solution(mesh):
    torus = Mesh(mesh.devices.reshape(4, 4, 4, 2), DOM)
    in_specs = (
        P(DOM, None),
        P(),
        P(DOM, None, None),
        P(DOM, None, None),
        P(DOM),
        P(DOM, None, None),
        P(DOM),
    )
    out_specs = (P(), P(), P(DOM, None))
    return jax.shard_map(on_device, mesh=torus, in_specs=in_specs, out_specs=out_specs, check_vma=False)
```

```python
import jax
import jax.numpy as jnp
from jax import lax
from jax.experimental import pallas as pl
from jax.experimental.pallas import tpu as pltpu
from jax.sharding import Mesh
from jax.sharding import PartitionSpec as P

DOM = ("dom_0", "dom_1", "dom_2", "dom_3")
FAR = ("dom_0", "dom_1", "dom_2")
NEAR = ("dom_3",)
H = 512
RELS = 2
FAN = 8
TILE = 256
NODE_DEV = 512
NEG = 1024
NEG_DEV = 8
N_DOM = 128
HALO_PEER = 4
CHIPS = 64
GROUP = 4
HALF = 256
F32 = jnp.float32
BF16 = jnp.bfloat16
F16 = jnp.float16
SPAN = 60000.0
TINY = 1e-30
NT = (((1,), (1,)), ((), ()))
TN = (((0,), (0,)), ((), ()))
FROM_HBM = "hbm"


def swap(x, axes):
    return lax.all_to_all(x, axes, split_axis=0, concat_axis=0, tiled=True)


def core_swap(x):
    return lax.ppermute(x, "dom_3", [(0, 1), (1, 0)])


def dot(a, b):
    return jnp.dot(a, b, preferred_element_type=F32)


def split_two(x):
    high = x.astype(BF16)
    return high, (x - high.astype(F32)).astype(BF16)


def vmem():
    return pl.BlockSpec(memory_space=pltpu.VMEM)


def whole(shape):
    return pl.BlockSpec(shape, lambda i: (0,) * len(shape))


def weight_at(k):
    return pl.BlockSpec((1, H, H), lambda i: (k, 0, 0))


def smem():
    return pl.BlockSpec(memory_space=pltpu.SMEM)


def near_memory(x):
    return pltpu.with_memory_space_constraint(x, pltpu.VMEM)


def hbm(shape, kind):
    return pltpu.HBM(shape, kind)


def call(body, outs, specs, scratch=(), args=()):
    given = []
    for spec, x in zip(specs, args):
        if spec is FROM_HBM:
            x = pltpu.with_memory_space_constraint(x, pltpu.HBM)
        elif spec.memory_space == pltpu.VMEM and x.dtype != jnp.int32:
            x = near_memory(x)
        given.append(x)
    return pl.pallas_call(
        body,
        out_shape=[pltpu.VMEM(*o) if isinstance(o, tuple) else o for o in outs],
        grid=(1,),
        in_specs=[whole(x.shape) if spec is FROM_HBM else spec for spec, x in zip(specs, args)],
        out_specs=[vmem() if isinstance(o, tuple) else whole(o.shape) for o in outs],
        scratch_shapes=list(scratch),
        compiler_params=pltpu.CompilerParams(vmem_limit_bytes=28 << 20),
    )(*given)


def halo_body(send_ref, features_ref, out_ref):
    node = lax.broadcasted_iota(jnp.int32, (NODE_DEV, N_DOM), 0)
    own = features_ref[...]
    for k in range(HALO_PEER):
        hit = jnp.where(node == send_ref[k : k + 1, :], 1.0, 0.0).astype(BF16)
        out_ref[:, k, :] = lax.dot_general(hit, own, TN, preferred_element_type=F32).astype(BF16)


def counts_body(features_ref, w_ref, nbr_ref, halo_count_ref, own_sum_ref, pre_ref, own_count_ref):
    rows = 32
    lanes = lax.broadcasted_iota(jnp.int32, (rows, NODE_DEV), 1)

    def chunk(step, _):
        at = pl.ds(pl.multiple_of(step * rows, rows), rows)
        for r in range(RELS):
            index = nbr_ref[at, r * FAN : (r + 1) * FAN]
            for half in range(2):
                total = jnp.zeros((rows, NODE_DEV), F32)
                for k in range(FAN):
                    hit = lanes == (index[:, k : k + 1] - half * NODE_DEV)
                    total = total + jnp.where(hit, 1.0, 0.0)
                if half == 0:
                    own_count_ref[r, at, :] = total.astype(BF16)
                else:
                    halo_count_ref[r, at, :] = total.astype(BF16)
        return 0

    lax.fori_loop(0, NODE_DEV // rows, chunk, 0)
    own = features_ref[...]
    for r in range(RELS):
        own_sum_ref[r] = dot(own_count_ref[r], own)
    pre_ref[...] = dot(own, w_ref[0])


def layer_body(neg_ids_ref, halo_count_ref, halo_ref, own_sum_ref, pre_ref, first_ref, second_ref, means_ref, embed_ref, picked_ref):
    halo = halo_ref[...]
    preact = pre_ref[...]
    for r, w_ref in enumerate((first_ref, second_ref)):
        total = own_sum_ref[r] + dot(halo_count_ref[r], halo)
        mean = (total * (1.0 / FAN)).astype(BF16)
        means_ref[r] = mean
        preact = preact + dot(mean, w_ref[0])
    embed = preact.astype(BF16)
    embed_ref[...] = embed
    picked = dot(chosen_rows(neg_ids_ref), embed)[:NEG_DEV]
    picked_ref[...] = jnp.broadcast_to(picked[None], (CHIPS, NEG_DEV, H)).astype(BF16)


def soft_parts(x):
    small = jnp.exp(-jnp.abs(x))
    bottom = 1.0 / (1.0 + small)
    sigmoid = jnp.where(x >= 0, bottom, small * bottom)
    log_one = jnp.where(small < 1e-3, small * (1.0 - 0.5 * small), jnp.log(1.0 + small))
    return sigmoid, jnp.maximum(x, 0.0) + log_one


def largest(x):
    return jnp.max(jnp.max(jnp.abs(x), axis=0, keepdims=True), axis=1, keepdims=True)


def notes_of(values):
    lane = lax.broadcasted_iota(jnp.int32, (NEG_DEV, 128), 1)
    note = jnp.zeros((NEG_DEV, 128), F32)
    for place, value in enumerate(values):
        note = jnp.where(lane == place, value, note)
    return note


def positive_body(count_ref, embed_ref, ends_ref, features_ref, means_ref, grad_ref, note_ref, turned_ref, sources_ref, spread_ref, pairs_ref):
    tiles = count_ref[0]
    pairs_ref[...] = jnp.zeros((NODE_DEV, NODE_DEV), F32)
    node = lax.broadcasted_iota(jnp.int32, (NODE_DEV, TILE), 0)

    def group(step, _):
        sources, targets = [], []
        for j in range(GROUP):
            t = step * GROUP + j
            source = jnp.where(t < tiles, ends_ref[t, 0:1, :], -1)
            sources.append(jnp.where(node == source, 1.0, 0.0).astype(BF16))
            targets.append(jnp.where(node == ends_ref[t, 1:2, :], 1.0, 0.0).astype(BF16))
        pairs_ref[...] += lax.dot_general(
            jnp.concatenate(sources, axis=1), jnp.concatenate(targets, axis=1), NT, preferred_element_type=F32
        )
        return 0

    lax.fori_loop(0, (tiles + (GROUP - 1)) // GROUP, group, 0)
    embed = embed_ref[...]
    pairs = pairs_ref[...]
    sources = jnp.sum(pairs, axis=1, keepdims=True)
    sources_ref[...] = jnp.broadcast_to(sources, (NODE_DEV, 128))
    high, low = split_two(embed.astype(F32) * sources)
    spread_ref[:, 0:H] = high
    spread_ref[:, H:] = low
    scores = lax.dot_general(embed, embed, NT, preferred_element_type=F32)
    sigmoid, softplus = soft_parts(-scores)
    loss = jnp.sum(jnp.sum(pairs * softplus, axis=0, keepdims=True), axis=1, keepdims=True)
    widest = largest(features_ref[...].astype(F32))
    for r in range(RELS):
        widest = jnp.maximum(widest, largest(means_ref[r].astype(F32)))
    high, low = split_two(-((pairs + pairs.T) * sigmoid))
    base = dot(high, embed) + dot(low, embed)
    grad_ref[...] = base
    note_ref[...] = notes_of((loss, tiles.astype(F32), widest, NODE_DEV * largest(base)))
    turned_ref[0:H, :] = features_ref[...].T
    for r in range(RELS):
        turned_ref[(r + 1) * H : (r + 2) * H, :] = means_ref[r].T


def scored(embed, rows, sources, spread):
    scores = lax.dot_general(embed, rows, NT, preferred_element_type=F32)
    sigmoid, softplus = soft_parts(scores)
    per_source = jnp.sum(softplus, axis=1, keepdims=True)
    loss = jnp.sum(per_source * sources, axis=0, keepdims=True) * (1.0 / NEG)
    weight = (sigmoid * (1.0 / NEG)).astype(BF16)
    parts = lax.dot_general(weight, spread, TN, preferred_element_type=F32)
    return weight, loss, parts[:, :H] + parts[:, H:]


def near_body(embed_ref, rows_ref, spread_ref, sources_ref, note_in_ref, weight_ref, part_ref, note_ref):
    rows = rows_ref[...]
    weight, loss, part = scored(embed_ref[...], rows, sources_ref[:, 0:1], spread_ref[...])
    weight_ref[...] = weight
    part_ref[...] = part.astype(part_ref.dtype)
    note = note_in_ref[...]
    lane = lax.broadcasted_iota(jnp.int32, note.shape, 1)
    note = note + jnp.where(lane == 0, loss, 0.0)
    tallest = jnp.maximum(note, jnp.where(lane == 4, largest(rows.astype(F32)), 0.0))
    note = jnp.where(lane == 4, tallest, note)
    note_ref[...] = jnp.where(lane == 5, jnp.maximum(note, largest(part)), note)


def rest_body(near_weight_ref, near_rows_ref, weight_ref, rows_ref, sources_ref, base_ref, grad_ref):
    total = dot(near_weight_ref[...], near_rows_ref[...]) + dot(weight_ref[...], rows_ref[...])
    grad_ref[...] = base_ref[...] + sources_ref[:, 0:1] * total


def shared_note(note_ref):
    loss, tiles, widest, base, tallest, part = (note_ref[0:1, i : i + 1] for i in range(6))
    return loss, tiles, widest * (base + TILE * tiles * tallest), NEG_DEV * widest, part


def merge_body(part_ref, arrived_ref, own_note_ref, other_note_ref, send_ref):
    total = part_ref[...] + arrived_ref[...].astype(F32)
    send_ref[:, :, 0:H] = total.reshape(CHIPS, NEG_DEV, H).astype(BF16)
    both = zip(shared_note(own_note_ref), shared_note(other_note_ref))
    loss, tiles, known, wide, part = (own + other for own, other in both)
    first = loss.astype(BF16).astype(F32)
    second = (loss - first).astype(BF16).astype(F32)
    note = notes_of((first, second, (loss - first) - second, tiles, known, wide, part))
    send_ref[:, :, H:] = jnp.broadcast_to(note[None], (CHIPS, NEG_DEV, 128)).astype(BF16)


def chosen_rows(neg_ids_ref):
    row = lax.broadcasted_iota(jnp.int32, (16, NODE_DEV), 0)
    lane = lax.broadcasted_iota(jnp.int32, (16, NODE_DEV), 1)
    chosen = jnp.zeros((16, NODE_DEV), F32)
    for i in range(NEG_DEV):
        chosen = jnp.where((row == i) & (lane == neg_ids_ref[i]), 1.0, chosen)
    return chosen.astype(BF16)


def half_at(core):
    return pl.ds(pl.multiple_of(core * HALF, HALF), HALF)


def known_body(neg_ids_ref, core_ref, grad_ref, turned_ref, own_ref, other_ref, chosen_ref, pre_ref):
    node = lax.broadcasted_iota(jnp.int32, (NODE_DEV, H), 0)
    grad = grad_ref[...]
    for i in range(NEG_DEV):
        grad = jnp.where(node == neg_ids_ref[i], 0.0, grad)
    pre_ref[...] = grad.astype(BF16)
    turned = turned_ref[...]
    chosen = lax.dot_general(chosen_rows(neg_ids_ref), turned, NT, preferred_element_type=F32)
    chosen_ref[...] = chosen.astype(BF16)
    other_ref[...] = dot(turned, pre_ref[:, half_at(1 - core_ref[0])])
    own_ref[...] = dot(turned, pre_ref[:, half_at(core_ref[0])])


def outer_body(neg_ids_ref, core_ref, arrived_ref, grad_ref, pre_ref, own_ref, other_ref, note_ref, sum_ref, row_ref):
    total = jnp.sum(arrived_ref[...].astype(F32), axis=0)
    note_ref[...] = total[:, H:]
    sum_ref[...] = grad_ref[...]
    for i in range(NEG_DEV):
        at = pl.ds(neg_ids_ref[i], 1)
        sum_ref[at, :] += total[i : i + 1, 0:H]
    row_ref[...] = jnp.zeros((16, H), F32)
    for i in range(NEG_DEV):
        fresh = jnp.bool_(True)
        for j in range(i):
            fresh = fresh & (neg_ids_ref[j] != neg_ids_ref[i])
        row = sum_ref[pl.ds(neg_ids_ref[i], 1), :]
        row_ref[i : i + 1, :] = jnp.where(fresh, row, 0.0)
    pre_ref[...] = sum_ref[...].astype(BF16)
    own_ref[...] = row_ref[:, half_at(core_ref[0])].astype(BF16)
    other_ref[...] = row_ref[:, half_at(1 - core_ref[0])].astype(BF16)


def update_body(known_ref, own_chosen_ref, other_chosen_ref, own_row_ref, other_row_ref, note_ref, out_ref):
    chosen = jnp.concatenate([own_chosen_ref[...], other_chosen_ref[...]], axis=0)
    rows = jnp.concatenate([own_row_ref[...], other_row_ref[...]], axis=0)
    extra = lax.dot_general(chosen, rows, TN, preferred_element_type=F32)
    out_ref[...] = (known_ref[...] + extra) * scale_of(note_ref)


def scale_of(note_ref):
    known, wide, part = (note_ref[0:1, i : i + 1] for i in (4, 5, 6))
    return SPAN / (known + wide * part + TINY)


def factor_of(note_ref):
    return 1.0 / scale_of(note_ref) / (note_ref[0:1, 3:4] * TILE)


def first_half_body(core_ref, half_ref, note_ref, weight_ref, loss_ref):
    note = note_ref[0:1, :]
    loss = note[:, 0:1] + note[:, 1:2] + note[:, 2:3]
    loss_ref[...] = loss / (note[:, 3:4] * TILE)
    weight_ref[...] = (half_ref[...] * factor_of(note_ref)).reshape(RELS + 1, H, HALF)


def second_half_body(core_ref, half_ref, note_ref, begun_ref, weight_ref):
    weight_ref[...] = (half_ref[...] * factor_of(note_ref)).reshape(RELS + 1, H, HALF)


def halves(body, which, extra, alias):
    whole = jax.ShapeDtypeStruct((RELS + 1, H, H), F32)
    block = pl.BlockSpec((RELS + 1, H, HALF), lambda i, core: (0, 0, which(core[0])))
    scalar = pl.BlockSpec((1, 1), lambda i, core: (0, 0))
    full = vmem()
    note = vmem()
    return pl.pallas_call(
        body,
        out_shape=[whole, jax.ShapeDtypeStruct((1, 1), F32)][: 1 + extra],
        grid_spec=pltpu.PrefetchScalarGridSpec(
            num_scalar_prefetch=1,
            grid=(1,),
            in_specs=[full, note] + [pl.BlockSpec(memory_space=pl.ANY)] * len(alias),
            out_specs=[block, scalar][: 1 + extra],
        ),
        input_output_aliases=alias,
        compiler_params=pltpu.CompilerParams(vmem_limit_bytes=28 << 20),
    )


def on_device(features, weights, halo_send, nbr_index, tile_count, edge_ends, neg_ids):
    square = (NODE_DEV, H)
    tall = ((RELS + 1) * H, HALF)
    core = lax.axis_index(NEAR).astype(jnp.int32).reshape(1)
    core, halo_send = lax.optimization_barrier((core, halo_send))
    (outgoing,) = call(halo_body, [hbm((N_DOM, HALO_PEER, H), BF16)], [vmem(), whole((NODE_DEV, H))], (), (halo_send[0].T, features))
    incoming = swap(outgoing, DOM)
    neighbours = nbr_index.reshape(NODE_DEV, RELS * FAN)
    halo_count, own_sum, pre = call(
        counts_body,
        [hbm((RELS, NODE_DEV, 512), BF16), hbm((RELS, *square), F32), hbm(square, F32)],
        [FROM_HBM, weight_at(0), vmem()],
        [pltpu.VMEM((RELS, NODE_DEV, NODE_DEV), BF16)],
        (features, weights, neighbours),
    )
    means, embed, picked = call(
        layer_body,
        [hbm((RELS, *square), BF16), (square, BF16), hbm((CHIPS, NEG_DEV, H), BF16)],
        [smem(), FROM_HBM, vmem(), FROM_HBM, FROM_HBM, weight_at(1), weight_at(2)],
        (),
        (neg_ids, halo_count, incoming.reshape(512, H), own_sum, pre, weights, weights),
    )
    near_rows = swap(picked, FAR).reshape(square)
    base, note, turned, sources, spread = call(
        positive_body,
        [hbm(square, F32), ((8, 128), F32), hbm(((RELS + 1) * H, NODE_DEV), BF16), ((NODE_DEV, 128), F32), ((NODE_DEV, 2 * H), BF16)],
        [smem(), vmem(), vmem(), FROM_HBM, FROM_HBM],
        [pltpu.VMEM((NODE_DEV, NODE_DEV), F32)],
        (tile_count, embed, edge_ends, features, means),
    )
    near_rows, note = lax.optimization_barrier((near_rows, note))
    other_rows = core_swap(near_rows)
    near_weight, near_part, note = call(
        near_body,
        [(square, BF16), (square, F32), ((8, 128), F32)],
        [vmem()] * 5,
        (),
        (embed, near_rows, spread, sources, note),
    )
    weight, other_part, note = call(
        near_body,
        [(square, BF16), (square, BF16), ((8, 128), F32)],
        [vmem()] * 5,
        (),
        (embed, other_rows, spread, sources, note),
    )
    other_note = core_swap(note)
    part_arrived = core_swap(other_part)
    (grad,) = call(
        rest_body,
        [(square, F32)],
        [vmem()] * 5 + [FROM_HBM],
        (),
        (near_weight, near_rows, weight, other_rows, sources, base),
    )
    part_arrived, grad = lax.optimization_barrier((part_arrived, grad))
    (outgoing_grad,) = call(
        merge_body,
        [hbm((CHIPS, NEG_DEV, H + 128), BF16)],
        [vmem()] * 4,
        (),
        (near_part, part_arrived, note, other_note),
    )
    outgoing_grad, grad = lax.optimization_barrier((outgoing_grad, grad))
    arrived = swap(outgoing_grad, FAR)
    known_own, known_other, chosen = call(
        known_body,
        [(tall, F32), (tall, F32), ((16, (RELS + 1) * H), BF16)],
        [smem(), smem(), vmem(), FROM_HBM],
        [pltpu.VMEM(square, BF16)],
        (neg_ids, core, grad, turned),
    )
    other_chosen = core_swap(chosen)
    known = known_own + core_swap(known_other)
    arrived, known, other_chosen = lax.optimization_barrier((arrived, known, other_chosen))
    pre_grad, own_row, send_row, note = call(
        outer_body,
        [hbm(square, BF16), ((16, HALF), BF16), ((16, HALF), BF16), ((NEG_DEV, 128), F32)],
        [smem(), smem(), vmem(), vmem()],
        [pltpu.VMEM(square, F32), pltpu.VMEM((16, H), F32)],
        (neg_ids, core, arrived, grad),
    )
    (partial,) = call(
        update_body,
        [(tall, F32)],
        [vmem()] * 6,
        (),
        (known, chosen, other_chosen, own_row, core_swap(send_row), note),
    )
    chunks = (CHIPS, 24, HALF)
    mine = jnp.sum(swap(partial.astype(F16).reshape(chunks), FAR).astype(F32), axis=0).astype(F16)
    half = swap(jnp.broadcast_to(mine, chunks), FAR).reshape(tall)
    other_half = core_swap(half).astype(F32)
    half = half.astype(F32)
    note = near_memory(note)
    begun, mean_loss = halves(first_half_body, lambda c: c, 1, {})(core, near_memory(half), note)
    (begun, other_half) = lax.optimization_barrier((begun, other_half))
    (weight_grad,) = halves(second_half_body, lambda c: 1 - c, 0, {3: 0})(core, near_memory(other_half), note, begun)
    return weight_grad, mean_loss.reshape(()), pre_grad


def solution(mesh):
    torus = Mesh(mesh.devices.reshape(4, 4, 4, 2), DOM)
    in_specs = (
        P(DOM, None),
        P(),
        P(DOM, None, None),
        P(DOM, None, None),
        P(DOM),
        P(DOM, None, None),
        P(DOM),
    )
    out_specs = (P(), P(), P(DOM, None))
    return jax.shard_map(on_device, mesh=torus, in_specs=in_specs, out_specs=out_specs, check_vma=False)
```

```python
import jax
import jax.numpy as jnp
from jax import lax
from jax.experimental import pallas as pl
from jax.experimental.pallas import tpu as pltpu
from jax.sharding import Mesh
from jax.sharding import PartitionSpec as P

DOM = ("dom_0", "dom_1", "dom_2", "dom_3")
FAR = ("dom_0", "dom_1", "dom_2")
NEAR = ("dom_3",)
H = 512
RELS = 2
FAN = 8
TILE = 256
NODE_DEV = 512
NEG = 1024
NEG_DEV = 8
N_DOM = 128
HALO_PEER = 4
CHIPS = 64
GROUP = 4
HALF = 256
F32 = jnp.float32
BF16 = jnp.bfloat16
F16 = jnp.float16
SPAN = 60000.0
TINY = 1e-30
NT = (((1,), (1,)), ((), ()))
TN = (((0,), (0,)), ((), ()))
FROM_HBM = "hbm"


def swap(x, axes):
    return lax.all_to_all(x, axes, split_axis=0, concat_axis=0, tiled=True)


def core_swap(x):
    return lax.ppermute(x, "dom_3", [(0, 1), (1, 0)])


def dot(a, b):
    return jnp.dot(a, b, preferred_element_type=F32)


def split_two(x):
    high = x.astype(BF16)
    return high, (x - high.astype(F32)).astype(BF16)


def vmem():
    return pl.BlockSpec(memory_space=pltpu.VMEM)


def whole(shape):
    return pl.BlockSpec(shape, lambda i: (0,) * len(shape))


def weight_at(k):
    return pl.BlockSpec((1, H, H), lambda i: (k, 0, 0))


def smem():
    return pl.BlockSpec(memory_space=pltpu.SMEM)


def near_memory(x):
    return pltpu.with_memory_space_constraint(x, pltpu.VMEM)


def hbm(shape, kind):
    return pltpu.HBM(shape, kind)


def call(body, outs, specs, scratch=(), args=()):
    given = []
    for spec, x in zip(specs, args):
        if spec is FROM_HBM:
            x = pltpu.with_memory_space_constraint(x, pltpu.HBM)
        elif spec.memory_space == pltpu.VMEM and x.dtype != jnp.int32:
            x = near_memory(x)
        given.append(x)
    return pl.pallas_call(
        body,
        out_shape=[pltpu.VMEM(*o) if isinstance(o, tuple) else o for o in outs],
        grid=(1,),
        in_specs=[whole(x.shape) if spec is FROM_HBM else spec for spec, x in zip(specs, args)],
        out_specs=[vmem() if isinstance(o, tuple) else whole(o.shape) for o in outs],
        scratch_shapes=list(scratch),
        compiler_params=pltpu.CompilerParams(vmem_limit_bytes=28 << 20),
    )(*given)


def halo_body(send_ref, features_ref, out_ref):
    node = lax.broadcasted_iota(jnp.int32, (NODE_DEV, N_DOM), 0)
    own = features_ref[...]
    for k in range(HALO_PEER):
        hit = jnp.where(node == send_ref[k : k + 1, :], 1.0, 0.0).astype(BF16)
        out_ref[:, k, :] = lax.dot_general(hit, own, TN, preferred_element_type=F32).astype(BF16)


def counts_body(features_ref, w_ref, nbr_ref, halo_count_ref, own_sum_ref, pre_ref, own_count_ref):
    rows = 32
    lanes = lax.broadcasted_iota(jnp.int32, (rows, NODE_DEV), 1)

    def chunk(step, _):
        at = pl.ds(pl.multiple_of(step * rows, rows), rows)
        for r in range(RELS):
            index = nbr_ref[at, r * FAN : (r + 1) * FAN]
            for half in range(2):
                total = jnp.zeros((rows, NODE_DEV), F32)
                for k in range(FAN):
                    hit = lanes == (index[:, k : k + 1] - half * NODE_DEV)
                    total = total + jnp.where(hit, 1.0, 0.0)
                if half == 0:
                    own_count_ref[r, at, :] = total.astype(BF16)
                else:
                    halo_count_ref[r, at, :] = total.astype(BF16)
        return 0

    lax.fori_loop(0, NODE_DEV // rows, chunk, 0)
    own = features_ref[...]
    for r in range(RELS):
        own_sum_ref[r] = dot(own_count_ref[r], own)
    pre_ref[...] = dot(own, w_ref[0])


def layer_body(neg_ids_ref, halo_count_ref, halo_ref, own_sum_ref, pre_ref, w_ref, mean_ref, embed_ref, picked_ref, total_ref):
    r = pl.program_id(0)
    total = own_sum_ref[0] + dot(halo_count_ref[0], halo_ref[...])
    mean = (total * (1.0 / FAN)).astype(BF16)
    mean_ref[0] = mean
    part = dot(mean, w_ref[0])

    @pl.when(r == 0)
    def _():
        total_ref[...] = pre_ref[...] + part

    @pl.when(r == RELS - 1)
    def _():
        embed = (total_ref[...] + part).astype(BF16)
        embed_ref[...] = embed
        picked = dot(chosen_rows(neg_ids_ref), embed)[:NEG_DEV]
        picked_ref[...] = jnp.broadcast_to(picked[None], (CHIPS, NEG_DEV, H)).astype(BF16)


def layer(neg_ids, halo_count, halo, own_sum, pre, weights):
    per_relation = pl.BlockSpec((1, NODE_DEV, H), lambda r: (r, 0, 0))
    from_hbm = lambda x: pltpu.with_memory_space_constraint(x, pltpu.HBM)
    return pl.pallas_call(
        layer_body,
        out_shape=[hbm((RELS, NODE_DEV, H), BF16), pltpu.VMEM((NODE_DEV, H), BF16), hbm((CHIPS, NEG_DEV, H), BF16)],
        grid=(RELS,),
        in_specs=[
            smem(),
            per_relation,
            vmem(),
            per_relation,
            pl.BlockSpec((NODE_DEV, H), lambda r: (0, 0)),
            pl.BlockSpec((1, H, H), lambda r: (r + 1, 0, 0)),
        ],
        out_specs=[per_relation, vmem(), pl.BlockSpec((CHIPS, NEG_DEV, H), lambda r: (0, 0, 0))],
        scratch_shapes=[pltpu.VMEM((NODE_DEV, H), F32)],
        compiler_params=pltpu.CompilerParams(vmem_limit_bytes=28 << 20),
    )(neg_ids, from_hbm(halo_count), near_memory(halo), from_hbm(own_sum), from_hbm(pre), from_hbm(weights))


def soft_parts(x):
    small = jnp.exp(-jnp.abs(x))
    bottom = 1.0 / (1.0 + small)
    sigmoid = jnp.where(x >= 0, bottom, small * bottom)
    log_one = jnp.where(small < 1e-3, small * (1.0 - 0.5 * small), jnp.log(1.0 + small))
    return sigmoid, jnp.maximum(x, 0.0) + log_one


def largest(x):
    return jnp.max(jnp.max(jnp.abs(x), axis=0, keepdims=True), axis=1, keepdims=True)


def notes_of(values):
    lane = lax.broadcasted_iota(jnp.int32, (NEG_DEV, 128), 1)
    note = jnp.zeros((NEG_DEV, 128), F32)
    for place, value in enumerate(values):
        note = jnp.where(lane == place, value, note)
    return note


def positive_body(count_ref, embed_ref, ends_ref, features_ref, means_ref, grad_ref, note_ref, sources_ref, spread_ref, pairs_ref, sigmoid_ref, softplus_ref):
    embed = embed_ref[...]
    scores = lax.dot_general(embed, embed, NT, preferred_element_type=F32)
    sigmoid, softplus = soft_parts(-scores)
    sigmoid_ref[...] = sigmoid
    softplus_ref[...] = softplus
    pairs_ref[...] = jnp.zeros((NODE_DEV, NODE_DEV), F32)
    node = lax.broadcasted_iota(jnp.int32, (NODE_DEV, TILE), 0)
    widest = largest(features_ref[...].astype(F32))
    for r in range(RELS):
        widest = jnp.maximum(widest, largest(means_ref[r].astype(F32)))
    tiles = count_ref[0]

    def group(step, _):
        sources, targets = [], []
        for j in range(GROUP):
            t = step * GROUP + j
            source = jnp.where(t < tiles, ends_ref[t, 0:1, :], -1)
            sources.append(jnp.where(node == source, 1.0, 0.0).astype(BF16))
            targets.append(jnp.where(node == ends_ref[t, 1:2, :], 1.0, 0.0).astype(BF16))
        pairs_ref[...] += lax.dot_general(
            jnp.concatenate(sources, axis=1), jnp.concatenate(targets, axis=1), NT, preferred_element_type=F32
        )
        return 0

    lax.fori_loop(0, (tiles + (GROUP - 1)) // GROUP, group, 0)
    pairs = pairs_ref[...]
    sources = jnp.sum(pairs, axis=1, keepdims=True)
    sources_ref[...] = jnp.broadcast_to(sources, (NODE_DEV, 128))
    high, low = split_two(embed.astype(F32) * sources)
    spread_ref[:, 0:H] = high
    spread_ref[:, H:] = low
    loss = jnp.sum(jnp.sum(pairs * softplus_ref[...], axis=0, keepdims=True), axis=1, keepdims=True)
    high, low = split_two(-((pairs + pairs.T) * sigmoid_ref[...]))
    base = dot(high, embed) + dot(low, embed)
    grad_ref[...] = base
    note_ref[...] = notes_of((loss, tiles.astype(F32), widest, NODE_DEV * largest(base)))


def scored(embed, rows, sources, spread):
    scores = lax.dot_general(embed, rows, NT, preferred_element_type=F32)
    sigmoid, softplus = soft_parts(scores)
    per_source = jnp.sum(softplus, axis=1, keepdims=True)
    loss = jnp.sum(per_source * sources, axis=0, keepdims=True) * (1.0 / NEG)
    weight = (sigmoid * (1.0 / NEG)).astype(BF16)
    parts = lax.dot_general(weight, spread, TN, preferred_element_type=F32)
    return weight, loss, parts[:, :H] + parts[:, H:]


def near_body(embed_ref, rows_ref, spread_ref, sources_ref, note_in_ref, weight_ref, part_ref, note_ref):
    rows = rows_ref[...]
    weight, loss, part = scored(embed_ref[...], rows, sources_ref[:, 0:1], spread_ref[...])
    weight_ref[...] = weight
    part_ref[...] = part.astype(part_ref.dtype)
    note = note_in_ref[...]
    lane = lax.broadcasted_iota(jnp.int32, note.shape, 1)
    note = note + jnp.where(lane == 0, loss, 0.0)
    tallest = jnp.maximum(note, jnp.where(lane == 4, largest(rows.astype(F32)), 0.0))
    note = jnp.where(lane == 4, tallest, note)
    note_ref[...] = jnp.where(lane == 5, jnp.maximum(note, largest(part)), note)


def rest_body(near_weight_ref, near_rows_ref, weight_ref, rows_ref, sources_ref, base_ref, grad_ref):
    total = dot(near_weight_ref[...], near_rows_ref[...]) + dot(weight_ref[...], rows_ref[...])
    grad_ref[...] = base_ref[...] + sources_ref[:, 0:1] * total


def shared_note(note_ref):
    loss, tiles, widest, base, tallest, part = (note_ref[0:1, i : i + 1] for i in range(6))
    return loss, tiles, widest * (base + TILE * tiles * tallest), NEG_DEV * widest, part


def merge_body(part_ref, arrived_ref, own_note_ref, other_note_ref, send_ref):
    total = part_ref[...] + arrived_ref[...].astype(F32)
    send_ref[:, :, 0:H] = total.reshape(CHIPS, NEG_DEV, H).astype(BF16)
    both = zip(shared_note(own_note_ref), shared_note(other_note_ref))
    loss, tiles, known, wide, part = (own + other for own, other in both)
    first = loss.astype(BF16).astype(F32)
    second = (loss - first).astype(BF16).astype(F32)
    note = notes_of((first, second, (loss - first) - second, tiles, known, wide, part))
    send_ref[:, :, H:] = jnp.broadcast_to(note[None], (CHIPS, NEG_DEV, 128)).astype(BF16)


def chosen_rows(neg_ids_ref):
    row = lax.broadcasted_iota(jnp.int32, (16, NODE_DEV), 0)
    lane = lax.broadcasted_iota(jnp.int32, (16, NODE_DEV), 1)
    chosen = jnp.zeros((16, NODE_DEV), F32)
    for i in range(NEG_DEV):
        chosen = jnp.where((row == i) & (lane == neg_ids_ref[i]), 1.0, chosen)
    return chosen.astype(BF16)


def half_at(core):
    return pl.ds(pl.multiple_of(core * HALF, HALF), HALF)


def known_body(neg_ids_ref, core_ref, grad_ref, features_ref, means_ref, own_ref, other_ref, chosen_ref):
    node = lax.broadcasted_iota(jnp.int32, (NODE_DEV, H), 0)
    grad = grad_ref[...]
    for i in range(NEG_DEV):
        grad = jnp.where(node == neg_ids_ref[i], 0.0, grad)
    pre = grad.astype(BF16)
    picks = chosen_rows(neg_ids_ref)
    swapped = core_ref[0] == 1
    for r, rows in enumerate((features_ref[...], means_ref[0], means_ref[1])):
        at = pl.ds(r * H, H)
        both = lax.dot_general(rows, pre, TN, preferred_element_type=F32)
        first, second = both[:, :HALF], both[:, HALF:]
        own_ref[at, :] = jnp.where(swapped, second, first)
        other_ref[at, :] = jnp.where(swapped, first, second)
        chosen_ref[:, at] = dot(picks, rows).astype(BF16)


def outer_body(neg_ids_ref, core_ref, arrived_ref, grad_ref, pre_ref, own_ref, other_ref, note_ref, sum_ref, row_ref):
    total = jnp.sum(arrived_ref[...].astype(F32), axis=0)
    note_ref[...] = total[:, H:]
    sum_ref[...] = grad_ref[...]
    for i in range(NEG_DEV):
        at = pl.ds(neg_ids_ref[i], 1)
        sum_ref[at, :] += total[i : i + 1, 0:H]
    row_ref[...] = jnp.zeros((16, H), F32)
    for i in range(NEG_DEV):
        fresh = jnp.bool_(True)
        for j in range(i):
            fresh = fresh & (neg_ids_ref[j] != neg_ids_ref[i])
        row = sum_ref[pl.ds(neg_ids_ref[i], 1), :]
        row_ref[i : i + 1, :] = jnp.where(fresh, row, 0.0)
    pre_ref[...] = sum_ref[...].astype(BF16)
    own_ref[...] = row_ref[:, half_at(core_ref[0])].astype(BF16)
    other_ref[...] = row_ref[:, half_at(1 - core_ref[0])].astype(BF16)


def update_body(known_ref, own_chosen_ref, other_chosen_ref, own_row_ref, other_row_ref, note_ref, out_ref):
    chosen = jnp.concatenate([own_chosen_ref[...], other_chosen_ref[...]], axis=0)
    rows = jnp.concatenate([own_row_ref[...], other_row_ref[...]], axis=0)
    extra = lax.dot_general(chosen, rows, TN, preferred_element_type=F32)
    out_ref[...] = (known_ref[...] + extra) * scale_of(note_ref)


def scale_of(note_ref):
    known, wide, part = (note_ref[0:1, i : i + 1] for i in (4, 5, 6))
    return SPAN / (known + wide * part + TINY)


def factor_of(note_ref):
    return 1.0 / scale_of(note_ref) / (note_ref[0:1, 3:4] * TILE)


def first_half_body(core_ref, half_ref, note_ref, weight_ref, loss_ref):
    note = note_ref[0:1, :]
    loss = note[:, 0:1] + note[:, 1:2] + note[:, 2:3]
    loss_ref[...] = loss / (note[:, 3:4] * TILE)
    weight_ref[...] = (half_ref[...] * factor_of(note_ref)).reshape(RELS + 1, H, HALF)


def second_half_body(core_ref, half_ref, note_ref, begun_ref, weight_ref):
    weight_ref[...] = (half_ref[...] * factor_of(note_ref)).reshape(RELS + 1, H, HALF)


def halves(body, which, extra, alias):
    whole = jax.ShapeDtypeStruct((RELS + 1, H, H), F32)
    block = pl.BlockSpec((RELS + 1, H, HALF), lambda i, core: (0, 0, which(core[0])))
    scalar = pl.BlockSpec((1, 1), lambda i, core: (0, 0))
    full = vmem()
    note = vmem()
    return pl.pallas_call(
        body,
        out_shape=[whole, jax.ShapeDtypeStruct((1, 1), F32)][: 1 + extra],
        grid_spec=pltpu.PrefetchScalarGridSpec(
            num_scalar_prefetch=1,
            grid=(1,),
            in_specs=[full, note] + [pl.BlockSpec(memory_space=pl.ANY)] * len(alias),
            out_specs=[block, scalar][: 1 + extra],
        ),
        input_output_aliases=alias,
        compiler_params=pltpu.CompilerParams(vmem_limit_bytes=28 << 20),
    )


def on_device(features, weights, halo_send, nbr_index, tile_count, edge_ends, neg_ids):
    square = (NODE_DEV, H)
    tall = ((RELS + 1) * H, HALF)
    core = lax.axis_index(NEAR).astype(jnp.int32).reshape(1)
    core, halo_send = lax.optimization_barrier((core, halo_send))
    (outgoing,) = call(halo_body, [hbm((N_DOM, HALO_PEER, H), BF16)], [FROM_HBM, FROM_HBM], (), (halo_send[0].T, features))
    incoming = swap(outgoing, DOM)
    neighbours = nbr_index.reshape(NODE_DEV, RELS * FAN)
    halo_count, own_sum, pre = call(
        counts_body,
        [hbm((RELS, NODE_DEV, 512), BF16), hbm((RELS, *square), F32), hbm(square, F32)],
        [FROM_HBM, weight_at(0), FROM_HBM],
        [pltpu.VMEM((RELS, NODE_DEV, NODE_DEV), BF16)],
        (features, weights, neighbours),
    )
    means, embed, picked = layer(neg_ids, halo_count, incoming.reshape(512, H), own_sum, pre, weights)
    near_rows = swap(picked, FAR).reshape(square)
    base, note, sources, spread = call(
        positive_body,
        [hbm(square, F32), ((8, 128), F32), ((NODE_DEV, 128), F32), ((NODE_DEV, 2 * H), BF16)],
        [smem(), vmem(), FROM_HBM, FROM_HBM, FROM_HBM],
        [pltpu.VMEM(square, F32)] * 3,
        (tile_count, embed, edge_ends, features, means),
    )
    near_rows, note = lax.optimization_barrier((near_rows, note))
    other_rows = core_swap(near_rows)
    near_weight, near_part, note = call(
        near_body,
        [(square, BF16), (square, F32), ((8, 128), F32)],
        [vmem()] * 5,
        (),
        (embed, near_rows, spread, sources, note),
    )
    weight, other_part, note = call(
        near_body,
        [(square, BF16), (square, BF16), ((8, 128), F32)],
        [vmem()] * 5,
        (),
        (embed, other_rows, spread, sources, note),
    )
    other_note = core_swap(note)
    part_arrived = core_swap(other_part)
    (grad,) = call(
        rest_body,
        [(square, F32)],
        [vmem()] * 5 + [FROM_HBM],
        (),
        (near_weight, near_rows, weight, other_rows, sources, base),
    )
    part_arrived, grad = lax.optimization_barrier((part_arrived, grad))
    (outgoing_grad,) = call(
        merge_body,
        [((CHIPS, NEG_DEV, H + 128), BF16)],
        [vmem()] * 4,
        (),
        (near_part, part_arrived, note, other_note),
    )
    outgoing_grad, grad = lax.optimization_barrier((outgoing_grad, grad))
    arrived = swap(outgoing_grad, FAR)
    known_own, known_other, chosen = call(
        known_body,
        [(tall, F32), (tall, F32), ((16, (RELS + 1) * H), BF16)],
        [smem(), smem(), vmem(), FROM_HBM, FROM_HBM],
        (),
        (neg_ids, core, grad, features, means),
    )
    other_chosen = core_swap(chosen)
    known = known_own + core_swap(known_other)
    arrived, known, other_chosen = lax.optimization_barrier((arrived, known, other_chosen))
    pre_grad, own_row, send_row, note = call(
        outer_body,
        [hbm(square, BF16), ((16, HALF), BF16), ((16, HALF), BF16), ((NEG_DEV, 128), F32)],
        [smem(), smem(), vmem(), vmem()],
        [pltpu.VMEM(square, F32), pltpu.VMEM((16, H), F32)],
        (neg_ids, core, arrived, grad),
    )
    (partial,) = call(
        update_body,
        [(tall, F32)],
        [vmem()] * 6,
        (),
        (known, chosen, other_chosen, own_row, core_swap(send_row), note),
    )
    chunks = (CHIPS, 24, HALF)
    mine = jnp.sum(swap(partial.astype(F16).reshape(chunks), FAR).astype(F32), axis=0).astype(F16)
    half = swap(jnp.broadcast_to(mine, chunks), FAR).reshape(tall)
    other_half = core_swap(half).astype(F32)
    half = half.astype(F32)
    note = near_memory(note)
    begun, mean_loss = halves(first_half_body, lambda c: c, 1, {})(core, near_memory(half), note)
    (begun, other_half) = lax.optimization_barrier((begun, other_half))
    (weight_grad,) = halves(second_half_body, lambda c: 1 - c, 0, {3: 0})(core, near_memory(other_half), note, begun)
    return weight_grad, mean_loss.reshape(()), pre_grad


def solution(mesh):
    torus = Mesh(mesh.devices.reshape(4, 4, 4, 2), DOM)
    in_specs = (
        P(DOM, None),
        P(),
        P(DOM, None, None),
        P(DOM, None, None),
        P(DOM),
        P(DOM, None, None),
        P(DOM),
    )
    out_specs = (P(), P(), P(DOM, None))
    return jax.shard_map(on_device, mesh=torus, in_specs=in_specs, out_specs=out_specs, check_vma=False)
```

```python
import jax
import jax.numpy as jnp
from jax import lax
from jax.experimental import pallas as pl
from jax.experimental.pallas import tpu as pltpu
from jax.sharding import Mesh
from jax.sharding import PartitionSpec as P

DOM = ("dom_0", "dom_1", "dom_2", "dom_3")
FAR = ("dom_0", "dom_1", "dom_2")
NEAR = ("dom_3",)
H = 512
RELS = 2
FAN = 8
TILE = 256
NODE_DEV = 512
NEG = 1024
NEG_DEV = 8
N_DOM = 128
HALO_PEER = 4
CHIPS = 64
GROUP = 4
HALF = 256
F32 = jnp.float32
BF16 = jnp.bfloat16
F16 = jnp.float16
SPAN = 60000.0
TINY = 1e-30
NT = (((1,), (1,)), ((), ()))
TN = (((0,), (0,)), ((), ()))
FROM_HBM = "hbm"


def swap(x, axes):
    return lax.all_to_all(x, axes, split_axis=0, concat_axis=0, tiled=True)


def core_swap(x):
    return lax.ppermute(x, "dom_3", [(0, 1), (1, 0)])


def dot(a, b):
    return jnp.dot(a, b, preferred_element_type=F32)


def split_two(x):
    high = x.astype(BF16)
    return high, (x - high.astype(F32)).astype(BF16)


def vmem():
    return pl.BlockSpec(memory_space=pltpu.VMEM)


def whole(shape):
    return pl.BlockSpec(shape, lambda i: (0,) * len(shape))


def weight_at(k):
    return pl.BlockSpec((1, H, H), lambda i: (k, 0, 0))


def smem():
    return pl.BlockSpec(memory_space=pltpu.SMEM)


def near_memory(x):
    return pltpu.with_memory_space_constraint(x, pltpu.VMEM)


def hbm(shape, kind):
    return pltpu.HBM(shape, kind)


def call(body, outs, specs, scratch=(), args=()):
    given = []
    for spec, x in zip(specs, args):
        if spec is FROM_HBM:
            x = pltpu.with_memory_space_constraint(x, pltpu.HBM)
        elif spec.memory_space == pltpu.VMEM and x.dtype != jnp.int32:
            x = near_memory(x)
        given.append(x)
    return pl.pallas_call(
        body,
        out_shape=[pltpu.VMEM(*o) if isinstance(o, tuple) else o for o in outs],
        grid=(1,),
        in_specs=[whole(x.shape) if spec is FROM_HBM else spec for spec, x in zip(specs, args)],
        out_specs=[vmem() if isinstance(o, tuple) else whole(o.shape) for o in outs],
        scratch_shapes=list(scratch),
        compiler_params=pltpu.CompilerParams(vmem_limit_bytes=28 << 20),
    )(*given)


def halo_body(send_ref, features_ref, out_ref):
    node = lax.broadcasted_iota(jnp.int32, (NODE_DEV, N_DOM), 0)
    own = features_ref[...]
    for k in range(HALO_PEER):
        hit = jnp.where(node == send_ref[k : k + 1, :], 1.0, 0.0).astype(BF16)
        out_ref[:, k, :] = lax.dot_general(hit, own, TN, preferred_element_type=F32).astype(BF16)


def counts_body(features_ref, w_ref, nbr_ref, halo_count_ref, own_sum_ref, pre_ref, own_count_ref):
    rows = 32
    lanes = lax.broadcasted_iota(jnp.int32, (rows, NODE_DEV), 1)

    def chunk(step, _):
        at = pl.ds(pl.multiple_of(step * rows, rows), rows)
        for r in range(RELS):
            index = nbr_ref[at, r * FAN : (r + 1) * FAN]
            for half in range(2):
                total = jnp.zeros((rows, NODE_DEV), F32)
                for k in range(FAN):
                    hit = lanes == (index[:, k : k + 1] - half * NODE_DEV)
                    total = total + jnp.where(hit, 1.0, 0.0)
                if half == 0:
                    own_count_ref[r, at, :] = total.astype(BF16)
                else:
                    halo_count_ref[r, at, :] = total.astype(BF16)
        return 0

    lax.fori_loop(0, NODE_DEV // rows, chunk, 0)
    own = features_ref[...]
    for r in range(RELS):
        own_sum_ref[r] = dot(own_count_ref[r], own)
    pre_ref[...] = dot(own, w_ref[0])


def layer_body(neg_ids_ref, halo_count_ref, halo_ref, own_sum_ref, pre_ref, first_ref, second_ref, means_ref, embed_ref, picked_ref):
    halo = halo_ref[...]
    preact = pre_ref[...]
    for r, w_ref in enumerate((first_ref, second_ref)):
        total = own_sum_ref[r] + dot(halo_count_ref[r], halo)
        mean = (total * (1.0 / FAN)).astype(BF16)
        means_ref[r] = mean
        preact = preact + dot(mean, w_ref[0])
    embed = preact.astype(BF16)
    embed_ref[...] = embed
    picked = dot(chosen_rows(neg_ids_ref), embed)[:NEG_DEV]
    picked_ref[...] = jnp.broadcast_to(picked[None], (CHIPS, NEG_DEV, H)).astype(BF16)


def soft_parts(x):
    small = jnp.exp(-jnp.abs(x))
    bottom = 1.0 / (1.0 + small)
    sigmoid = jnp.where(x >= 0, bottom, small * bottom)
    log_one = jnp.where(small < 1e-3, small * (1.0 - 0.5 * small), jnp.log(1.0 + small))
    return sigmoid, jnp.maximum(x, 0.0) + log_one


def largest(x):
    return jnp.max(jnp.max(jnp.abs(x), axis=0, keepdims=True), axis=1, keepdims=True)


def notes_of(values):
    lane = lax.broadcasted_iota(jnp.int32, (NEG_DEV, 128), 1)
    note = jnp.zeros((NEG_DEV, 128), F32)
    for place, value in enumerate(values):
        note = jnp.where(lane == place, value, note)
    return note


def positive_body(count_ref, embed_ref, ends_ref, features_ref, means_ref, grad_ref, note_ref, sources_ref, spread_ref, pairs_ref, sigmoid_ref, softplus_ref):
    embed = embed_ref[...]
    scores = lax.dot_general(embed, embed, NT, preferred_element_type=F32)
    sigmoid, softplus = soft_parts(-scores)
    sigmoid_ref[...] = sigmoid
    softplus_ref[...] = softplus
    pairs_ref[...] = jnp.zeros((NODE_DEV, NODE_DEV), F32)
    node = lax.broadcasted_iota(jnp.int32, (NODE_DEV, TILE), 0)
    widest = largest(features_ref[...].astype(F32))
    for r in range(RELS):
        widest = jnp.maximum(widest, largest(means_ref[r].astype(F32)))
    tiles = count_ref[0]

    def group(step, _):
        sources, targets = [], []
        for j in range(GROUP):
            t = step * GROUP + j
            source = jnp.where(t < tiles, ends_ref[t, 0:1, :], -1)
            sources.append(jnp.where(node == source, 1.0, 0.0).astype(BF16))
            targets.append(jnp.where(node == ends_ref[t, 1:2, :], 1.0, 0.0).astype(BF16))
        pairs_ref[...] += lax.dot_general(
            jnp.concatenate(sources, axis=1), jnp.concatenate(targets, axis=1), NT, preferred_element_type=F32
        )
        return 0

    lax.fori_loop(0, (tiles + (GROUP - 1)) // GROUP, group, 0)
    pairs = pairs_ref[...]
    sources = jnp.sum(pairs, axis=1, keepdims=True)
    sources_ref[...] = jnp.broadcast_to(sources, (NODE_DEV, 128))
    high, low = split_two(embed.astype(F32) * sources)
    spread_ref[:, 0:H] = high
    spread_ref[:, H:] = low
    loss = jnp.sum(jnp.sum(pairs * softplus_ref[...], axis=0, keepdims=True), axis=1, keepdims=True)
    high, low = split_two(-((pairs + pairs.T) * sigmoid_ref[...]))
    base = dot(high, embed) + dot(low, embed)
    grad_ref[...] = base
    count = tiles.astype(F32)
    known = widest * NODE_DEV * largest(base)
    note_ref[...] = notes_of((loss, count, 0.0, known, widest * TILE * count, NEG_DEV * widest, 0.0))


def scored(embed, rows, sources, spread):
    scores = lax.dot_general(embed, rows, NT, preferred_element_type=F32)
    sigmoid, softplus = soft_parts(scores)
    per_source = jnp.sum(softplus, axis=1, keepdims=True)
    loss = jnp.sum(per_source * sources, axis=0, keepdims=True) * (1.0 / NEG)
    weight = (sigmoid * (1.0 / NEG)).astype(BF16)
    parts = lax.dot_general(weight, spread, TN, preferred_element_type=F32)
    return weight, loss, parts[:, :H] + parts[:, H:]


def near_body(embed_ref, rows_ref, spread_ref, sources_ref, note_in_ref, weight_ref, part_ref, note_ref):
    rows = rows_ref[...]
    weight, loss, part = scored(embed_ref[...], rows, sources_ref[:, 0:1], spread_ref[...])
    weight_ref[...] = weight
    part_ref[...] = part.astype(part_ref.dtype)
    note = note_in_ref[...]
    lane = lax.broadcasted_iota(jnp.int32, note.shape, 1)
    tallest = largest(rows.astype(F32))
    note = jnp.where(lane == 0, note + loss, note)
    note = jnp.where(lane == 2, jnp.maximum(note, note[:, 3:4] + note[:, 4:5] * tallest), note)
    note_ref[...] = jnp.where(lane == 6, jnp.maximum(note, largest(part)), note)


def rest_body(near_weight_ref, near_rows_ref, weight_ref, rows_ref, sources_ref, base_ref, grad_ref):
    total = dot(near_weight_ref[...], near_rows_ref[...]) + dot(weight_ref[...], rows_ref[...])
    grad_ref[...] = base_ref[...] + sources_ref[:, 0:1] * total


def merge_body(part_ref, arrived_ref, own_note_ref, other_note_ref, send_ref):
    note = own_note_ref[...] + other_note_ref[...]
    first = note.astype(BF16).astype(F32)
    second = (note - first).astype(BF16).astype(F32)
    third = (note - first) - second
    lane = lax.broadcasted_iota(jnp.int32, note.shape, 1)
    note = jnp.where(lane == 3, pltpu.roll(second, 3, 1), jnp.where(lane == 4, pltpu.roll(third, 4, 1), first))
    send_ref[:, :, H:] = jnp.broadcast_to(note[None], (CHIPS, NEG_DEV, 128)).astype(BF16)
    total = part_ref[...] + arrived_ref[...].astype(F32)
    send_ref[:, :, 0:H] = total.reshape(CHIPS, NEG_DEV, H).astype(BF16)


def chosen_rows(neg_ids_ref):
    row = lax.broadcasted_iota(jnp.int32, (16, NODE_DEV), 0)
    lane = lax.broadcasted_iota(jnp.int32, (16, NODE_DEV), 1)
    chosen = jnp.zeros((16, NODE_DEV), F32)
    for i in range(NEG_DEV):
        chosen = jnp.where((row == i) & (lane == neg_ids_ref[i]), 1.0, chosen)
    return chosen.astype(BF16)


def half_at(core):
    return pl.ds(pl.multiple_of(core * HALF, HALF), HALF)


def known_body(neg_ids_ref, core_ref, grad_ref, features_ref, means_ref, own_ref, other_ref, chosen_ref):
    node = lax.broadcasted_iota(jnp.int32, (NODE_DEV, H), 0)
    grad = grad_ref[...]
    for i in range(NEG_DEV):
        grad = jnp.where(node == neg_ids_ref[i], 0.0, grad)
    pre = grad.astype(BF16)
    picks = chosen_rows(neg_ids_ref)
    swapped = core_ref[0] == 1
    for r, rows in enumerate((features_ref[...], means_ref[0], means_ref[1])):
        at = pl.ds(r * H, H)
        both = lax.dot_general(rows, pre, TN, preferred_element_type=F32)
        first, second = both[:, :HALF], both[:, HALF:]
        own_ref[at, :] = jnp.where(swapped, second, first)
        other_ref[at, :] = jnp.where(swapped, first, second)
        chosen_ref[:, at] = dot(picks, rows).astype(BF16)


def outer_body(neg_ids_ref, core_ref, arrived_ref, grad_ref, total_ref, own_ref, other_ref, note_ref, row_ref):
    total = jnp.sum(arrived_ref[...].astype(F32), axis=0)
    note_ref[...] = total[:, H:]
    total_ref[...] = total[:, :H]
    row_ref[...] = jnp.zeros((16, H), F32)
    firsts = []
    for i in range(NEG_DEV):
        first = i
        for j in reversed(range(i)):
            first = jnp.where(neg_ids_ref[j] == neg_ids_ref[i], j, first)
        firsts.append(first)
        row = grad_ref[pl.ds(neg_ids_ref[i], 1), :]
        row_ref[i : i + 1, :] = row if i == 0 else jnp.where(first == i, row, 0.0)
    for i, first in enumerate(firsts):
        row_ref[pl.ds(first, 1), :] += total_ref[i : i + 1, :]
    own_ref[...] = row_ref[:, half_at(core_ref[0])].astype(BF16)
    other_ref[...] = row_ref[:, half_at(1 - core_ref[0])].astype(BF16)


def pre_body(neg_ids_ref, total_ref, grad_ref, pre_ref, sum_ref):
    sum_ref[...] = grad_ref[...]
    for i in range(NEG_DEV):
        sum_ref[pl.ds(neg_ids_ref[i], 1), :] += total_ref[i : i + 1, :]
    pre_ref[...] = sum_ref[...].astype(BF16)


def update_body(known_ref, own_chosen_ref, other_chosen_ref, own_row_ref, other_row_ref, note_ref, out_ref, factor_ref):
    chosen = jnp.concatenate([own_chosen_ref[...], other_chosen_ref[...]], axis=0)
    rows = jnp.concatenate([own_row_ref[...], other_row_ref[...]], axis=0)
    extra = lax.dot_general(chosen, rows, TN, preferred_element_type=F32)
    known, wide, part = (note_ref[0:1, i : i + 1] for i in (2, 5, 6))
    bound = known + wide * part + TINY
    out_ref[...] = (known_ref[...] + extra) * (SPAN / bound)
    factor_ref[...] = jnp.broadcast_to(bound / SPAN / (note_ref[0:1, 1:2] * TILE), (8, HALF))


def first_half_body(core_ref, half_ref, factor_ref, note_ref, weight_ref, loss_ref):
    note = note_ref[0:1, :]
    loss_ref[...] = (note[:, 0:1] + note[:, 3:4] + note[:, 4:5]) / (note[:, 1:2] * TILE)
    weight_ref[0] = half_ref[...] * factor_ref[0:1, :]


def second_half_body(core_ref, half_ref, factor_ref, note_ref, begun_ref, weight_ref):
    weight_ref[0] = half_ref[...] * factor_ref[0:1, :]


def halves(body, which, extra, alias):
    whole_weight = jax.ShapeDtypeStruct((RELS + 1, H, H), F32)
    block = pl.BlockSpec((1, H, HALF), lambda r, core: (r, 0, which(core[0])))
    scalar = pl.BlockSpec((1, 1), lambda r, core: (0, 0))
    full = pl.BlockSpec((H, HALF), lambda r, core: (r, 0))
    return pl.pallas_call(
        body,
        out_shape=[whole_weight, jax.ShapeDtypeStruct((1, 1), F32)][: 1 + extra],
        grid_spec=pltpu.PrefetchScalarGridSpec(
            num_scalar_prefetch=1,
            grid=(RELS + 1,),
            in_specs=[full, vmem(), vmem()] + [pl.BlockSpec(memory_space=pl.ANY)] * len(alias),
            out_specs=[block, scalar][: 1 + extra],
        ),
        input_output_aliases=alias,
        compiler_params=pltpu.CompilerParams(vmem_limit_bytes=28 << 20),
    )


def on_device(features, weights, halo_send, nbr_index, tile_count, edge_ends, neg_ids):
    square = (NODE_DEV, H)
    tall = ((RELS + 1) * H, HALF)
    core = lax.axis_index(NEAR).astype(jnp.int32).reshape(1)
    core, halo_send = lax.optimization_barrier((core, halo_send))
    (outgoing,) = call(halo_body, [hbm((N_DOM, HALO_PEER, H), BF16)], [FROM_HBM, FROM_HBM], (), (halo_send[0].T, features))
    incoming = swap(outgoing, DOM)
    neighbours = nbr_index.reshape(NODE_DEV, RELS * FAN)
    weights = pltpu.with_memory_space_constraint(weights, pltpu.HBM)
    halo_count, own_sum, pre = call(
        counts_body,
        [hbm((RELS, NODE_DEV, 512), BF16), ((RELS, *square), F32), hbm(square, F32)],
        [FROM_HBM, weight_at(0), vmem()],
        [pltpu.VMEM((RELS, NODE_DEV, NODE_DEV), BF16)],
        (features, weights, neighbours),
    )
    means, embed, picked = call(
        layer_body,
        [hbm((RELS, *square), BF16), (square, BF16), hbm((CHIPS, NEG_DEV, H), BF16)],
        [smem(), FROM_HBM, vmem(), vmem(), FROM_HBM, weight_at(1), weight_at(2)],
        (),
        (neg_ids, halo_count, incoming.reshape(512, H), own_sum, pre, weights, weights),
    )
    near_rows = swap(picked, FAR).reshape(square)
    base, note, sources, spread = call(
        positive_body,
        [hbm(square, F32), ((8, 128), F32), ((NODE_DEV, 128), F32), ((NODE_DEV, 2 * H), BF16)],
        [smem(), vmem(), FROM_HBM, FROM_HBM, FROM_HBM],
        [pltpu.VMEM(square, F32)] * 3,
        (tile_count, embed, edge_ends, features, means),
    )
    near_rows, note = lax.optimization_barrier((near_rows, note))
    other_rows = core_swap(near_rows)
    near_weight, near_part, note = call(
        near_body,
        [(square, BF16), (square, F32), ((8, 128), F32)],
        [vmem()] * 5,
        (),
        (embed, near_rows, spread, sources, note),
    )
    weight, other_part, note = call(
        near_body,
        [(square, BF16), (square, BF16), ((8, 128), F32)],
        [vmem()] * 5,
        (),
        (embed, other_rows, spread, sources, note),
    )
    other_note = core_swap(note)
    part_arrived = core_swap(other_part)
    (grad,) = call(
        rest_body,
        [(square, F32)],
        [vmem()] * 5 + [FROM_HBM],
        (),
        (near_weight, near_rows, weight, other_rows, sources, base),
    )
    part_arrived, grad = lax.optimization_barrier((part_arrived, grad))
    (outgoing_grad,) = call(
        merge_body,
        [((CHIPS, NEG_DEV, H + 128), BF16)],
        [vmem()] * 4,
        (),
        (near_part, part_arrived, note, other_note),
    )
    outgoing_grad, grad = lax.optimization_barrier((outgoing_grad, grad))
    arrived = swap(outgoing_grad, FAR)
    known_own, known_other, chosen = call(
        known_body,
        [(tall, F32), (tall, F32), ((16, (RELS + 1) * H), BF16)],
        [smem(), smem(), vmem(), FROM_HBM, FROM_HBM],
        (),
        (neg_ids, core, grad, features, means),
    )
    other_chosen = core_swap(chosen)
    known = known_own + core_swap(known_other)
    arrived, known, other_chosen = lax.optimization_barrier((arrived, known, other_chosen))
    total, own_row, send_row, note = call(
        outer_body,
        [((NEG_DEV, H), F32), ((16, HALF), BF16), ((16, HALF), BF16), ((NEG_DEV, 128), F32)],
        [smem(), smem(), vmem(), vmem()],
        [pltpu.VMEM((16, H), F32)],
        (neg_ids, core, arrived, grad),
    )
    other_row = core_swap(send_row)
    (pre_grad,) = call(
        pre_body,
        [hbm(square, BF16)],
        [smem(), vmem(), vmem()],
        [pltpu.VMEM(square, F32)],
        (neg_ids, total, grad),
    )
    partial, factor = call(
        update_body,
        [(tall, F32), ((8, HALF), F32)],
        [vmem()] * 6,
        (),
        (known, chosen, other_chosen, own_row, other_row, note),
    )
    chunks = (CHIPS, 24, HALF)
    mine = jnp.sum(swap(partial.astype(F16).reshape(chunks), FAR).astype(F32), axis=0).astype(F16)
    half = swap(jnp.broadcast_to(mine, chunks), FAR).reshape(tall)
    other_half = core_swap(half).astype(F32)
    half = half.astype(F32)
    close = near_memory(factor), near_memory(note)
    begun, mean_loss = halves(first_half_body, lambda c: c, 1, {})(core, near_memory(half), *close)
    (begun, other_half) = lax.optimization_barrier((begun, other_half))
    (weight_grad,) = halves(second_half_body, lambda c: 1 - c, 0, {4: 0})(core, near_memory(other_half), *close, begun)
    return weight_grad, mean_loss.reshape(()), pre_grad


def solution(mesh):
    torus = Mesh(mesh.devices.reshape(4, 4, 4, 2), DOM)
    in_specs = (
        P(DOM, None),
        P(),
        P(DOM, None, None),
        P(DOM, None, None),
        P(DOM),
        P(DOM, None, None),
        P(DOM),
    )
    out_specs = (P(), P(), P(DOM, None))
    return jax.shard_map(on_device, mesh=torus, in_specs=in_specs, out_specs=out_specs, check_vma=False)
```

```python
import jax
import jax.numpy as jnp
from jax import lax
from jax.experimental import pallas as pl
from jax.experimental.pallas import tpu as pltpu
from jax.sharding import Mesh
from jax.sharding import PartitionSpec as P

DOM = ("dom_0", "dom_1", "dom_2", "dom_3")
FAR = ("dom_0", "dom_1", "dom_2")
NEAR = ("dom_3",)
H = 512
RELS = 2
FAN = 8
TILE = 256
NODE_DEV = 512
NEG = 1024
NEG_DEV = 8
N_DOM = 128
HALO_PEER = 4
CHIPS = 64
GROUP = 4
HALF = 256
F32 = jnp.float32
BF16 = jnp.bfloat16
F16 = jnp.float16
SPAN = 60000.0
TINY = 1e-30
NT = (((1,), (1,)), ((), ()))
TN = (((0,), (0,)), ((), ()))
FROM_HBM = "hbm"
BY_HAND = "by_hand"


def swap(x, axes):
    return lax.all_to_all(x, axes, split_axis=0, concat_axis=0, tiled=True)


def core_swap(x):
    return lax.ppermute(x, "dom_3", [(0, 1), (1, 0)])


def dot(a, b):
    return jnp.dot(a, b, preferred_element_type=F32)


def split_two(x):
    high = x.astype(BF16)
    return high, (x - high.astype(F32)).astype(BF16)


def vmem():
    return pl.BlockSpec(memory_space=pltpu.VMEM)


def whole(shape):
    return pl.BlockSpec(shape, lambda i: (0,) * len(shape))


def smem():
    return pl.BlockSpec(memory_space=pltpu.SMEM)


def near_memory(x):
    return pltpu.with_memory_space_constraint(x, pltpu.VMEM)


def hbm(shape, kind):
    return pltpu.HBM(shape, kind)


def call(body, outs, specs, scratch=(), args=()):
    given, ins, made, back = [], [], [], []
    for spec, x in zip(specs, args):
        if spec is FROM_HBM or spec is BY_HAND:
            x = pltpu.with_memory_space_constraint(x, pltpu.HBM)
            spec = whole(x.shape) if spec is FROM_HBM else pl.BlockSpec(memory_space=pl.ANY)
        elif spec.memory_space == pltpu.VMEM and x.dtype != jnp.int32:
            x = near_memory(x)
        given.append(x)
        ins.append(spec)
    for o in outs:
        if isinstance(o, tuple) and len(o) == 3:
            made.append(hbm(*o[:2]))
            back.append(pl.BlockSpec(memory_space=pl.ANY))
        elif isinstance(o, tuple):
            made.append(pltpu.VMEM(*o))
            back.append(vmem())
        else:
            made.append(o)
            back.append(whole(o.shape))
    return pl.pallas_call(
        body,
        out_shape=made,
        grid=(1,),
        in_specs=ins,
        out_specs=back,
        scratch_shapes=list(scratch),
        compiler_params=pltpu.CompilerParams(vmem_limit_bytes=28 << 20),
    )(*given)


def halo_body(send_ref, features_ref, out_ref):
    node = lax.broadcasted_iota(jnp.int32, (NODE_DEV, N_DOM), 0)
    own = features_ref[...]
    for k in range(HALO_PEER):
        hit = jnp.where(node == send_ref[k : k + 1, :], 1.0, 0.0).astype(BF16)
        out_ref[:, k, :] = lax.dot_general(hit, own, TN, preferred_element_type=F32).astype(BF16)


def counts_body(features_ref, w_ref, nbr_ref, halo_count_ref, own_sum_ref, pre_ref, own_buf, w_buf, halo_buf, count_buf, sum_buf, pre_buf, sems):
    copy = pltpu.make_async_copy
    fetch_own = copy(features_ref, own_buf, sems.at[0])
    fetch_w = copy(w_ref.at[0], w_buf, sems.at[1])
    fetch_own.start()
    fetch_w.start()
    rows = 32
    lanes = lax.broadcasted_iota(jnp.int32, (rows, NODE_DEV), 1)

    def chunk(step, _):
        at = pl.ds(pl.multiple_of(step * rows, rows), rows)
        for r in range(RELS):
            index = nbr_ref[at, r * FAN : (r + 1) * FAN]
            for half in range(2):
                total = jnp.zeros((rows, NODE_DEV), F32)
                for k in range(FAN):
                    hit = lanes == (index[:, k : k + 1] - half * NODE_DEV)
                    total = total + jnp.where(hit, 1.0, 0.0)
                if half == 0:
                    count_buf[r, at, :] = total.astype(BF16)
                else:
                    halo_buf[r, at, :] = total.astype(BF16)
        return 0

    lax.fori_loop(0, NODE_DEV // rows, chunk, 0)
    leave = [copy(halo_buf, halo_count_ref, sems.at[2])]
    leave[0].start()
    fetch_own.wait()
    own = own_buf[...]
    for r in range(RELS):
        sum_buf[r] = dot(count_buf[r], own)
        leave.append(copy(sum_buf.at[r], own_sum_ref.at[r], sems.at[3 + r]))
        leave[-1].start()
    fetch_w.wait()
    pre_buf[...] = dot(own, w_buf[...])
    leave.append(copy(pre_buf, pre_ref, sems.at[5]))
    leave[-1].start()
    for one in leave:
        one.wait()


def layer_body(neg_ids_ref, halo_count_ref, halo_ref, own_sum_ref, pre_ref, w_ref, means_ref, embed_ref, picked_ref, count_buf, sum_buf, w_buf, pre_buf, mean_buf, sems):
    copy = pltpu.make_async_copy
    counts = [copy(halo_count_ref.at[r], count_buf.at[r], sems.at[r]) for r in range(RELS)]
    sums = [copy(own_sum_ref.at[r], sum_buf.at[r], sems.at[2 + r]) for r in range(RELS)]
    maps = [copy(w_ref.at[r + 1], w_buf.at[r], sems.at[4 + r]) for r in range(RELS)]
    first = copy(pre_ref, pre_buf, sems.at[6])
    for one in (counts[0], sums[0], maps[0], counts[1], sums[1], first, maps[1]):
        one.start()
    halo = halo_ref[...]
    parts, leave = [], []
    for r in range(RELS):
        counts[r].wait()
        total = dot(count_buf[r], halo)
        sums[r].wait()
        mean_buf[r] = ((sum_buf[r] + total) * (1.0 / FAN)).astype(BF16)
        leave.append(copy(mean_buf.at[r], means_ref.at[r], sems.at[7 + r]))
        leave[r].start()
        maps[r].wait()
        parts.append(dot(mean_buf[r], w_buf[r]))
    first.wait()
    embed = (pre_buf[...] + parts[0] + parts[1]).astype(BF16)
    embed_ref[...] = embed
    picked = dot(chosen_rows(neg_ids_ref), embed)[:NEG_DEV]
    picked_ref[...] = jnp.broadcast_to(picked[None], (CHIPS, NEG_DEV, H)).astype(BF16)
    for one in leave:
        one.wait()


def soft_parts(x):
    small = jnp.exp(-jnp.abs(x))
    bottom = 1.0 / (1.0 + small)
    sigmoid = jnp.where(x >= 0, bottom, small * bottom)
    log_one = jnp.where(small < 1e-3, small * (1.0 - 0.5 * small), jnp.log(1.0 + small))
    return sigmoid, jnp.maximum(x, 0.0) + log_one


def largest(x):
    return jnp.max(jnp.max(jnp.abs(x), axis=0, keepdims=True), axis=1, keepdims=True)


def notes_of(values):
    lane = lax.broadcasted_iota(jnp.int32, (NEG_DEV, 128), 1)
    note = jnp.zeros((NEG_DEV, 128), F32)
    for place, value in enumerate(values):
        note = jnp.where(lane == place, value, note)
    return note


def positive_body(count_ref, embed_ref, ends_ref, features_ref, means_ref, grad_ref, note_ref, sources_ref, spread_ref, pairs_ref, sigmoid_ref, softplus_ref):
    embed = embed_ref[...]
    scores = lax.dot_general(embed, embed, NT, preferred_element_type=F32)
    sigmoid, softplus = soft_parts(-scores)
    sigmoid_ref[...] = sigmoid
    softplus_ref[...] = softplus
    pairs_ref[...] = jnp.zeros((NODE_DEV, NODE_DEV), F32)
    node = lax.broadcasted_iota(jnp.int32, (NODE_DEV, TILE), 0)
    widest = largest(features_ref[...].astype(F32))
    for r in range(RELS):
        widest = jnp.maximum(widest, largest(means_ref[r].astype(F32)))
    tiles = count_ref[0]

    def group(step, _):
        sources, targets = [], []
        for j in range(GROUP):
            t = step * GROUP + j
            source = jnp.where(t < tiles, ends_ref[t, 0:1, :], -1)
            sources.append(jnp.where(node == source, 1.0, 0.0).astype(BF16))
            targets.append(jnp.where(node == ends_ref[t, 1:2, :], 1.0, 0.0).astype(BF16))
        pairs_ref[...] += lax.dot_general(
            jnp.concatenate(sources, axis=1), jnp.concatenate(targets, axis=1), NT, preferred_element_type=F32
        )
        return 0

    lax.fori_loop(0, (tiles + (GROUP - 1)) // GROUP, group, 0)
    pairs = pairs_ref[...]
    sources = jnp.sum(pairs, axis=1, keepdims=True)
    sources_ref[...] = jnp.broadcast_to(sources, (NODE_DEV, 128))
    high, low = split_two(embed.astype(F32) * sources)
    spread_ref[:, 0:H] = high
    spread_ref[:, H:] = low
    loss = jnp.sum(jnp.sum(pairs * softplus_ref[...], axis=0, keepdims=True), axis=1, keepdims=True)
    high, low = split_two(-((pairs + pairs.T) * sigmoid_ref[...]))
    base = dot(high, embed) + dot(low, embed)
    grad_ref[...] = base
    count = tiles.astype(F32)
    known = widest * NODE_DEV * largest(base)
    note_ref[...] = notes_of((loss, count, 0.0, known, widest * TILE * count, NEG_DEV * widest, 0.0))


def scored(embed, rows, sources, spread):
    scores = lax.dot_general(embed, rows, NT, preferred_element_type=F32)
    sigmoid, softplus = soft_parts(scores)
    per_source = jnp.sum(softplus, axis=1, keepdims=True)
    loss = jnp.sum(per_source * sources, axis=0, keepdims=True) * (1.0 / NEG)
    weight = (sigmoid * (1.0 / NEG)).astype(BF16)
    parts = lax.dot_general(weight, spread, TN, preferred_element_type=F32)
    return weight, loss, parts[:, :H] + parts[:, H:]


def near_body(embed_ref, rows_ref, spread_ref, sources_ref, note_in_ref, weight_ref, part_ref, note_ref):
    rows = rows_ref[...]
    weight, loss, part = scored(embed_ref[...], rows, sources_ref[:, 0:1], spread_ref[...])
    weight_ref[...] = weight
    part_ref[...] = part.astype(part_ref.dtype)
    note = note_in_ref[...]
    lane = lax.broadcasted_iota(jnp.int32, note.shape, 1)
    tallest = largest(rows.astype(F32))
    note = jnp.where(lane == 0, note + loss, note)
    note = jnp.where(lane == 2, jnp.maximum(note, note[:, 3:4] + note[:, 4:5] * tallest), note)
    note_ref[...] = jnp.where(lane == 6, jnp.maximum(note, largest(part)), note)


def rest_body(near_weight_ref, near_rows_ref, weight_ref, rows_ref, sources_ref, base_ref, grad_ref):
    total = dot(near_weight_ref[...], near_rows_ref[...]) + dot(weight_ref[...], rows_ref[...])
    grad_ref[...] = base_ref[...] + sources_ref[:, 0:1] * total


def merge_body(part_ref, arrived_ref, own_note_ref, other_note_ref, send_ref):
    note = own_note_ref[...] + other_note_ref[...]
    first = note.astype(BF16).astype(F32)
    second = (note - first).astype(BF16).astype(F32)
    third = (note - first) - second
    lane = lax.broadcasted_iota(jnp.int32, note.shape, 1)
    note = jnp.where(lane == 3, pltpu.roll(second, 3, 1), jnp.where(lane == 4, pltpu.roll(third, 4, 1), first))
    send_ref[:, :, H:] = jnp.broadcast_to(note[None], (CHIPS, NEG_DEV, 128)).astype(BF16)
    total = part_ref[...] + arrived_ref[...].astype(F32)
    send_ref[:, :, 0:H] = total.reshape(CHIPS, NEG_DEV, H).astype(BF16)


def chosen_rows(neg_ids_ref):
    row = lax.broadcasted_iota(jnp.int32, (16, NODE_DEV), 0)
    lane = lax.broadcasted_iota(jnp.int32, (16, NODE_DEV), 1)
    chosen = jnp.zeros((16, NODE_DEV), F32)
    for i in range(NEG_DEV):
        chosen = jnp.where((row == i) & (lane == neg_ids_ref[i]), 1.0, chosen)
    return chosen.astype(BF16)


def half_at(core):
    return pl.ds(pl.multiple_of(core * HALF, HALF), HALF)


def known_body(neg_ids_ref, core_ref, grad_ref, features_ref, means_ref, own_ref, other_ref, chosen_ref):
    node = lax.broadcasted_iota(jnp.int32, (NODE_DEV, H), 0)
    grad = grad_ref[...]
    for i in range(NEG_DEV):
        grad = jnp.where(node == neg_ids_ref[i], 0.0, grad)
    pre = grad.astype(BF16)
    picks = chosen_rows(neg_ids_ref)
    swapped = core_ref[0] == 1
    for r, rows in enumerate((features_ref[...], means_ref[0], means_ref[1])):
        at = pl.ds(r * H, H)
        both = lax.dot_general(rows, pre, TN, preferred_element_type=F32)
        first, second = both[:, :HALF], both[:, HALF:]
        own_ref[at, :] = jnp.where(swapped, second, first)
        other_ref[at, :] = jnp.where(swapped, first, second)
        chosen_ref[:, at] = dot(picks, rows).astype(BF16)


def outer_body(neg_ids_ref, core_ref, arrived_ref, grad_ref, total_ref, own_ref, other_ref, note_ref, row_ref):
    total = jnp.sum(arrived_ref[...].astype(F32), axis=0)
    note_ref[...] = total[:, H:]
    total_ref[...] = total[:, :H]
    row_ref[...] = jnp.zeros((16, H), F32)
    firsts = []
    for i in range(NEG_DEV):
        first = i
        for j in reversed(range(i)):
            first = jnp.where(neg_ids_ref[j] == neg_ids_ref[i], j, first)
        firsts.append(first)
        row = grad_ref[pl.ds(neg_ids_ref[i], 1), :]
        row_ref[i : i + 1, :] = row if i == 0 else jnp.where(first == i, row, 0.0)
    for i, first in enumerate(firsts):
        row_ref[pl.ds(first, 1), :] += total_ref[i : i + 1, :]
    own_ref[...] = row_ref[:, half_at(core_ref[0])].astype(BF16)
    other_ref[...] = row_ref[:, half_at(1 - core_ref[0])].astype(BF16)


def pre_body(neg_ids_ref, total_ref, grad_ref, pre_ref, sum_ref):
    sum_ref[...] = grad_ref[...]
    for i in range(NEG_DEV):
        sum_ref[pl.ds(neg_ids_ref[i], 1), :] += total_ref[i : i + 1, :]
    pre_ref[...] = sum_ref[...].astype(BF16)


def update_body(known_ref, own_chosen_ref, other_chosen_ref, own_row_ref, other_row_ref, note_ref, out_ref, factor_ref):
    chosen = jnp.concatenate([own_chosen_ref[...], other_chosen_ref[...]], axis=0)
    rows = jnp.concatenate([own_row_ref[...], other_row_ref[...]], axis=0)
    extra = lax.dot_general(chosen, rows, TN, preferred_element_type=F32)
    known, wide, part = (note_ref[0:1, i : i + 1] for i in (2, 5, 6))
    bound = known + wide * part + TINY
    out_ref[...] = (known_ref[...] + extra) * (SPAN / bound)
    factor_ref[...] = jnp.broadcast_to(bound / SPAN / (note_ref[0:1, 1:2] * TILE), (8, HALF))


def first_half_body(core_ref, half_ref, factor_ref, note_ref, weight_ref, loss_ref):
    note = note_ref[0:1, :]
    loss_ref[...] = (note[:, 0:1] + note[:, 3:4] + note[:, 4:5]) / (note[:, 1:2] * TILE)
    weight_ref[...] = (half_ref[...] * factor_ref[0:1, :]).reshape(RELS + 1, H, HALF)


def second_half_body(core_ref, half_ref, factor_ref, note_ref, begun_ref, weight_ref):
    weight_ref[...] = (half_ref[...] * factor_ref[0:1, :]).reshape(RELS + 1, H, HALF)


def halves(body, which, extra, alias):
    whole_weight = jax.ShapeDtypeStruct((RELS + 1, H, H), F32)
    block = pl.BlockSpec((RELS + 1, H, HALF), lambda r, core: (0, 0, which(core[0])))
    scalar = pl.BlockSpec((1, 1), lambda r, core: (0, 0))
    return pl.pallas_call(
        body,
        out_shape=[whole_weight, jax.ShapeDtypeStruct((1, 1), F32)][: 1 + extra],
        grid_spec=pltpu.PrefetchScalarGridSpec(
            num_scalar_prefetch=1,
            grid=(1,),
            in_specs=[vmem(), vmem(), vmem()] + [pl.BlockSpec(memory_space=pl.ANY)] * len(alias),
            out_specs=[block, scalar][: 1 + extra],
        ),
        input_output_aliases=alias,
        compiler_params=pltpu.CompilerParams(vmem_limit_bytes=28 << 20),
    )


def on_device(features, weights, halo_send, nbr_index, tile_count, edge_ends, neg_ids):
    square = (NODE_DEV, H)
    tall = ((RELS + 1) * H, HALF)
    core = lax.axis_index(NEAR).astype(jnp.int32).reshape(1)
    core, halo_send = lax.optimization_barrier((core, halo_send))
    (outgoing,) = call(halo_body, [hbm((N_DOM, HALO_PEER, H), BF16)], [FROM_HBM, FROM_HBM], (), (halo_send[0].T, features))
    incoming = swap(outgoing, DOM)
    neighbours = nbr_index.reshape(NODE_DEV, RELS * FAN)
    two = (RELS, *square)
    halo_count, own_sum, pre = call(
        counts_body,
        [(two, BF16, BY_HAND), (two, F32, BY_HAND), (square, F32, BY_HAND)],
        [BY_HAND, BY_HAND, vmem()],
        [pltpu.VMEM(square, BF16)] * 2 + [pltpu.VMEM(two, BF16)] * 2 + [pltpu.VMEM(two, F32), pltpu.VMEM(square, F32), pltpu.SemaphoreType.DMA((6,))],
        (features, weights, neighbours),
    )
    means, embed, picked = call(
        layer_body,
        [(two, BF16, BY_HAND), (square, BF16), hbm((CHIPS, NEG_DEV, H), BF16)],
        [smem(), BY_HAND, vmem(), BY_HAND, BY_HAND, BY_HAND],
        [pltpu.VMEM(two, BF16), pltpu.VMEM(two, F32), pltpu.VMEM(two, BF16), pltpu.VMEM(square, F32), pltpu.VMEM(two, BF16), pltpu.SemaphoreType.DMA((9,))],
        (neg_ids, halo_count, incoming.reshape(512, H), own_sum, pre, weights),
    )
    near_rows = swap(picked, FAR).reshape(square)
    base, note, sources, spread = call(
        positive_body,
        [hbm(square, F32), ((8, 128), F32), ((NODE_DEV, 128), F32), ((NODE_DEV, 2 * H), BF16)],
        [smem(), vmem(), FROM_HBM, FROM_HBM, FROM_HBM],
        [pltpu.VMEM(square, F32)] * 3,
        (tile_count, embed, edge_ends, features, means),
    )
    near_rows, note = lax.optimization_barrier((near_rows, note))
    other_rows = core_swap(near_rows)
    near_weight, near_part, note = call(
        near_body,
        [(square, BF16), (square, F32), ((8, 128), F32)],
        [vmem()] * 5,
        (),
        (embed, near_rows, spread, sources, note),
    )
    weight, other_part, note = call(
        near_body,
        [(square, BF16), (square, BF16), ((8, 128), F32)],
        [vmem()] * 5,
        (),
        (embed, other_rows, spread, sources, note),
    )
    other_note = core_swap(note)
    part_arrived = core_swap(other_part)
    (grad,) = call(
        rest_body,
        [(square, F32)],
        [vmem()] * 5 + [FROM_HBM],
        (),
        (near_weight, near_rows, weight, other_rows, sources, base),
    )
    part_arrived, grad = lax.optimization_barrier((part_arrived, grad))
    (outgoing_grad,) = call(
        merge_body,
        [((CHIPS, NEG_DEV, H + 128), BF16)],
        [vmem()] * 4,
        (),
        (near_part, part_arrived, note, other_note),
    )
    outgoing_grad, grad = lax.optimization_barrier((outgoing_grad, grad))
    arrived = swap(outgoing_grad, FAR)
    known_own, known_other, chosen = call(
        known_body,
        [(tall, F32), (tall, F32), ((16, (RELS + 1) * H), BF16)],
        [smem(), smem(), vmem(), FROM_HBM, FROM_HBM],
        (),
        (neg_ids, core, grad, features, means),
    )
    other_chosen = core_swap(chosen)
    known = known_own + core_swap(known_other)
    arrived, known, other_chosen = lax.optimization_barrier((arrived, known, other_chosen))
    total, own_row, send_row, note = call(
        outer_body,
        [((NEG_DEV, H), F32), ((16, HALF), BF16), ((16, HALF), BF16), ((NEG_DEV, 128), F32)],
        [smem(), smem(), vmem(), vmem()],
        [pltpu.VMEM((16, H), F32)],
        (neg_ids, core, arrived, grad),
    )
    other_row = core_swap(send_row)
    (pre_grad,) = call(
        pre_body,
        [hbm(square, BF16)],
        [smem(), vmem(), vmem()],
        [pltpu.VMEM(square, F32)],
        (neg_ids, total, grad),
    )
    partial, factor = call(
        update_body,
        [(tall, F32), ((8, HALF), F32)],
        [vmem()] * 6,
        (),
        (known, chosen, other_chosen, own_row, other_row, note),
    )
    chunks = (CHIPS, 24, HALF)
    sums = swap(partial.astype(F16).reshape(chunks), FAR)
    mine = jnp.sum(sums.astype(F32), axis=0).astype(F16)
    half = swap(jnp.broadcast_to(mine, chunks), FAR).reshape(tall)
    other_half = core_swap(half).astype(F32)
    half = half.astype(F32)
    close = near_memory(factor), near_memory(note)
    begun, mean_loss = halves(first_half_body, lambda c: c, 1, {})(core, near_memory(half), *close)
    (begun, other_half) = lax.optimization_barrier((begun, other_half))
    (weight_grad,) = halves(second_half_body, lambda c: 1 - c, 0, {4: 0})(core, near_memory(other_half), *close, begun)
    return weight_grad, mean_loss.reshape(()), pre_grad


def solution(mesh):
    torus = Mesh(mesh.devices.reshape(4, 4, 4, 2), DOM)
    in_specs = (
        P(DOM, None),
        P(),
        P(DOM, None, None),
        P(DOM, None, None),
        P(DOM),
        P(DOM, None, None),
        P(DOM),
    )
    out_specs = (P(), P(), P(DOM, None))
    return jax.shard_map(on_device, mesh=torus, in_specs=in_specs, out_specs=out_specs, check_vma=False)
```

```python
import jax
import jax.numpy as jnp
from jax import lax
from jax.experimental import pallas as pl
from jax.experimental.pallas import tpu as pltpu
from jax.sharding import Mesh
from jax.sharding import PartitionSpec as P

DOM = ("dom_0", "dom_1", "dom_2", "dom_3")
FAR = ("dom_0", "dom_1", "dom_2")
NEAR = ("dom_3",)
H = 512
RELS = 2
FAN = 8
TILE = 256
NODE_DEV = 512
NEG = 1024
NEG_DEV = 8
N_DOM = 128
HALO_PEER = 4
CHIPS = 64
GROUP = 4
HALF = 256
F32 = jnp.float32
BF16 = jnp.bfloat16
F16 = jnp.float16
SPAN = 60000.0
TINY = 1e-30
NT = (((1,), (1,)), ((), ()))
TN = (((0,), (0,)), ((), ()))
FROM_HBM = "hbm"
BY_HAND = "by_hand"


def swap(x, axes):
    return lax.all_to_all(x, axes, split_axis=0, concat_axis=0, tiled=True)


def core_swap(x):
    return lax.ppermute(x, "dom_3", [(0, 1), (1, 0)])


def dot(a, b):
    return jnp.dot(a, b, preferred_element_type=F32)


def split_two(x):
    high = x.astype(BF16)
    return high, (x - high.astype(F32)).astype(BF16)


def vmem():
    return pl.BlockSpec(memory_space=pltpu.VMEM)


def whole(shape):
    return pl.BlockSpec(shape, lambda i: (0,) * len(shape))


def smem():
    return pl.BlockSpec(memory_space=pltpu.SMEM)


def near_memory(x):
    return pltpu.with_memory_space_constraint(x, pltpu.VMEM)


def hbm(shape, kind):
    return pltpu.HBM(shape, kind)


def call(body, outs, specs, scratch=(), args=()):
    given, ins, made, back = [], [], [], []
    for spec, x in zip(specs, args):
        if spec is FROM_HBM or spec is BY_HAND:
            x = pltpu.with_memory_space_constraint(x, pltpu.HBM)
            spec = whole(x.shape) if spec is FROM_HBM else pl.BlockSpec(memory_space=pl.ANY)
        elif spec.memory_space == pltpu.VMEM and x.dtype != jnp.int32:
            x = near_memory(x)
        given.append(x)
        ins.append(spec)
    for o in outs:
        if isinstance(o, tuple) and len(o) == 3:
            made.append(hbm(*o[:2]))
            back.append(pl.BlockSpec(memory_space=pl.ANY))
        elif isinstance(o, tuple):
            made.append(pltpu.VMEM(*o))
            back.append(vmem())
        else:
            made.append(o)
            back.append(whole(o.shape))
    return pl.pallas_call(
        body,
        out_shape=made,
        grid=(1,),
        in_specs=ins,
        out_specs=back,
        scratch_shapes=list(scratch),
        compiler_params=pltpu.CompilerParams(vmem_limit_bytes=28 << 20),
    )(*given)


def halo_body(send_ref, features_ref, out_ref):
    node = lax.broadcasted_iota(jnp.int32, (NODE_DEV, N_DOM), 0)
    own = features_ref[...]
    for k in range(HALO_PEER):
        hit = jnp.where(node == send_ref[k : k + 1, :], 1.0, 0.0).astype(BF16)
        out_ref[:, k, :] = lax.dot_general(hit, own, TN, preferred_element_type=F32).astype(BF16)


def counts_body(features_ref, w_ref, nbr_ref, halo_count_ref, own_sum_ref, pre_ref, own_buf, w_buf, halo_buf, count_buf, sum_buf, pre_buf, sems):
    copy = pltpu.make_async_copy
    fetch_own = copy(features_ref, own_buf, sems.at[0])
    fetch_w = copy(w_ref.at[0], w_buf, sems.at[1])
    fetch_own.start()
    fetch_w.start()
    rows = 32
    lanes = lax.broadcasted_iota(jnp.int32, (rows, NODE_DEV), 1)

    def chunk(step, _):
        at = pl.ds(pl.multiple_of(step * rows, rows), rows)
        for r in range(RELS):
            index = nbr_ref[at, r * FAN : (r + 1) * FAN]
            for half in range(2):
                total = jnp.zeros((rows, NODE_DEV), F32)
                for k in range(FAN):
                    hit = lanes == (index[:, k : k + 1] - half * NODE_DEV)
                    total = total + jnp.where(hit, 1.0, 0.0)
                if half == 0:
                    count_buf[r, at, :] = total.astype(BF16)
                else:
                    halo_buf[r, at, :] = total.astype(BF16)
        return 0

    lax.fori_loop(0, NODE_DEV // rows, chunk, 0)
    leave = [copy(halo_buf, halo_count_ref, sems.at[2])]
    leave[0].start()
    fetch_own.wait()
    own = own_buf[...]
    for r in range(RELS):
        sum_buf[r] = dot(count_buf[r], own)
        leave.append(copy(sum_buf.at[r], own_sum_ref.at[r], sems.at[3 + r]))
        leave[-1].start()
    fetch_w.wait()
    pre_buf[...] = dot(own, w_buf[...])
    leave.append(copy(pre_buf, pre_ref, sems.at[5]))
    leave[-1].start()
    for one in leave:
        one.wait()


def layer_body(neg_ids_ref, count_ref, halo_ref, own_sum_ref, pre_ref, w_ref, means_ref, embed_ref, picked_ref, count_buf, sum_buf, pre_buf, mean_buf, row_buf, sems):
    copy = pltpu.make_async_copy
    counts = [copy(count_ref.at[r], count_buf.at[r], sems.at[5 + r]) for r in range(RELS)]
    sums = [copy(own_sum_ref.at[r], sum_buf.at[r], sems.at[r]) for r in range(RELS)]
    first = copy(pre_ref, pre_buf, sems.at[2])
    for one in (counts[0], sums[0], counts[1], sums[1], first):
        one.start()
    halo = halo_ref[...]
    parts, leave = [], []
    for r in range(RELS):
        counts[r].wait()
        total = dot(count_buf[r], halo)
        sums[r].wait()
        mean_buf[r] = ((sum_buf[r] + total) * (1.0 / FAN)).astype(BF16)
        leave.append(copy(mean_buf.at[r], means_ref.at[r], sems.at[3 + r]))
        leave[r].start()
        parts.append(dot(mean_buf[r], w_ref[r + 1]))
    first.wait()
    preact = pre_buf[...] + parts[0] + parts[1]
    pre_buf[...] = preact
    for i in range(NEG_DEV):
        row_buf[i : i + 1, :] = pre_buf[pl.ds(neg_ids_ref[i], 1), :]
    picked_ref[...] = jnp.broadcast_to(row_buf[...][None], (CHIPS, NEG_DEV, H)).astype(BF16)
    embed_ref[...] = preact.astype(BF16)
    for one in leave:
        one.wait()


def soft_parts(x):
    small = jnp.exp(-jnp.abs(x))
    bottom = 1.0 / (1.0 + small)
    sigmoid = jnp.where(x >= 0, bottom, small * bottom)
    log_one = jnp.where(small < 1e-3, small * (1.0 - 0.5 * small), jnp.log(1.0 + small))
    return sigmoid, jnp.maximum(x, 0.0) + log_one


def largest(x):
    return jnp.max(jnp.max(jnp.abs(x), axis=0, keepdims=True), axis=1, keepdims=True)


def notes_of(values):
    lane = lax.broadcasted_iota(jnp.int32, (NEG_DEV, 128), 1)
    note = jnp.zeros((NEG_DEV, 128), F32)
    for place, value in enumerate(values):
        note = jnp.where(lane == place, value, note)
    return note


def positive_body(count_ref, embed_ref, ends_ref, features_ref, means_ref, grad_ref, note_ref, sources_ref, spread_ref, pairs_ref, sigmoid_ref, softplus_ref, own_buf, mean_buf, sems):
    fetch_own = pltpu.make_async_copy(features_ref, own_buf, sems.at[0])
    fetch_means = pltpu.make_async_copy(means_ref, mean_buf, sems.at[1])
    fetch_own.start()
    fetch_means.start()
    embed = embed_ref[...]
    scores = lax.dot_general(embed, embed, NT, preferred_element_type=F32)
    sigmoid, softplus = soft_parts(-scores)
    sigmoid_ref[...] = sigmoid
    softplus_ref[...] = softplus
    pairs_ref[...] = jnp.zeros((NODE_DEV, NODE_DEV), F32)
    node = lax.broadcasted_iota(jnp.int32, (NODE_DEV, TILE), 0)
    tiles = count_ref[0]

    def group(step, _):
        sources, targets = [], []
        for j in range(GROUP):
            t = step * GROUP + j
            source = jnp.where(t < tiles, ends_ref[t, 0:1, :], -1)
            sources.append(jnp.where(node == source, 1.0, 0.0).astype(BF16))
            targets.append(jnp.where(node == ends_ref[t, 1:2, :], 1.0, 0.0).astype(BF16))
        pairs_ref[...] += lax.dot_general(
            jnp.concatenate(sources, axis=1), jnp.concatenate(targets, axis=1), NT, preferred_element_type=F32
        )
        return 0

    lax.fori_loop(0, (tiles + (GROUP - 1)) // GROUP, group, 0)
    pairs = pairs_ref[...]
    sources = jnp.sum(pairs, axis=1, keepdims=True)
    sources_ref[...] = jnp.broadcast_to(sources, (NODE_DEV, 128))
    high, low = split_two(embed.astype(F32) * sources)
    spread_ref[:, 0:H] = high
    spread_ref[:, H:] = low
    loss = jnp.sum(jnp.sum(pairs * softplus_ref[...], axis=0, keepdims=True), axis=1, keepdims=True)
    high, low = split_two(-((pairs + pairs.T) * sigmoid_ref[...]))
    base = dot(high, embed) + dot(low, embed)
    grad_ref[...] = base
    fetch_own.wait()
    fetch_means.wait()
    widest = largest(own_buf[...].astype(F32))
    for r in range(RELS):
        widest = jnp.maximum(widest, largest(mean_buf[r].astype(F32)))
    count = tiles.astype(F32)
    known = widest * NODE_DEV * largest(base)
    note_ref[...] = notes_of((loss, count, 0.0, known, widest * TILE * count, NEG_DEV * widest, 0.0))


def scored(embed, rows, sources, spread):
    scores = lax.dot_general(embed, rows, NT, preferred_element_type=F32)
    sigmoid, softplus = soft_parts(scores)
    per_source = jnp.sum(softplus, axis=1, keepdims=True)
    loss = jnp.sum(per_source * sources, axis=0, keepdims=True) * (1.0 / NEG)
    weight = (sigmoid * (1.0 / NEG)).astype(BF16)
    parts = lax.dot_general(weight, spread, TN, preferred_element_type=F32)
    return weight, loss, parts[:, :H] + parts[:, H:]


def near_body(embed_ref, rows_ref, spread_ref, sources_ref, note_in_ref, weight_ref, part_ref, note_ref):
    rows = rows_ref[...]
    weight, loss, part = scored(embed_ref[...], rows, sources_ref[:, 0:1], spread_ref[...])
    weight_ref[...] = weight
    part_ref[...] = part.astype(part_ref.dtype)
    note = note_in_ref[...]
    lane = lax.broadcasted_iota(jnp.int32, note.shape, 1)
    tallest = largest(rows.astype(F32))
    note = jnp.where(lane == 0, note + loss, note)
    note = jnp.where(lane == 2, jnp.maximum(note, note[:, 3:4] + note[:, 4:5] * tallest), note)
    note_ref[...] = jnp.where(lane == 6, jnp.maximum(note, largest(part)), note)


def rest_body(near_weight_ref, near_rows_ref, weight_ref, rows_ref, sources_ref, base_ref, grad_ref):
    total = dot(near_weight_ref[...], near_rows_ref[...]) + dot(weight_ref[...], rows_ref[...])
    grad_ref[...] = base_ref[...] + sources_ref[:, 0:1] * total


def merge_body(part_ref, arrived_ref, own_note_ref, other_note_ref, send_ref):
    note = own_note_ref[...] + other_note_ref[...]
    first = note.astype(BF16).astype(F32)
    second = (note - first).astype(BF16).astype(F32)
    third = (note - first) - second
    lane = lax.broadcasted_iota(jnp.int32, note.shape, 1)
    note = jnp.where(lane == 3, pltpu.roll(second, 3, 1), jnp.where(lane == 4, pltpu.roll(third, 4, 1), first))
    send_ref[:, :, H:] = jnp.broadcast_to(note[None], (CHIPS, NEG_DEV, 128)).astype(BF16)
    total = part_ref[...] + arrived_ref[...].astype(F32)
    send_ref[:, :, 0:H] = total.reshape(CHIPS, NEG_DEV, H).astype(BF16)


def chosen_rows(neg_ids_ref):
    row = lax.broadcasted_iota(jnp.int32, (16, NODE_DEV), 0)
    lane = lax.broadcasted_iota(jnp.int32, (16, NODE_DEV), 1)
    chosen = jnp.zeros((16, NODE_DEV), F32)
    for i in range(NEG_DEV):
        chosen = jnp.where((row == i) & (lane == neg_ids_ref[i]), 1.0, chosen)
    return chosen.astype(BF16)


def half_at(core):
    return pl.ds(pl.multiple_of(core * HALF, HALF), HALF)


def known_body(neg_ids_ref, core_ref, grad_ref, features_ref, means_ref, own_ref, other_ref, chosen_ref):
    node = lax.broadcasted_iota(jnp.int32, (NODE_DEV, H), 0)
    grad = grad_ref[...]
    for i in range(NEG_DEV):
        grad = jnp.where(node == neg_ids_ref[i], 0.0, grad)
    pre = grad.astype(BF16)
    picks = chosen_rows(neg_ids_ref)
    swapped = core_ref[0] == 1
    for r, rows in enumerate((features_ref[...], means_ref[0], means_ref[1])):
        at = pl.ds(r * H, H)
        both = lax.dot_general(rows, pre, TN, preferred_element_type=F32)
        first, second = both[:, :HALF], both[:, HALF:]
        own_ref[at, :] = jnp.where(swapped, second, first)
        other_ref[at, :] = jnp.where(swapped, first, second)
        chosen_ref[:, at] = dot(picks, rows).astype(BF16)


def outer_body(neg_ids_ref, core_ref, arrived_ref, grad_ref, total_ref, own_ref, other_ref, note_ref, row_ref):
    total = jnp.sum(arrived_ref[...].astype(F32), axis=0)
    note_ref[...] = total[:, H:]
    total_ref[...] = total[:, :H]
    row_ref[...] = jnp.zeros((16, H), F32)
    firsts = []
    for i in range(NEG_DEV):
        first = i
        for j in reversed(range(i)):
            first = jnp.where(neg_ids_ref[j] == neg_ids_ref[i], j, first)
        firsts.append(first)
        row = grad_ref[pl.ds(neg_ids_ref[i], 1), :]
        row_ref[i : i + 1, :] = row if i == 0 else jnp.where(first == i, row, 0.0)
    for i, first in enumerate(firsts):
        row_ref[pl.ds(first, 1), :] += total_ref[i : i + 1, :]
    own_ref[...] = row_ref[:, half_at(core_ref[0])].astype(BF16)
    other_ref[...] = row_ref[:, half_at(1 - core_ref[0])].astype(BF16)


def pre_body(neg_ids_ref, total_ref, grad_ref, pre_ref, sum_ref):
    sum_ref[...] = grad_ref[...]
    for i in range(NEG_DEV):
        sum_ref[pl.ds(neg_ids_ref[i], 1), :] += total_ref[i : i + 1, :]
    pre_ref[...] = sum_ref[...].astype(BF16)


def update_body(known_ref, own_chosen_ref, other_chosen_ref, own_row_ref, other_row_ref, note_ref, out_ref, factor_ref):
    chosen = jnp.concatenate([own_chosen_ref[...], other_chosen_ref[...]], axis=0)
    rows = jnp.concatenate([own_row_ref[...], other_row_ref[...]], axis=0)
    extra = lax.dot_general(chosen, rows, TN, preferred_element_type=F32)
    known, wide, part = (note_ref[0:1, i : i + 1] for i in (2, 5, 6))
    bound = known + wide * part + TINY
    out_ref[...] = (known_ref[...] + extra) * (SPAN / bound)
    factor_ref[...] = jnp.broadcast_to(bound / SPAN / (note_ref[0:1, 1:2] * TILE), (8, HALF))


def first_half_body(core_ref, half_ref, factor_ref, note_ref, weight_ref, loss_ref):
    note = note_ref[0:1, :]
    loss_ref[...] = (note[:, 0:1] + note[:, 3:4] + note[:, 4:5]) / (note[:, 1:2] * TILE)
    weight_ref[...] = (half_ref[...] * factor_ref[0:1, :]).reshape(RELS + 1, H, HALF)


def second_half_body(core_ref, half_ref, factor_ref, note_ref, begun_ref, weight_ref):
    weight_ref[...] = (half_ref[...] * factor_ref[0:1, :]).reshape(RELS + 1, H, HALF)


def halves(body, which, extra, alias):
    whole_weight = jax.ShapeDtypeStruct((RELS + 1, H, H), F32)
    block = pl.BlockSpec((RELS + 1, H, HALF), lambda r, core: (0, 0, which(core[0])))
    scalar = pl.BlockSpec((1, 1), lambda r, core: (0, 0))
    return pl.pallas_call(
        body,
        out_shape=[whole_weight, jax.ShapeDtypeStruct((1, 1), F32)][: 1 + extra],
        grid_spec=pltpu.PrefetchScalarGridSpec(
            num_scalar_prefetch=1,
            grid=(1,),
            in_specs=[vmem(), vmem(), vmem()] + [pl.BlockSpec(memory_space=pl.ANY)] * len(alias),
            out_specs=[block, scalar][: 1 + extra],
        ),
        input_output_aliases=alias,
        compiler_params=pltpu.CompilerParams(vmem_limit_bytes=28 << 20),
    )


def on_device(features, weights, halo_send, nbr_index, tile_count, edge_ends, neg_ids):
    square = (NODE_DEV, H)
    tall = ((RELS + 1) * H, HALF)
    core = lax.axis_index(NEAR).astype(jnp.int32).reshape(1)
    core, halo_send = lax.optimization_barrier((core, halo_send))
    (outgoing,) = call(halo_body, [hbm((N_DOM, HALO_PEER, H), BF16)], [FROM_HBM, FROM_HBM], (), (halo_send[0].T, features))
    incoming = swap(outgoing, DOM)
    neighbours = nbr_index.reshape(NODE_DEV, RELS * FAN)
    two = (RELS, *square)
    halo_count, own_sum, pre = call(
        counts_body,
        [(two, BF16, BY_HAND), (two, F32, BY_HAND), (square, F32, BY_HAND)],
        [BY_HAND, BY_HAND, vmem()],
        [pltpu.VMEM(square, BF16)] * 2 + [pltpu.VMEM(two, BF16)] * 2 + [pltpu.VMEM(two, F32), pltpu.VMEM(square, F32), pltpu.SemaphoreType.DMA((6,))],
        (features, weights, neighbours),
    )
    means, embed, picked = call(
        layer_body,
        [(two, BF16, BY_HAND), (square, BF16), hbm((CHIPS, NEG_DEV, H), BF16)],
        [smem(), BY_HAND, vmem(), BY_HAND, BY_HAND, vmem()],
        [pltpu.VMEM(two, BF16), pltpu.VMEM(two, F32), pltpu.VMEM(square, F32), pltpu.VMEM(two, BF16), pltpu.VMEM((NEG_DEV, H), F32), pltpu.SemaphoreType.DMA((7,))],
        (neg_ids, halo_count, incoming.reshape(512, H), own_sum, pre, weights),
    )
    near_rows = swap(picked, FAR).reshape(square)
    base, note, sources, spread = call(
        positive_body,
        [hbm(square, F32), ((8, 128), F32), ((NODE_DEV, 128), F32), ((NODE_DEV, 2 * H), BF16)],
        [smem(), vmem(), FROM_HBM, BY_HAND, BY_HAND],
        [pltpu.VMEM(square, F32)] * 3 + [pltpu.VMEM(square, BF16), pltpu.VMEM(two, BF16), pltpu.SemaphoreType.DMA((2,))],
        (tile_count, embed, edge_ends, features, means),
    )
    near_rows, note = lax.optimization_barrier((near_rows, note))
    other_rows = core_swap(near_rows)
    near_weight, near_part, note = call(
        near_body,
        [(square, BF16), (square, F32), ((8, 128), F32)],
        [vmem()] * 5,
        (),
        (embed, near_rows, spread, sources, note),
    )
    weight, other_part, note = call(
        near_body,
        [(square, BF16), (square, BF16), ((8, 128), F32)],
        [vmem()] * 5,
        (),
        (embed, other_rows, spread, sources, note),
    )
    other_note = core_swap(note)
    part_arrived = core_swap(other_part)
    (grad,) = call(
        rest_body,
        [(square, F32)],
        [vmem()] * 5 + [FROM_HBM],
        (),
        (near_weight, near_rows, weight, other_rows, sources, base),
    )
    part_arrived, grad = lax.optimization_barrier((part_arrived, grad))
    (outgoing_grad,) = call(
        merge_body,
        [((CHIPS, NEG_DEV, H + 128), BF16)],
        [vmem()] * 4,
        (),
        (near_part, part_arrived, note, other_note),
    )
    outgoing_grad, grad = lax.optimization_barrier((outgoing_grad, grad))
    arrived = swap(outgoing_grad, FAR)
    known_own, known_other, chosen = call(
        known_body,
        [(tall, F32), (tall, F32), ((16, (RELS + 1) * H), BF16)],
        [smem(), smem(), vmem(), FROM_HBM, FROM_HBM],
        (),
        (neg_ids, core, grad, features, means),
    )
    other_chosen = core_swap(chosen)
    known = known_own + core_swap(known_other)
    arrived, known, other_chosen = lax.optimization_barrier((arrived, known, other_chosen))
    total, own_row, send_row, note = call(
        outer_body,
        [((NEG_DEV, H), F32), ((16, HALF), BF16), ((16, HALF), BF16), ((NEG_DEV, 128), F32)],
        [smem(), smem(), vmem(), vmem()],
        [pltpu.VMEM((16, H), F32)],
        (neg_ids, core, arrived, grad),
    )
    other_row = core_swap(send_row)
    (pre_grad,) = call(
        pre_body,
        [hbm(square, BF16)],
        [smem(), vmem(), vmem()],
        [pltpu.VMEM(square, F32)],
        (neg_ids, total, grad),
    )
    partial, factor = call(
        update_body,
        [(tall, F32), ((8, HALF), F32)],
        [vmem()] * 6,
        (),
        (known, chosen, other_chosen, own_row, other_row, note),
    )
    chunks = (CHIPS, 24, HALF)
    sums = swap(partial.astype(F16).reshape(chunks), FAR)
    mine = jnp.sum(sums.astype(F32), axis=0).astype(F16)
    half = swap(jnp.broadcast_to(mine, chunks), FAR).reshape(tall)
    other_half = core_swap(half).astype(F32)
    half = half.astype(F32)
    close = near_memory(factor), near_memory(note)
    begun, mean_loss = halves(first_half_body, lambda c: c, 1, {})(core, near_memory(half), *close)
    (begun, other_half) = lax.optimization_barrier((begun, other_half))
    (weight_grad,) = halves(second_half_body, lambda c: 1 - c, 0, {4: 0})(core, near_memory(other_half), *close, begun)
    return weight_grad, mean_loss.reshape(()), pre_grad


def solution(mesh):
    torus = Mesh(mesh.devices.reshape(4, 4, 4, 2), DOM)
    in_specs = (
        P(DOM, None),
        P(),
        P(DOM, None, None),
        P(DOM, None, None),
        P(DOM),
        P(DOM, None, None),
        P(DOM),
    )
    out_specs = (P(), P(), P(DOM, None))
    return jax.shard_map(on_device, mesh=torus, in_specs=in_specs, out_specs=out_specs, check_vma=False)
```

```python
import jax
import jax.numpy as jnp
from jax import lax
from jax.experimental import pallas as pl
from jax.experimental.pallas import tpu as pltpu
from jax.sharding import Mesh
from jax.sharding import PartitionSpec as P

DOM = ("dom_0", "dom_1", "dom_2", "dom_3")
FAR = ("dom_0", "dom_1", "dom_2")
NEAR = ("dom_3",)
H = 512
RELS = 2
FAN = 8
TILE = 256
NODE_DEV = 512
NEG = 1024
NEG_DEV = 8
N_DOM = 128
HALO_PEER = 4
CHIPS = 64
GROUP = 4
HALF = 256
F32 = jnp.float32
BF16 = jnp.bfloat16
F16 = jnp.float16
SPAN = 60000.0
TINY = 1e-30
NT = (((1,), (1,)), ((), ()))
TN = (((0,), (0,)), ((), ()))
FROM_HBM = "hbm"
BY_HAND = "by_hand"


def swap(x, axes):
    return lax.all_to_all(x, axes, split_axis=0, concat_axis=0, tiled=True)


def core_swap(x):
    return lax.ppermute(x, "dom_3", [(0, 1), (1, 0)])


def dot(a, b):
    return jnp.dot(a, b, preferred_element_type=F32)


def split_two(x):
    high = x.astype(BF16)
    return high, (x - high.astype(F32)).astype(BF16)


def vmem():
    return pl.BlockSpec(memory_space=pltpu.VMEM)


def whole(shape):
    return pl.BlockSpec(shape, lambda i: (0,) * len(shape))


def smem():
    return pl.BlockSpec(memory_space=pltpu.SMEM)


def near_memory(x):
    return pltpu.with_memory_space_constraint(x, pltpu.VMEM)


def hbm(shape, kind):
    return pltpu.HBM(shape, kind)


def call(body, outs, specs, scratch=(), args=()):
    given, ins, made, back = [], [], [], []
    for spec, x in zip(specs, args):
        if spec is FROM_HBM or spec is BY_HAND:
            x = pltpu.with_memory_space_constraint(x, pltpu.HBM)
            spec = whole(x.shape) if spec is FROM_HBM else pl.BlockSpec(memory_space=pl.ANY)
        elif spec.memory_space == pltpu.VMEM and x.dtype != jnp.int32:
            x = near_memory(x)
        given.append(x)
        ins.append(spec)
    for o in outs:
        if isinstance(o, tuple) and len(o) == 3:
            made.append(hbm(*o[:2]))
            back.append(pl.BlockSpec(memory_space=pl.ANY))
        elif isinstance(o, tuple):
            made.append(pltpu.VMEM(*o))
            back.append(vmem())
        else:
            made.append(o)
            back.append(whole(o.shape))
    return pl.pallas_call(
        body,
        out_shape=made,
        grid=(1,),
        in_specs=ins,
        out_specs=back,
        scratch_shapes=list(scratch),
        compiler_params=pltpu.CompilerParams(vmem_limit_bytes=28 << 20),
    )(*given)


def halo_body(send_ref, features_ref, out_ref):
    node = lax.broadcasted_iota(jnp.int32, (NODE_DEV, N_DOM), 0)
    own = features_ref[...]
    for k in range(HALO_PEER):
        hit = jnp.where(node == send_ref[k : k + 1, :], 1.0, 0.0).astype(BF16)
        out_ref[:, k, :] = lax.dot_general(hit, own, TN, preferred_element_type=F32).astype(BF16)


def counts_body(features_ref, w_ref, nbr_ref, halo_count_ref, own_sum_ref, pre_ref, own_buf, w_buf, halo_buf, count_buf, sum_buf, pre_buf, sems):
    copy = pltpu.make_async_copy
    fetch_own = copy(features_ref, own_buf, sems.at[0])
    fetch_w = copy(w_ref.at[0], w_buf, sems.at[1])
    fetch_own.start()
    fetch_w.start()
    rows = 32
    lanes = lax.broadcasted_iota(jnp.int32, (rows, NODE_DEV), 1)

    def chunk(step, _):
        at = pl.ds(pl.multiple_of(step * rows, rows), rows)
        for r in range(RELS):
            index = nbr_ref[at, r * FAN : (r + 1) * FAN]
            for half in range(2):
                total = jnp.zeros((rows, NODE_DEV), F32)
                for k in range(FAN):
                    hit = lanes == (index[:, k : k + 1] - half * NODE_DEV)
                    total = total + jnp.where(hit, 1.0, 0.0)
                if half == 0:
                    count_buf[r, at, :] = total.astype(BF16)
                else:
                    halo_buf[r, at, :] = total.astype(BF16)
        return 0

    lax.fori_loop(0, NODE_DEV // rows, chunk, 0)
    leave = [copy(halo_buf, halo_count_ref, sems.at[2])]
    leave[0].start()
    fetch_own.wait()
    own = own_buf[...]
    for r in range(RELS):
        sum_buf[r] = dot(count_buf[r], own)
        leave.append(copy(sum_buf.at[r], own_sum_ref.at[r], sems.at[3 + r]))
        leave[-1].start()
    fetch_w.wait()
    pre_buf[...] = dot(own, w_buf[...])
    leave.append(copy(pre_buf, pre_ref, sems.at[5]))
    leave[-1].start()
    for one in leave:
        one.wait()


def layer_body(neg_ids_ref, count_ref, halo_ref, own_sum_ref, pre_ref, w_ref, means_ref, embed_ref, picked_ref, pre_buf, mean_buf, row_buf, sems):
    halo = halo_ref[...]
    preact = pre_ref[...]
    for r in range(RELS):
        total = own_sum_ref[r] + dot(count_ref[r], halo)
        mean = (total * (1.0 / FAN)).astype(BF16)
        mean_buf[r] = mean
        preact = preact + dot(mean, w_ref[r + 1])
    leave = [pltpu.make_async_copy(mean_buf.at[r], means_ref.at[r], sems.at[r]) for r in range(RELS)]
    for one in leave:
        one.start()
    pre_buf[...] = preact
    for i in range(NEG_DEV):
        row_buf[i : i + 1, :] = pre_buf[pl.ds(neg_ids_ref[i], 1), :]
    picked_ref[...] = jnp.broadcast_to(row_buf[...][None], (CHIPS, NEG_DEV, H)).astype(BF16)
    embed_ref[...] = preact.astype(BF16)
    for one in leave:
        one.wait()


def soft_parts(x):
    small = jnp.exp(-jnp.abs(x))
    bottom = 1.0 / (1.0 + small)
    sigmoid = jnp.where(x >= 0, bottom, small * bottom)
    log_one = jnp.where(small < 1e-3, small * (1.0 - 0.5 * small), jnp.log(1.0 + small))
    return sigmoid, jnp.maximum(x, 0.0) + log_one


def largest(x):
    return jnp.max(jnp.max(jnp.abs(x), axis=0, keepdims=True), axis=1, keepdims=True)


def notes_of(values):
    lane = lax.broadcasted_iota(jnp.int32, (NEG_DEV, 128), 1)
    note = jnp.zeros((NEG_DEV, 128), F32)
    for place, value in enumerate(values):
        note = jnp.where(lane == place, value, note)
    return note


def positive_body(count_ref, embed_ref, ends_ref, features_ref, means_ref, grad_ref, note_ref, sources_ref, spread_ref, pairs_ref, sigmoid_ref, softplus_ref, own_buf, mean_buf, sems):
    fetch_own = pltpu.make_async_copy(features_ref, own_buf, sems.at[0])
    fetch_means = pltpu.make_async_copy(means_ref, mean_buf, sems.at[1])
    fetch_own.start()
    fetch_means.start()
    embed = embed_ref[...]
    scores = lax.dot_general(embed, embed, NT, preferred_element_type=F32)
    sigmoid, softplus = soft_parts(-scores)
    sigmoid_ref[...] = sigmoid
    softplus_ref[...] = softplus
    pairs_ref[...] = jnp.zeros((NODE_DEV, NODE_DEV), F32)
    node = lax.broadcasted_iota(jnp.int32, (NODE_DEV, TILE), 0)
    tiles = count_ref[0]

    def group(step, _):
        sources, targets = [], []
        for j in range(GROUP):
            t = step * GROUP + j
            source = jnp.where(t < tiles, ends_ref[t, 0:1, :], -1)
            sources.append(jnp.where(node == source, 1.0, 0.0).astype(BF16))
            targets.append(jnp.where(node == ends_ref[t, 1:2, :], 1.0, 0.0).astype(BF16))
        pairs_ref[...] += lax.dot_general(
            jnp.concatenate(sources, axis=1), jnp.concatenate(targets, axis=1), NT, preferred_element_type=F32
        )
        return 0

    lax.fori_loop(0, (tiles + (GROUP - 1)) // GROUP, group, 0)
    pairs = pairs_ref[...]
    sources = jnp.sum(pairs, axis=1, keepdims=True)
    sources_ref[...] = jnp.broadcast_to(sources, (NODE_DEV, 128))
    high, low = split_two(embed.astype(F32) * sources)
    spread_ref[:, 0:H] = high
    spread_ref[:, H:] = low
    loss = jnp.sum(jnp.sum(pairs * softplus_ref[...], axis=0, keepdims=True), axis=1, keepdims=True)
    high, low = split_two(-((pairs + pairs.T) * sigmoid_ref[...]))
    base = dot(high, embed) + dot(low, embed)
    grad_ref[...] = base
    fetch_own.wait()
    fetch_means.wait()
    widest = largest(own_buf[...].astype(F32))
    for r in range(RELS):
        widest = jnp.maximum(widest, largest(mean_buf[r].astype(F32)))
    count = tiles.astype(F32)
    known = widest * NODE_DEV * largest(base)
    note_ref[...] = notes_of((loss, count, 0.0, known, widest * TILE * count, NEG_DEV * widest, 0.0))


def scored(embed, rows, sources, spread):
    scores = lax.dot_general(embed, rows, NT, preferred_element_type=F32)
    sigmoid, softplus = soft_parts(scores)
    per_source = jnp.sum(softplus, axis=1, keepdims=True)
    loss = jnp.sum(per_source * sources, axis=0, keepdims=True) * (1.0 / NEG)
    weight = (sigmoid * (1.0 / NEG)).astype(BF16)
    parts = lax.dot_general(weight, spread, TN, preferred_element_type=F32)
    return weight, loss, parts[:, :H] + parts[:, H:]


def near_body(embed_ref, rows_ref, spread_ref, sources_ref, note_in_ref, weight_ref, part_ref, note_ref):
    rows = rows_ref[...]
    weight, loss, part = scored(embed_ref[...], rows, sources_ref[:, 0:1], spread_ref[...])
    weight_ref[...] = weight
    part_ref[...] = part.astype(part_ref.dtype)
    note = note_in_ref[...]
    lane = lax.broadcasted_iota(jnp.int32, note.shape, 1)
    tallest = largest(rows.astype(F32))
    note = jnp.where(lane == 0, note + loss, note)
    note = jnp.where(lane == 2, jnp.maximum(note, note[:, 3:4] + note[:, 4:5] * tallest), note)
    note_ref[...] = jnp.where(lane == 6, jnp.maximum(note, largest(part)), note)


def rest_body(near_weight_ref, near_rows_ref, weight_ref, rows_ref, sources_ref, base_ref, grad_ref):
    total = dot(near_weight_ref[...], near_rows_ref[...]) + dot(weight_ref[...], rows_ref[...])
    grad_ref[...] = base_ref[...] + sources_ref[:, 0:1] * total


def merge_body(part_ref, arrived_ref, own_note_ref, other_note_ref, send_ref):
    note = own_note_ref[...] + other_note_ref[...]
    first = note.astype(BF16).astype(F32)
    second = (note - first).astype(BF16).astype(F32)
    third = (note - first) - second
    lane = lax.broadcasted_iota(jnp.int32, note.shape, 1)
    note = jnp.where(lane == 3, pltpu.roll(second, 3, 1), jnp.where(lane == 4, pltpu.roll(third, 4, 1), first))
    send_ref[:, :, H:] = jnp.broadcast_to(note[None], (CHIPS, NEG_DEV, 128)).astype(BF16)
    total = part_ref[...] + arrived_ref[...].astype(F32)
    send_ref[:, :, 0:H] = total.reshape(CHIPS, NEG_DEV, H).astype(BF16)


def chosen_rows(neg_ids_ref):
    row = lax.broadcasted_iota(jnp.int32, (16, NODE_DEV), 0)
    lane = lax.broadcasted_iota(jnp.int32, (16, NODE_DEV), 1)
    chosen = jnp.zeros((16, NODE_DEV), F32)
    for i in range(NEG_DEV):
        chosen = jnp.where((row == i) & (lane == neg_ids_ref[i]), 1.0, chosen)
    return chosen.astype(BF16)


def half_at(core):
    return pl.ds(pl.multiple_of(core * HALF, HALF), HALF)


def known_body(neg_ids_ref, core_ref, grad_ref, features_ref, means_ref, own_ref, other_ref, chosen_ref):
    node = lax.broadcasted_iota(jnp.int32, (NODE_DEV, H), 0)
    grad = grad_ref[...]
    for i in range(NEG_DEV):
        grad = jnp.where(node == neg_ids_ref[i], 0.0, grad)
    pre = grad.astype(BF16)
    picks = chosen_rows(neg_ids_ref)
    swapped = core_ref[0] == 1
    for r, rows in enumerate((features_ref[...], means_ref[0], means_ref[1])):
        at = pl.ds(r * H, H)
        both = lax.dot_general(rows, pre, TN, preferred_element_type=F32)
        first, second = both[:, :HALF], both[:, HALF:]
        own_ref[at, :] = jnp.where(swapped, second, first)
        other_ref[at, :] = jnp.where(swapped, first, second)
        chosen_ref[:, at] = dot(picks, rows).astype(BF16)


def outer_body(neg_ids_ref, core_ref, arrived_ref, grad_ref, total_ref, own_ref, other_ref, note_ref, row_ref):
    total = jnp.sum(arrived_ref[...].astype(F32), axis=0)
    note_ref[...] = total[:, H:]
    total_ref[...] = total[:, :H]
    row_ref[...] = jnp.zeros((16, H), F32)
    firsts = []
    for i in range(NEG_DEV):
        first = i
        for j in reversed(range(i)):
            first = jnp.where(neg_ids_ref[j] == neg_ids_ref[i], j, first)
        firsts.append(first)
        row = grad_ref[pl.ds(neg_ids_ref[i], 1), :]
        row_ref[i : i + 1, :] = row if i == 0 else jnp.where(first == i, row, 0.0)
    for i, first in enumerate(firsts):
        row_ref[pl.ds(first, 1), :] += total_ref[i : i + 1, :]
    own_ref[...] = row_ref[:, half_at(core_ref[0])].astype(BF16)
    other_ref[...] = row_ref[:, half_at(1 - core_ref[0])].astype(BF16)


def pre_body(neg_ids_ref, total_ref, grad_ref, pre_ref, sum_ref):
    sum_ref[...] = grad_ref[...]
    for i in range(NEG_DEV):
        sum_ref[pl.ds(neg_ids_ref[i], 1), :] += total_ref[i : i + 1, :]
    pre_ref[...] = sum_ref[...].astype(BF16)


def update_body(known_ref, own_chosen_ref, other_chosen_ref, own_row_ref, other_row_ref, note_ref, out_ref, factor_ref):
    chosen = jnp.concatenate([own_chosen_ref[...], other_chosen_ref[...]], axis=0)
    rows = jnp.concatenate([own_row_ref[...], other_row_ref[...]], axis=0)
    extra = lax.dot_general(chosen, rows, TN, preferred_element_type=F32)
    known, wide, part = (note_ref[0:1, i : i + 1] for i in (2, 5, 6))
    bound = known + wide * part + TINY
    out_ref[...] = (known_ref[...] + extra) * (SPAN / bound)
    factor_ref[...] = jnp.broadcast_to(bound / SPAN / (note_ref[0:1, 1:2] * TILE), (8, HALF))


def first_half_body(core_ref, half_ref, factor_ref, note_ref, weight_ref, loss_ref):
    note = note_ref[0:1, :]
    loss_ref[...] = (note[:, 0:1] + note[:, 3:4] + note[:, 4:5]) / (note[:, 1:2] * TILE)
    weight_ref[...] = (half_ref[...] * factor_ref[0:1, :]).reshape(RELS + 1, H, HALF)


def second_half_body(core_ref, half_ref, factor_ref, note_ref, begun_ref, weight_ref):
    weight_ref[...] = (half_ref[...] * factor_ref[0:1, :]).reshape(RELS + 1, H, HALF)


def halves(body, which, extra, alias):
    whole_weight = jax.ShapeDtypeStruct((RELS + 1, H, H), F32)
    block = pl.BlockSpec((RELS + 1, H, HALF), lambda r, core: (0, 0, which(core[0])))
    scalar = pl.BlockSpec((1, 1), lambda r, core: (0, 0))
    return pl.pallas_call(
        body,
        out_shape=[whole_weight, jax.ShapeDtypeStruct((1, 1), F32)][: 1 + extra],
        grid_spec=pltpu.PrefetchScalarGridSpec(
            num_scalar_prefetch=1,
            grid=(1,),
            in_specs=[vmem(), vmem(), vmem()] + [pl.BlockSpec(memory_space=pl.ANY)] * len(alias),
            out_specs=[block, scalar][: 1 + extra],
        ),
        input_output_aliases=alias,
        compiler_params=pltpu.CompilerParams(vmem_limit_bytes=28 << 20),
    )


def on_device(features, weights, halo_send, nbr_index, tile_count, edge_ends, neg_ids):
    square = (NODE_DEV, H)
    tall = ((RELS + 1) * H, HALF)
    core = lax.axis_index(NEAR).astype(jnp.int32).reshape(1)
    core, halo_send = lax.optimization_barrier((core, halo_send))
    (outgoing,) = call(halo_body, [hbm((N_DOM, HALO_PEER, H), BF16)], [FROM_HBM, FROM_HBM], (), (halo_send[0].T, features))
    incoming = swap(outgoing, DOM)
    neighbours = nbr_index.reshape(NODE_DEV, RELS * FAN)
    two = (RELS, *square)
    halo_count, own_sum, pre = call(
        counts_body,
        [(two, BF16, BY_HAND), (two, F32, BY_HAND), (square, F32, BY_HAND)],
        [BY_HAND, BY_HAND, vmem()],
        [pltpu.VMEM(square, BF16)] * 2 + [pltpu.VMEM(two, BF16)] * 2 + [pltpu.VMEM(two, F32), pltpu.VMEM(square, F32), pltpu.SemaphoreType.DMA((6,))],
        (features, weights, neighbours),
    )
    means, embed, picked = call(
        layer_body,
        [(two, BF16, BY_HAND), (square, BF16), hbm((CHIPS, NEG_DEV, H), BF16)],
        [smem(), FROM_HBM, vmem(), FROM_HBM, FROM_HBM, vmem()],
        [pltpu.VMEM(square, F32), pltpu.VMEM(two, BF16), pltpu.VMEM((NEG_DEV, H), F32), pltpu.SemaphoreType.DMA((RELS,))],
        (neg_ids, halo_count, incoming.reshape(512, H), own_sum, pre, weights),
    )
    near_rows = swap(picked, FAR).reshape(square)
    base, note, sources, spread = call(
        positive_body,
        [hbm(square, F32), ((8, 128), F32), ((NODE_DEV, 128), F32), ((NODE_DEV, 2 * H), BF16)],
        [smem(), vmem(), FROM_HBM, BY_HAND, BY_HAND],
        [pltpu.VMEM(square, F32)] * 3 + [pltpu.VMEM(square, BF16), pltpu.VMEM(two, BF16), pltpu.SemaphoreType.DMA((2,))],
        (tile_count, embed, edge_ends, features, means),
    )
    near_rows, note = lax.optimization_barrier((near_rows, note))
    other_rows = core_swap(near_rows)
    near_weight, near_part, note = call(
        near_body,
        [(square, BF16), (square, F32), ((8, 128), F32)],
        [vmem()] * 5,
        (),
        (embed, near_rows, spread, sources, note),
    )
    weight, other_part, note = call(
        near_body,
        [(square, BF16), (square, BF16), ((8, 128), F32)],
        [vmem()] * 5,
        (),
        (embed, other_rows, spread, sources, note),
    )
    other_note = core_swap(note)
    part_arrived = core_swap(other_part)
    (grad,) = call(
        rest_body,
        [(square, F32)],
        [vmem()] * 5 + [FROM_HBM],
        (),
        (near_weight, near_rows, weight, other_rows, sources, base),
    )
    part_arrived, grad = lax.optimization_barrier((part_arrived, grad))
    (outgoing_grad,) = call(
        merge_body,
        [((CHIPS, NEG_DEV, H + 128), BF16)],
        [vmem()] * 4,
        (),
        (near_part, part_arrived, note, other_note),
    )
    outgoing_grad, grad = lax.optimization_barrier((outgoing_grad, grad))
    arrived = swap(outgoing_grad, FAR)
    known_own, known_other, chosen = call(
        known_body,
        [(tall, F32), (tall, F32), ((16, (RELS + 1) * H), BF16)],
        [smem(), smem(), vmem(), FROM_HBM, FROM_HBM],
        (),
        (neg_ids, core, grad, features, means),
    )
    other_chosen = core_swap(chosen)
    known = known_own + core_swap(known_other)
    arrived, known, other_chosen = lax.optimization_barrier((arrived, known, other_chosen))
    total, own_row, send_row, note = call(
        outer_body,
        [((NEG_DEV, H), F32), ((16, HALF), BF16), ((16, HALF), BF16), ((NEG_DEV, 128), F32)],
        [smem(), smem(), vmem(), vmem()],
        [pltpu.VMEM((16, H), F32)],
        (neg_ids, core, arrived, grad),
    )
    other_row = core_swap(send_row)
    (pre_grad,) = call(
        pre_body,
        [hbm(square, BF16)],
        [smem(), vmem(), vmem()],
        [pltpu.VMEM(square, F32)],
        (neg_ids, total, grad),
    )
    partial, factor = call(
        update_body,
        [(tall, F32), ((8, HALF), F32)],
        [vmem()] * 6,
        (),
        (known, chosen, other_chosen, own_row, other_row, note),
    )
    chunks = (CHIPS, 24, HALF)
    sums = swap(partial.astype(F16).reshape(chunks), FAR)
    mine = jnp.sum(sums.astype(F32), axis=0).astype(F16)
    half = swap(jnp.broadcast_to(mine, chunks), FAR).reshape(tall)
    other_half = core_swap(half).astype(F32)
    half = half.astype(F32)
    close = near_memory(factor), near_memory(note)
    begun, mean_loss = halves(first_half_body, lambda c: c, 1, {})(core, near_memory(half), *close)
    (begun, other_half) = lax.optimization_barrier((begun, other_half))
    (weight_grad,) = halves(second_half_body, lambda c: 1 - c, 0, {4: 0})(core, near_memory(other_half), *close, begun)
    return weight_grad, mean_loss.reshape(()), pre_grad


def solution(mesh):
    torus = Mesh(mesh.devices.reshape(4, 4, 4, 2), DOM)
    in_specs = (
        P(DOM, None),
        P(),
        P(DOM, None, None),
        P(DOM, None, None),
        P(DOM),
        P(DOM, None, None),
        P(DOM),
    )
    out_specs = (P(), P(), P(DOM, None))
    return jax.shard_map(on_device, mesh=torus, in_specs=in_specs, out_specs=out_specs, check_vma=False)
```

```python
import jax
import jax.numpy as jnp
from jax import lax
from jax.experimental import pallas as pl
from jax.experimental.pallas import tpu as pltpu
from jax.sharding import Mesh
from jax.sharding import PartitionSpec as P

DOM = ("dom_0", "dom_1", "dom_2", "dom_3")
FAR = ("dom_0", "dom_1", "dom_2")
NEAR = ("dom_3",)
H = 512
RELS = 2
FAN = 8
TILE = 256
NODE_DEV = 512
NEG = 1024
NEG_DEV = 8
N_DOM = 128
HALO_PEER = 4
CHIPS = 64
GROUP = 4
HALF = 256
F32 = jnp.float32
BF16 = jnp.bfloat16
F16 = jnp.float16
SPAN = 60000.0
TINY = 1e-30
NT = (((1,), (1,)), ((), ()))
TN = (((0,), (0,)), ((), ()))
FROM_HBM = "hbm"
BY_HAND = "by_hand"


def swap(x, axes):
    return lax.all_to_all(x, axes, split_axis=0, concat_axis=0, tiled=True)


def core_swap(x):
    return lax.ppermute(x, "dom_3", [(0, 1), (1, 0)])


def dot(a, b):
    return jnp.dot(a, b, preferred_element_type=F32)


def split_two(x):
    high = x.astype(BF16)
    return high, (x - high.astype(F32)).astype(BF16)


def vmem():
    return pl.BlockSpec(memory_space=pltpu.VMEM)


def whole(shape):
    return pl.BlockSpec(shape, lambda i: (0,) * len(shape))


def smem():
    return pl.BlockSpec(memory_space=pltpu.SMEM)


def near_memory(x):
    return pltpu.with_memory_space_constraint(x, pltpu.VMEM)


def hbm(shape, kind):
    return pltpu.HBM(shape, kind)


def call(body, outs, specs, scratch=(), args=()):
    given, ins, made, back = [], [], [], []
    for spec, x in zip(specs, args):
        if spec is FROM_HBM or spec is BY_HAND:
            x = pltpu.with_memory_space_constraint(x, pltpu.HBM)
            spec = whole(x.shape) if spec is FROM_HBM else pl.BlockSpec(memory_space=pl.ANY)
        elif spec.memory_space == pltpu.VMEM and x.dtype != jnp.int32:
            x = near_memory(x)
        given.append(x)
        ins.append(spec)
    for o in outs:
        if isinstance(o, tuple) and len(o) == 3:
            made.append(hbm(*o[:2]))
            back.append(pl.BlockSpec(memory_space=pl.ANY))
        elif isinstance(o, tuple):
            made.append(pltpu.VMEM(*o))
            back.append(vmem())
        else:
            made.append(o)
            back.append(whole(o.shape))
    return pl.pallas_call(
        body,
        out_shape=made,
        grid=(1,),
        in_specs=ins,
        out_specs=back,
        scratch_shapes=list(scratch),
        compiler_params=pltpu.CompilerParams(vmem_limit_bytes=28 << 20),
    )(*given)


def halo_body(send_ref, features_ref, out_ref):
    node = lax.broadcasted_iota(jnp.int32, (NODE_DEV, N_DOM), 0)
    own = features_ref[...]
    for k in range(HALO_PEER):
        hit = jnp.where(node == send_ref[k : k + 1, :], 1.0, 0.0).astype(BF16)
        out_ref[:, k, :] = lax.dot_general(hit, own, TN, preferred_element_type=F32).astype(BF16)


def counts_body(features_ref, w_ref, nbr_ref, halo_count_ref, own_sum_ref, pre_ref, own_buf, w_buf, halo_buf, count_buf, sum_buf, pre_buf, sems):
    copy = pltpu.make_async_copy
    fetch_own = copy(features_ref, own_buf, sems.at[0])
    fetch_w = copy(w_ref.at[0], w_buf, sems.at[1])
    fetch_own.start()
    fetch_w.start()
    rows = 32
    lanes = lax.broadcasted_iota(jnp.int32, (rows, NODE_DEV), 1)

    def chunk(step, _):
        at = pl.ds(pl.multiple_of(step * rows, rows), rows)
        for r in range(RELS):
            index = nbr_ref[at, r * FAN : (r + 1) * FAN]
            for half in range(2):
                total = jnp.zeros((rows, NODE_DEV), F32)
                for k in range(FAN):
                    hit = lanes == (index[:, k : k + 1] - half * NODE_DEV)
                    total = total + jnp.where(hit, 1.0, 0.0)
                if half == 0:
                    count_buf[r, at, :] = total.astype(BF16)
                else:
                    halo_buf[r, at, :] = total.astype(BF16)
        return 0

    lax.fori_loop(0, NODE_DEV // rows, chunk, 0)
    leave = [copy(halo_buf, halo_count_ref, sems.at[2])]
    leave[0].start()
    fetch_own.wait()
    own = own_buf[...]
    for r in range(RELS):
        sum_buf[r] = dot(count_buf[r], own)
        leave.append(copy(sum_buf.at[r], own_sum_ref.at[r], sems.at[3 + r]))
        leave[-1].start()
    fetch_w.wait()
    pre_buf[...] = dot(own, w_buf[...])
    leave.append(copy(pre_buf, pre_ref, sems.at[5]))
    leave[-1].start()
    for one in leave:
        one.wait()


def layer_body(neg_ids_ref, count_ref, halo_ref, own_sum_ref, pre_ref, w_ref, means_ref, embed_ref, picked_ref):
    halo = halo_ref[...]
    preact = pre_ref[...]
    for r in range(RELS):
        total = own_sum_ref[r] + dot(count_ref[r], halo)
        mean = (total * (1.0 / FAN)).astype(BF16)
        means_ref[r] = mean
        preact = preact + dot(mean, w_ref[r + 1])
    embed = preact.astype(BF16)
    embed_ref[...] = embed
    picked = dot(chosen_rows(neg_ids_ref), embed)[:NEG_DEV]
    picked_ref[...] = jnp.broadcast_to(picked[None], (CHIPS, NEG_DEV, H)).astype(BF16)


def soft_parts(x):
    small = jnp.exp(-jnp.abs(x))
    bottom = 1.0 / (1.0 + small)
    sigmoid = jnp.where(x >= 0, bottom, small * bottom)
    log_one = jnp.where(small < 1e-3, small * (1.0 - 0.5 * small), jnp.log(1.0 + small))
    return sigmoid, jnp.maximum(x, 0.0) + log_one


def largest(x):
    return jnp.max(jnp.max(jnp.abs(x), axis=0, keepdims=True), axis=1, keepdims=True)


def notes_of(values):
    lane = lax.broadcasted_iota(jnp.int32, (NEG_DEV, 128), 1)
    note = jnp.zeros((NEG_DEV, 128), F32)
    for place, value in enumerate(values):
        note = jnp.where(lane == place, value, note)
    return note


def positive_body(count_ref, embed_ref, ends_ref, features_ref, means_ref, grad_ref, note_ref, sources_ref, spread_ref, pairs_ref, sigmoid_ref, softplus_ref, own_buf, mean_buf, sems):
    fetch_own = pltpu.make_async_copy(features_ref, own_buf, sems.at[0])
    fetch_means = pltpu.make_async_copy(means_ref, mean_buf, sems.at[1])
    fetch_own.start()
    fetch_means.start()
    embed = embed_ref[...]
    scores = lax.dot_general(embed, embed, NT, preferred_element_type=F32)
    sigmoid, softplus = soft_parts(-scores)
    sigmoid_ref[...] = sigmoid
    softplus_ref[...] = softplus
    pairs_ref[...] = jnp.zeros((NODE_DEV, NODE_DEV), F32)
    node = lax.broadcasted_iota(jnp.int32, (NODE_DEV, TILE), 0)
    tiles = count_ref[0]

    def group(step, _):
        sources, targets = [], []
        for j in range(GROUP):
            t = step * GROUP + j
            source = jnp.where(t < tiles, ends_ref[t, 0:1, :], -1)
            sources.append(jnp.where(node == source, 1.0, 0.0).astype(BF16))
            targets.append(jnp.where(node == ends_ref[t, 1:2, :], 1.0, 0.0).astype(BF16))
        pairs_ref[...] += lax.dot_general(
            jnp.concatenate(sources, axis=1), jnp.concatenate(targets, axis=1), NT, preferred_element_type=F32
        )
        return 0

    lax.fori_loop(0, (tiles + (GROUP - 1)) // GROUP, group, 0)
    pairs = pairs_ref[...]
    sources = jnp.sum(pairs, axis=1, keepdims=True)
    sources_ref[...] = jnp.broadcast_to(sources, (NODE_DEV, 128))
    high, low = split_two(embed.astype(F32) * sources)
    spread_ref[:, 0:H] = high
    spread_ref[:, H:] = low
    loss = jnp.sum(jnp.sum(pairs * softplus_ref[...], axis=0, keepdims=True), axis=1, keepdims=True)
    high, low = split_two(-((pairs + pairs.T) * sigmoid_ref[...]))
    base = dot(high, embed) + dot(low, embed)
    grad_ref[...] = base
    fetch_own.wait()
    fetch_means.wait()
    widest = largest(own_buf[...].astype(F32))
    for r in range(RELS):
        widest = jnp.maximum(widest, largest(mean_buf[r].astype(F32)))
    count = tiles.astype(F32)
    known = widest * NODE_DEV * largest(base)
    note_ref[...] = notes_of((loss, count, 0.0, known, widest * TILE * count, NEG_DEV * widest, 0.0))


def scored(embed, rows, sources, spread):
    scores = lax.dot_general(embed, rows, NT, preferred_element_type=F32)
    sigmoid, softplus = soft_parts(scores)
    per_source = jnp.sum(softplus, axis=1, keepdims=True)
    loss = jnp.sum(per_source * sources, axis=0, keepdims=True) * (1.0 / NEG)
    weight = (sigmoid * (1.0 / NEG)).astype(BF16)
    parts = lax.dot_general(weight, spread, TN, preferred_element_type=F32)
    return weight, loss, parts[:, :H] + parts[:, H:]


def near_body(embed_ref, rows_ref, spread_ref, sources_ref, note_in_ref, weight_ref, part_ref, note_ref):
    rows = rows_ref[...]
    weight, loss, part = scored(embed_ref[...], rows, sources_ref[:, 0:1], spread_ref[...])
    weight_ref[...] = weight
    part_ref[...] = part.astype(part_ref.dtype)
    note = note_in_ref[...]
    lane = lax.broadcasted_iota(jnp.int32, note.shape, 1)
    tallest = largest(rows.astype(F32))
    note = jnp.where(lane == 0, note + loss, note)
    note = jnp.where(lane == 2, jnp.maximum(note, note[:, 3:4] + note[:, 4:5] * tallest), note)
    note_ref[...] = jnp.where(lane == 6, jnp.maximum(note, largest(part)), note)


def rest_body(near_weight_ref, near_rows_ref, weight_ref, rows_ref, sources_ref, base_ref, grad_ref):
    total = dot(near_weight_ref[...], near_rows_ref[...]) + dot(weight_ref[...], rows_ref[...])
    grad_ref[...] = base_ref[...] + sources_ref[:, 0:1] * total


def merge_body(part_ref, arrived_ref, own_note_ref, other_note_ref, send_ref):
    note = own_note_ref[...] + other_note_ref[...]
    first = note.astype(BF16).astype(F32)
    second = (note - first).astype(BF16).astype(F32)
    third = (note - first) - second
    lane = lax.broadcasted_iota(jnp.int32, note.shape, 1)
    note = jnp.where(lane == 3, pltpu.roll(second, 3, 1), jnp.where(lane == 4, pltpu.roll(third, 4, 1), first))
    send_ref[:, :, H:] = jnp.broadcast_to(note[None], (CHIPS, NEG_DEV, 128)).astype(BF16)
    total = part_ref[...] + arrived_ref[...].astype(F32)
    send_ref[:, :, 0:H] = total.reshape(CHIPS, NEG_DEV, H).astype(BF16)


def chosen_rows(neg_ids_ref):
    row = lax.broadcasted_iota(jnp.int32, (16, NODE_DEV), 0)
    lane = lax.broadcasted_iota(jnp.int32, (16, NODE_DEV), 1)
    chosen = jnp.zeros((16, NODE_DEV), F32)
    for i in range(NEG_DEV):
        chosen = jnp.where((row == i) & (lane == neg_ids_ref[i]), 1.0, chosen)
    return chosen.astype(BF16)


def half_at(core):
    return pl.ds(pl.multiple_of(core * HALF, HALF), HALF)


def known_body(neg_ids_ref, core_ref, grad_ref, features_ref, means_ref, own_ref, other_ref, chosen_ref):
    node = lax.broadcasted_iota(jnp.int32, (NODE_DEV, H), 0)
    grad = grad_ref[...]
    for i in range(NEG_DEV):
        grad = jnp.where(node == neg_ids_ref[i], 0.0, grad)
    pre = grad.astype(BF16)
    picks = chosen_rows(neg_ids_ref)
    swapped = core_ref[0] == 1
    for r, rows in enumerate((features_ref[...], means_ref[0], means_ref[1])):
        at = pl.ds(r * H, H)
        both = lax.dot_general(rows, pre, TN, preferred_element_type=F32)
        first, second = both[:, :HALF], both[:, HALF:]
        own_ref[at, :] = jnp.where(swapped, second, first)
        other_ref[at, :] = jnp.where(swapped, first, second)
        chosen_ref[:, at] = dot(picks, rows).astype(BF16)


def outer_body(neg_ids_ref, core_ref, arrived_ref, grad_ref, total_ref, own_ref, other_ref, note_ref, row_ref):
    total = jnp.sum(arrived_ref[...].astype(F32), axis=0)
    note_ref[...] = total[:, H:]
    total_ref[...] = total[:, :H]
    row_ref[...] = jnp.zeros((16, H), F32)
    firsts = []
    for i in range(NEG_DEV):
        first = i
        for j in reversed(range(i)):
            first = jnp.where(neg_ids_ref[j] == neg_ids_ref[i], j, first)
        firsts.append(first)
        row = grad_ref[pl.ds(neg_ids_ref[i], 1), :]
        row_ref[i : i + 1, :] = row if i == 0 else jnp.where(first == i, row, 0.0)
    for i, first in enumerate(firsts):
        row_ref[pl.ds(first, 1), :] += total_ref[i : i + 1, :]
    own_ref[...] = row_ref[:, half_at(core_ref[0])].astype(BF16)
    other_ref[...] = row_ref[:, half_at(1 - core_ref[0])].astype(BF16)


def pre_body(neg_ids_ref, total_ref, grad_ref, pre_ref, sum_ref):
    sum_ref[...] = grad_ref[...]
    for i in range(NEG_DEV):
        sum_ref[pl.ds(neg_ids_ref[i], 1), :] += total_ref[i : i + 1, :]
    pre_ref[...] = sum_ref[...].astype(BF16)


def update_body(known_ref, own_chosen_ref, other_chosen_ref, own_row_ref, other_row_ref, note_ref, out_ref, factor_ref):
    chosen = jnp.concatenate([own_chosen_ref[...], other_chosen_ref[...]], axis=0)
    rows = jnp.concatenate([own_row_ref[...], other_row_ref[...]], axis=0)
    extra = lax.dot_general(chosen, rows, TN, preferred_element_type=F32)
    known, wide, part = (note_ref[0:1, i : i + 1] for i in (2, 5, 6))
    bound = known + wide * part + TINY
    out_ref[...] = (known_ref[...] + extra) * (SPAN / bound)
    factor_ref[...] = jnp.broadcast_to(bound / SPAN / (note_ref[0:1, 1:2] * TILE), (8, HALF))


def first_half_body(core_ref, half_ref, factor_ref, note_ref, weight_ref, loss_ref):
    note = note_ref[0:1, :]
    loss_ref[...] = (note[:, 0:1] + note[:, 3:4] + note[:, 4:5]) / (note[:, 1:2] * TILE)
    weight_ref[...] = (half_ref[...] * factor_ref[0:1, :]).reshape(RELS + 1, H, HALF)


def second_half_body(core_ref, half_ref, factor_ref, note_ref, begun_ref, weight_ref):
    weight_ref[...] = (half_ref[...] * factor_ref[0:1, :]).reshape(RELS + 1, H, HALF)


def halves(body, which, extra, alias):
    whole_weight = jax.ShapeDtypeStruct((RELS + 1, H, H), F32)
    block = pl.BlockSpec((RELS + 1, H, HALF), lambda r, core: (0, 0, which(core[0])))
    scalar = pl.BlockSpec((1, 1), lambda r, core: (0, 0))
    return pl.pallas_call(
        body,
        out_shape=[whole_weight, jax.ShapeDtypeStruct((1, 1), F32)][: 1 + extra],
        grid_spec=pltpu.PrefetchScalarGridSpec(
            num_scalar_prefetch=1,
            grid=(1,),
            in_specs=[vmem(), vmem(), vmem()] + [pl.BlockSpec(memory_space=pl.ANY)] * len(alias),
            out_specs=[block, scalar][: 1 + extra],
        ),
        input_output_aliases=alias,
        compiler_params=pltpu.CompilerParams(vmem_limit_bytes=28 << 20),
    )


def on_device(features, weights, halo_send, nbr_index, tile_count, edge_ends, neg_ids):
    square = (NODE_DEV, H)
    tall = ((RELS + 1) * H, HALF)
    core = lax.axis_index(NEAR).astype(jnp.int32).reshape(1)
    core, halo_send = lax.optimization_barrier((core, halo_send))
    (outgoing,) = call(halo_body, [hbm((N_DOM, HALO_PEER, H), BF16)], [FROM_HBM, FROM_HBM], (), (halo_send[0].T, features))
    incoming = swap(outgoing, DOM)
    neighbours = nbr_index.reshape(NODE_DEV, RELS * FAN)
    two = (RELS, *square)
    halo_count, own_sum, pre = call(
        counts_body,
        [(two, BF16, BY_HAND), (two, F32, BY_HAND), (square, F32, BY_HAND)],
        [BY_HAND, BY_HAND, vmem()],
        [pltpu.VMEM(square, BF16)] * 2 + [pltpu.VMEM(two, BF16)] * 2 + [pltpu.VMEM(two, F32), pltpu.VMEM(square, F32), pltpu.SemaphoreType.DMA((6,))],
        (features, weights, neighbours),
    )
    means, embed, picked = call(
        layer_body,
        [hbm(two, BF16), (square, BF16), hbm((CHIPS, NEG_DEV, H), BF16)],
        [smem(), FROM_HBM, vmem(), FROM_HBM, FROM_HBM, vmem()],
        (),
        (neg_ids, halo_count, incoming.reshape(512, H), own_sum, pre, weights),
    )
    near_rows = swap(picked, FAR).reshape(square)
    base, note, sources, spread = call(
        positive_body,
        [hbm(square, F32), ((8, 128), F32), ((NODE_DEV, 128), F32), ((NODE_DEV, 2 * H), BF16)],
        [smem(), vmem(), FROM_HBM, BY_HAND, BY_HAND],
        [pltpu.VMEM(square, F32)] * 3 + [pltpu.VMEM(square, BF16), pltpu.VMEM(two, BF16), pltpu.SemaphoreType.DMA((2,))],
        (tile_count, embed, edge_ends, features, means),
    )
    near_rows, note = lax.optimization_barrier((near_rows, note))
    other_rows = core_swap(near_rows)
    near_weight, near_part, note = call(
        near_body,
        [(square, BF16), (square, F32), ((8, 128), F32)],
        [vmem()] * 5,
        (),
        (embed, near_rows, spread, sources, note),
    )
    weight, other_part, note = call(
        near_body,
        [(square, BF16), (square, BF16), ((8, 128), F32)],
        [vmem()] * 5,
        (),
        (embed, other_rows, spread, sources, note),
    )
    other_note = core_swap(note)
    part_arrived = core_swap(other_part)
    (grad,) = call(
        rest_body,
        [(square, F32)],
        [vmem()] * 5 + [FROM_HBM],
        (),
        (near_weight, near_rows, weight, other_rows, sources, base),
    )
    part_arrived, grad = lax.optimization_barrier((part_arrived, grad))
    (outgoing_grad,) = call(
        merge_body,
        [((CHIPS, NEG_DEV, H + 128), BF16)],
        [vmem()] * 4,
        (),
        (near_part, part_arrived, note, other_note),
    )
    outgoing_grad, grad = lax.optimization_barrier((outgoing_grad, grad))
    arrived = swap(outgoing_grad, FAR)
    known_own, known_other, chosen = call(
        known_body,
        [(tall, F32), (tall, F32), ((16, (RELS + 1) * H), BF16)],
        [smem(), smem(), vmem(), FROM_HBM, FROM_HBM],
        (),
        (neg_ids, core, grad, features, means),
    )
    other_chosen = core_swap(chosen)
    known = known_own + core_swap(known_other)
    arrived, known, other_chosen = lax.optimization_barrier((arrived, known, other_chosen))
    total, own_row, send_row, note = call(
        outer_body,
        [((NEG_DEV, H), F32), ((16, HALF), BF16), ((16, HALF), BF16), ((NEG_DEV, 128), F32)],
        [smem(), smem(), vmem(), vmem()],
        [pltpu.VMEM((16, H), F32)],
        (neg_ids, core, arrived, grad),
    )
    other_row = core_swap(send_row)
    (pre_grad,) = call(
        pre_body,
        [hbm(square, BF16)],
        [smem(), vmem(), vmem()],
        [pltpu.VMEM(square, F32)],
        (neg_ids, total, grad),
    )
    partial, factor = call(
        update_body,
        [(tall, F32), ((8, HALF), F32)],
        [vmem()] * 6,
        (),
        (known, chosen, other_chosen, own_row, other_row, note),
    )
    chunks = (CHIPS, 24, HALF)
    sums = swap(partial.astype(F16).reshape(chunks), FAR)
    mine = jnp.sum(sums.astype(F32), axis=0).astype(F16)
    half = swap(jnp.broadcast_to(mine, chunks), FAR).reshape(tall)
    other_half = core_swap(half).astype(F32)
    half = half.astype(F32)
    close = near_memory(factor), near_memory(note)
    begun, mean_loss = halves(first_half_body, lambda c: c, 1, {})(core, near_memory(half), *close)
    (begun, other_half) = lax.optimization_barrier((begun, other_half))
    (weight_grad,) = halves(second_half_body, lambda c: 1 - c, 0, {4: 0})(core, near_memory(other_half), *close, begun)
    return weight_grad, mean_loss.reshape(()), pre_grad


def solution(mesh):
    torus = Mesh(mesh.devices.reshape(4, 4, 4, 2), DOM)
    in_specs = (
        P(DOM, None),
        P(),
        P(DOM, None, None),
        P(DOM, None, None),
        P(DOM),
        P(DOM, None, None),
        P(DOM),
    )
    out_specs = (P(), P(), P(DOM, None))
    return jax.shard_map(on_device, mesh=torus, in_specs=in_specs, out_specs=out_specs, check_vma=False)
```

```python
import jax
import jax.numpy as jnp
from jax import lax
from jax.experimental import pallas as pl
from jax.experimental.pallas import tpu as pltpu
from jax.sharding import Mesh
from jax.sharding import PartitionSpec as P

DOM = ("dom_0", "dom_1", "dom_2", "dom_3")
FAR = ("dom_0", "dom_1", "dom_2")
NEAR = ("dom_3",)
H = 512
RELS = 2
FAN = 8
TILE = 256
NODE_DEV = 512
NEG = 1024
NEG_DEV = 8
N_DOM = 128
HALO_PEER = 4
CHIPS = 64
GROUP = 4
HALF = 256
F32 = jnp.float32
BF16 = jnp.bfloat16
F16 = jnp.float16
SPAN = 60000.0
TINY = 1e-30
CODE = 32.0
NT = (((1,), (1,)), ((), ()))
TN = (((0,), (0,)), ((), ()))
FROM_HBM = "hbm"
BY_HAND = "by_hand"


def swap(x, axes):
    return lax.all_to_all(x, axes, split_axis=0, concat_axis=0, tiled=True)


def core_swap(x):
    return lax.ppermute(x, "dom_3", [(0, 1), (1, 0)])


def dot(a, b):
    return jnp.dot(a, b, preferred_element_type=F32)


def split_two(x):
    high = x.astype(BF16)
    return high, (x - high.astype(F32)).astype(BF16)


def vmem():
    return pl.BlockSpec(memory_space=pltpu.VMEM)


def whole(shape):
    return pl.BlockSpec(shape, lambda i: (0,) * len(shape))


def smem():
    return pl.BlockSpec(memory_space=pltpu.SMEM)


def near_memory(x):
    return pltpu.with_memory_space_constraint(x, pltpu.VMEM)


def hbm(shape, kind):
    return pltpu.HBM(shape, kind)


def call(body, outs, specs, scratch=(), args=()):
    given, ins, made, back = [], [], [], []
    for spec, x in zip(specs, args):
        if spec is FROM_HBM or spec is BY_HAND:
            x = pltpu.with_memory_space_constraint(x, pltpu.HBM)
            spec = whole(x.shape) if spec is FROM_HBM else pl.BlockSpec(memory_space=pl.ANY)
        elif spec.memory_space == pltpu.VMEM and x.dtype != jnp.int32:
            x = near_memory(x)
        given.append(x)
        ins.append(spec)
    for o in outs:
        if isinstance(o, tuple) and len(o) == 3:
            made.append(hbm(*o[:2]))
            back.append(pl.BlockSpec(memory_space=pl.ANY))
        elif isinstance(o, tuple):
            made.append(pltpu.VMEM(*o))
            back.append(vmem())
        else:
            made.append(o)
            back.append(whole(o.shape))
    return pl.pallas_call(
        body,
        out_shape=made,
        grid=(1,),
        in_specs=ins,
        out_specs=back,
        scratch_shapes=list(scratch),
        compiler_params=pltpu.CompilerParams(vmem_limit_bytes=28 << 20),
    )(*given)


def halo_body(send_ref, features_ref, out_ref):
    node = lax.broadcasted_iota(jnp.int32, (NODE_DEV, N_DOM), 0)
    own = features_ref[...]
    for k in range(HALO_PEER):
        hit = jnp.where(node == send_ref[k : k + 1, :], 1.0, 0.0).astype(BF16)
        out_ref[:, k, :] = lax.dot_general(hit, own, TN, preferred_element_type=F32).astype(BF16)


def counts_body(features_ref, w_ref, nbr_ref, halo_count_ref, own_sum_ref, pre_ref, own_buf, w_buf, halo_buf, count_buf, sum_buf, pre_buf, sems):
    copy = pltpu.make_async_copy
    fetch_own = copy(features_ref, own_buf, sems.at[0])
    fetch_w = copy(w_ref.at[0], w_buf, sems.at[1])
    fetch_own.start()
    fetch_w.start()
    rows = 32
    lanes = lax.broadcasted_iota(jnp.int32, (rows, NODE_DEV), 1)

    def chunk(step, _):
        at = pl.ds(pl.multiple_of(step * rows, rows), rows)
        for r in range(RELS):
            index = nbr_ref[at, r * FAN : (r + 1) * FAN]
            place = index & (NODE_DEV - 1)
            code = jnp.where(index < NODE_DEV, 1.0, CODE)
            total = jnp.zeros((rows, NODE_DEV), F32)
            for k in range(FAN):
                hit = lanes == place[:, k : k + 1]
                total = total + jnp.where(hit, code[:, k : k + 1], 0.0)
            halo = jnp.floor(total * (1.0 / CODE))
            halo_buf[r, at, :] = halo.astype(BF16)
            count_buf[r, at, :] = (total - CODE * halo).astype(BF16)
        return 0

    lax.fori_loop(0, NODE_DEV // rows, chunk, 0)
    leave = [copy(halo_buf, halo_count_ref, sems.at[2])]
    leave[0].start()
    fetch_own.wait()
    own = own_buf[...]
    for r in range(RELS):
        sum_buf[r] = dot(count_buf[r], own)
        leave.append(copy(sum_buf.at[r], own_sum_ref.at[r], sems.at[3 + r]))
        leave[-1].start()
    fetch_w.wait()
    pre_buf[...] = dot(own, w_buf[...])
    leave.append(copy(pre_buf, pre_ref, sems.at[5]))
    leave[-1].start()
    for one in leave:
        one.wait()


def layer_body(neg_ids_ref, count_ref, halo_ref, own_sum_ref, pre_ref, w_ref, means_ref, embed_ref, picked_ref):
    halo = halo_ref[...]
    preact = pre_ref[...]
    for r in range(RELS):
        total = own_sum_ref[r] + dot(count_ref[r], halo)
        mean = (total * (1.0 / FAN)).astype(BF16)
        means_ref[r] = mean
        preact = preact + dot(mean, w_ref[r + 1])
    embed = preact.astype(BF16)
    embed_ref[...] = embed
    picked = dot(chosen_rows(neg_ids_ref), embed)[:NEG_DEV]
    picked_ref[...] = jnp.broadcast_to(picked[None], (CHIPS, NEG_DEV, H)).astype(BF16)


def soft_parts(x):
    small = jnp.exp(-jnp.abs(x))
    bottom = 1.0 / (1.0 + small)
    sigmoid = jnp.where(x >= 0, bottom, small * bottom)
    log_one = jnp.where(small < 1e-3, small * (1.0 - 0.5 * small), jnp.log(1.0 + small))
    return sigmoid, jnp.maximum(x, 0.0) + log_one


def largest(x):
    return jnp.max(jnp.max(jnp.abs(x), axis=0, keepdims=True), axis=1, keepdims=True)


def notes_of(values):
    lane = lax.broadcasted_iota(jnp.int32, (NEG_DEV, 128), 1)
    note = jnp.zeros((NEG_DEV, 128), F32)
    for place, value in enumerate(values):
        note = jnp.where(lane == place, value, note)
    return note


def positive_body(count_ref, embed_ref, ends_ref, features_ref, means_ref, grad_ref, note_ref, sources_ref, spread_ref, pairs_ref, sigmoid_ref, softplus_ref, own_buf, mean_buf, sems):
    fetch_own = pltpu.make_async_copy(features_ref, own_buf, sems.at[0])
    fetch_means = pltpu.make_async_copy(means_ref, mean_buf, sems.at[1])
    fetch_own.start()
    fetch_means.start()
    embed = embed_ref[...]
    scores = lax.dot_general(embed, embed, NT, preferred_element_type=F32)
    sigmoid, softplus = soft_parts(-scores)
    sigmoid_ref[...] = sigmoid
    softplus_ref[...] = softplus
    pairs_ref[...] = jnp.zeros((NODE_DEV, NODE_DEV), F32)
    node = lax.broadcasted_iota(jnp.int32, (NODE_DEV, TILE), 0)
    tiles = count_ref[0]

    def group(step, _):
        sources, targets = [], []
        for j in range(GROUP):
            t = step * GROUP + j
            source = jnp.where(t < tiles, ends_ref[t, 0:1, :], -1)
            sources.append(jnp.where(node == source, 1.0, 0.0).astype(BF16))
            targets.append(jnp.where(node == ends_ref[t, 1:2, :], 1.0, 0.0).astype(BF16))
        pairs_ref[...] += lax.dot_general(
            jnp.concatenate(sources, axis=1), jnp.concatenate(targets, axis=1), NT, preferred_element_type=F32
        )
        return 0

    lax.fori_loop(0, (tiles + (GROUP - 1)) // GROUP, group, 0)
    pairs = pairs_ref[...]
    sources = jnp.sum(pairs, axis=1, keepdims=True)
    sources_ref[...] = jnp.broadcast_to(sources, (NODE_DEV, 128))
    high, low = split_two(embed.astype(F32) * sources)
    spread_ref[:, 0:H] = high
    spread_ref[:, H:] = low
    loss = jnp.sum(jnp.sum(pairs * softplus_ref[...], axis=0, keepdims=True), axis=1, keepdims=True)
    high, low = split_two(-((pairs + pairs.T) * sigmoid_ref[...]))
    base = dot(high, embed) + dot(low, embed)
    grad_ref[...] = base
    fetch_own.wait()
    fetch_means.wait()
    widest = largest(own_buf[...].astype(F32))
    for r in range(RELS):
        widest = jnp.maximum(widest, largest(mean_buf[r].astype(F32)))
    count = tiles.astype(F32)
    known = widest * NODE_DEV * largest(base)
    note_ref[...] = notes_of((loss, count, 0.0, known, widest * TILE * count, NEG_DEV * widest, 0.0))


def scored(embed, rows, sources, spread):
    scores = lax.dot_general(embed, rows, NT, preferred_element_type=F32)
    sigmoid, softplus = soft_parts(scores)
    per_source = jnp.sum(softplus, axis=1, keepdims=True)
    loss = jnp.sum(per_source * sources, axis=0, keepdims=True) * (1.0 / NEG)
    weight = (sigmoid * (1.0 / NEG)).astype(BF16)
    parts = lax.dot_general(weight, spread, TN, preferred_element_type=F32)
    return weight, loss, parts[:, :H] + parts[:, H:]


def near_body(embed_ref, rows_ref, spread_ref, sources_ref, note_in_ref, weight_ref, part_ref, note_ref):
    rows = rows_ref[...]
    weight, loss, part = scored(embed_ref[...], rows, sources_ref[:, 0:1], spread_ref[...])
    weight_ref[...] = weight
    part_ref[...] = part.astype(part_ref.dtype)
    note = note_in_ref[...]
    lane = lax.broadcasted_iota(jnp.int32, note.shape, 1)
    tallest = largest(rows.astype(F32))
    note = jnp.where(lane == 0, note + loss, note)
    note = jnp.where(lane == 2, jnp.maximum(note, note[:, 3:4] + note[:, 4:5] * tallest), note)
    note_ref[...] = jnp.where(lane == 6, jnp.maximum(note, largest(part)), note)


def rest_body(near_weight_ref, near_rows_ref, weight_ref, rows_ref, sources_ref, base_ref, grad_ref):
    total = dot(near_weight_ref[...], near_rows_ref[...]) + dot(weight_ref[...], rows_ref[...])
    grad_ref[...] = base_ref[...] + sources_ref[:, 0:1] * total


def merge_body(part_ref, arrived_ref, own_note_ref, other_note_ref, send_ref):
    note = own_note_ref[...] + other_note_ref[...]
    first = note.astype(BF16).astype(F32)
    second = (note - first).astype(BF16).astype(F32)
    third = (note - first) - second
    lane = lax.broadcasted_iota(jnp.int32, note.shape, 1)
    note = jnp.where(lane == 3, pltpu.roll(second, 3, 1), jnp.where(lane == 4, pltpu.roll(third, 4, 1), first))
    send_ref[:, :, H:] = jnp.broadcast_to(note[None], (CHIPS, NEG_DEV, 128)).astype(BF16)
    total = part_ref[...] + arrived_ref[...].astype(F32)
    send_ref[:, :, 0:H] = total.reshape(CHIPS, NEG_DEV, H).astype(BF16)


def chosen_rows(neg_ids_ref):
    row = lax.broadcasted_iota(jnp.int32, (16, NODE_DEV), 0)
    lane = lax.broadcasted_iota(jnp.int32, (16, NODE_DEV), 1)
    chosen = jnp.zeros((16, NODE_DEV), F32)
    for i in range(NEG_DEV):
        chosen = jnp.where((row == i) & (lane == neg_ids_ref[i]), 1.0, chosen)
    return chosen.astype(BF16)


def half_at(core):
    return pl.ds(pl.multiple_of(core * HALF, HALF), HALF)


def known_body(neg_ids_ref, core_ref, grad_ref, features_ref, means_ref, own_ref, other_ref, chosen_ref):
    node = lax.broadcasted_iota(jnp.int32, (NODE_DEV, H), 0)
    grad = grad_ref[...]
    for i in range(NEG_DEV):
        grad = jnp.where(node == neg_ids_ref[i], 0.0, grad)
    pre = grad.astype(BF16)
    picks = chosen_rows(neg_ids_ref)
    swapped = core_ref[0] == 1
    for r, rows in enumerate((features_ref[...], means_ref[0], means_ref[1])):
        at = pl.ds(r * H, H)
        both = lax.dot_general(rows, pre, TN, preferred_element_type=F32)
        first, second = both[:, :HALF], both[:, HALF:]
        own_ref[at, :] = jnp.where(swapped, second, first)
        other_ref[at, :] = jnp.where(swapped, first, second)
        chosen_ref[:, at] = dot(picks, rows).astype(BF16)


def outer_body(neg_ids_ref, core_ref, arrived_ref, grad_ref, total_ref, own_ref, other_ref, note_ref, row_ref):
    total = jnp.sum(arrived_ref[...].astype(F32), axis=0)
    note_ref[...] = total[:, H:]
    total_ref[...] = total[:, :H]
    row_ref[...] = jnp.zeros((16, H), F32)
    firsts = []
    for i in range(NEG_DEV):
        first = i
        for j in reversed(range(i)):
            first = jnp.where(neg_ids_ref[j] == neg_ids_ref[i], j, first)
        firsts.append(first)
        row = grad_ref[pl.ds(neg_ids_ref[i], 1), :]
        row_ref[i : i + 1, :] = row if i == 0 else jnp.where(first == i, row, 0.0)
    for i, first in enumerate(firsts):
        row_ref[pl.ds(first, 1), :] += total_ref[i : i + 1, :]
    own_ref[...] = row_ref[:, half_at(core_ref[0])].astype(BF16)
    other_ref[...] = row_ref[:, half_at(1 - core_ref[0])].astype(BF16)


def pre_body(neg_ids_ref, total_ref, grad_ref, pre_ref, sum_ref):
    sum_ref[...] = grad_ref[...]
    for i in range(NEG_DEV):
        sum_ref[pl.ds(neg_ids_ref[i], 1), :] += total_ref[i : i + 1, :]
    pre_ref[...] = sum_ref[...].astype(BF16)


def update_body(known_ref, own_chosen_ref, other_chosen_ref, own_row_ref, other_row_ref, note_ref, out_ref, factor_ref):
    chosen = jnp.concatenate([own_chosen_ref[...], other_chosen_ref[...]], axis=0)
    rows = jnp.concatenate([own_row_ref[...], other_row_ref[...]], axis=0)
    extra = lax.dot_general(chosen, rows, TN, preferred_element_type=F32)
    known, wide, part = (note_ref[0:1, i : i + 1] for i in (2, 5, 6))
    bound = known + wide * part + TINY
    out_ref[...] = (known_ref[...] + extra) * (SPAN / bound)
    factor_ref[...] = jnp.broadcast_to(bound / SPAN / (note_ref[0:1, 1:2] * TILE), (8, HALF))


def first_half_body(core_ref, half_ref, factor_ref, note_ref, weight_ref, loss_ref):
    note = note_ref[0:1, :]
    loss_ref[...] = (note[:, 0:1] + note[:, 3:4] + note[:, 4:5]) / (note[:, 1:2] * TILE)
    weight_ref[...] = (half_ref[...] * factor_ref[0:1, :]).reshape(RELS + 1, H, HALF)


def second_half_body(core_ref, half_ref, factor_ref, note_ref, begun_ref, weight_ref):
    weight_ref[...] = (half_ref[...] * factor_ref[0:1, :]).reshape(RELS + 1, H, HALF)


def halves(body, which, extra, alias):
    whole_weight = jax.ShapeDtypeStruct((RELS + 1, H, H), F32)
    block = pl.BlockSpec((RELS + 1, H, HALF), lambda r, core: (0, 0, which(core[0])))
    scalar = pl.BlockSpec((1, 1), lambda r, core: (0, 0))
    return pl.pallas_call(
        body,
        out_shape=[whole_weight, jax.ShapeDtypeStruct((1, 1), F32)][: 1 + extra],
        grid_spec=pltpu.PrefetchScalarGridSpec(
            num_scalar_prefetch=1,
            grid=(1,),
            in_specs=[vmem(), vmem(), vmem()] + [pl.BlockSpec(memory_space=pl.ANY)] * len(alias),
            out_specs=[block, scalar][: 1 + extra],
        ),
        input_output_aliases=alias,
        compiler_params=pltpu.CompilerParams(vmem_limit_bytes=28 << 20),
    )


def on_device(features, weights, halo_send, nbr_index, tile_count, edge_ends, neg_ids):
    square = (NODE_DEV, H)
    tall = ((RELS + 1) * H, HALF)
    core = lax.axis_index(NEAR).astype(jnp.int32).reshape(1)
    core, halo_send = lax.optimization_barrier((core, halo_send))
    (outgoing,) = call(halo_body, [((N_DOM, HALO_PEER, H), BF16)], [FROM_HBM, FROM_HBM], (), (halo_send[0].T, features))
    incoming = swap(outgoing, DOM)
    neighbours = nbr_index.reshape(NODE_DEV, RELS * FAN)
    two = (RELS, *square)
    halo_count, own_sum, pre = call(
        counts_body,
        [(two, BF16, BY_HAND), (two, F32, BY_HAND), (square, F32, BY_HAND)],
        [BY_HAND, BY_HAND, vmem()],
        [pltpu.VMEM(square, BF16)] * 2 + [pltpu.VMEM(two, BF16)] * 2 + [pltpu.VMEM(two, F32), pltpu.VMEM(square, F32), pltpu.SemaphoreType.DMA((6,))],
        (features, weights, neighbours),
    )
    means, embed, picked = call(
        layer_body,
        [hbm(two, BF16), (square, BF16), hbm((CHIPS, NEG_DEV, H), BF16)],
        [smem(), FROM_HBM, vmem(), FROM_HBM, FROM_HBM, vmem()],
        (),
        (neg_ids, halo_count, incoming.reshape(512, H), own_sum, pre, weights),
    )
    near_rows = swap(picked, FAR).reshape(square)
    base, note, sources, spread = call(
        positive_body,
        [hbm(square, F32), ((8, 128), F32), ((NODE_DEV, 128), F32), ((NODE_DEV, 2 * H), BF16)],
        [smem(), vmem(), FROM_HBM, BY_HAND, BY_HAND],
        [pltpu.VMEM(square, F32)] * 3 + [pltpu.VMEM(square, BF16), pltpu.VMEM(two, BF16), pltpu.SemaphoreType.DMA((2,))],
        (tile_count, embed, edge_ends, features, means),
    )
    near_rows, note = lax.optimization_barrier((near_rows, note))
    other_rows = core_swap(near_rows)
    near_weight, near_part, note = call(
        near_body,
        [(square, BF16), (square, F32), ((8, 128), F32)],
        [vmem()] * 5,
        (),
        (embed, near_rows, spread, sources, note),
    )
    weight, other_part, note = call(
        near_body,
        [(square, BF16), (square, BF16), ((8, 128), F32)],
        [vmem()] * 5,
        (),
        (embed, other_rows, spread, sources, note),
    )
    other_note = core_swap(note)
    part_arrived = core_swap(other_part)
    (grad,) = call(
        rest_body,
        [(square, F32)],
        [vmem()] * 5 + [FROM_HBM],
        (),
        (near_weight, near_rows, weight, other_rows, sources, base),
    )
    part_arrived, grad = lax.optimization_barrier((part_arrived, grad))
    (outgoing_grad,) = call(
        merge_body,
        [((CHIPS, NEG_DEV, H + 128), BF16)],
        [vmem()] * 4,
        (),
        (near_part, part_arrived, note, other_note),
    )
    outgoing_grad, grad = lax.optimization_barrier((outgoing_grad, grad))
    arrived = swap(outgoing_grad, FAR)
    known_own, known_other, chosen = call(
        known_body,
        [(tall, F32), (tall, F32), ((16, (RELS + 1) * H), BF16)],
        [smem(), smem(), vmem(), FROM_HBM, FROM_HBM],
        (),
        (neg_ids, core, grad, features, means),
    )
    other_chosen = core_swap(chosen)
    known = known_own + core_swap(known_other)
    arrived, known, other_chosen = lax.optimization_barrier((arrived, known, other_chosen))
    total, own_row, send_row, note = call(
        outer_body,
        [((NEG_DEV, H), F32), ((16, HALF), BF16), ((16, HALF), BF16), ((NEG_DEV, 128), F32)],
        [smem(), smem(), vmem(), vmem()],
        [pltpu.VMEM((16, H), F32)],
        (neg_ids, core, arrived, grad),
    )
    other_row = core_swap(send_row)
    (pre_grad,) = call(
        pre_body,
        [hbm(square, BF16)],
        [smem(), vmem(), vmem()],
        [pltpu.VMEM(square, F32)],
        (neg_ids, total, grad),
    )
    partial, factor = call(
        update_body,
        [(tall, F32), ((8, HALF), F32)],
        [vmem()] * 6,
        (),
        (known, chosen, other_chosen, own_row, other_row, note),
    )
    chunks = (CHIPS, 24, HALF)
    sums = swap(partial.astype(F16).reshape(chunks), FAR)
    mine = jnp.sum(sums.astype(F32), axis=0).astype(F16)
    half = swap(jnp.broadcast_to(mine, chunks), FAR).reshape(tall)
    other_half = core_swap(half).astype(F32)
    half = half.astype(F32)
    close = near_memory(factor), near_memory(note)
    begun, mean_loss = halves(first_half_body, lambda c: c, 1, {})(core, near_memory(half), *close)
    (begun, other_half) = lax.optimization_barrier((begun, other_half))
    (weight_grad,) = halves(second_half_body, lambda c: 1 - c, 0, {4: 0})(core, near_memory(other_half), *close, begun)
    return weight_grad, mean_loss.reshape(()), pre_grad


def solution(mesh):
    torus = Mesh(mesh.devices.reshape(4, 4, 4, 2), DOM)
    in_specs = (
        P(DOM, None),
        P(),
        P(DOM, None, None),
        P(DOM, None, None),
        P(DOM),
        P(DOM, None, None),
        P(DOM),
    )
    out_specs = (P(), P(), P(DOM, None))
    return jax.shard_map(on_device, mesh=torus, in_specs=in_specs, out_specs=out_specs, check_vma=False)
```

```python
import jax
import jax.numpy as jnp
from jax import lax
from jax.experimental import pallas as pl
from jax.experimental.pallas import tpu as pltpu
from jax.sharding import Mesh
from jax.sharding import PartitionSpec as P

DOM = ("dom_0", "dom_1", "dom_2", "dom_3")
FAR = ("dom_0", "dom_1", "dom_2")
NEAR = ("dom_3",)
H = 512
RELS = 2
FAN = 8
TILE = 256
NODE_DEV = 512
NEG = 1024
NEG_DEV = 8
N_DOM = 128
HALO_PEER = 4
CHIPS = 64
GROUP = 4
HALF = 256
F32 = jnp.float32
BF16 = jnp.bfloat16
F16 = jnp.float16
SPAN = 60000.0
TINY = 1e-30
CODE = 32.0
NT = (((1,), (1,)), ((), ()))
TN = (((0,), (0,)), ((), ()))
FROM_HBM = "hbm"
BY_HAND = "by_hand"


def swap(x, axes):
    return lax.all_to_all(x, axes, split_axis=0, concat_axis=0, tiled=True)


def core_swap(x):
    return lax.ppermute(x, "dom_3", [(0, 1), (1, 0)])


def dot(a, b):
    return jnp.dot(a, b, preferred_element_type=F32)


def split_two(x):
    high = x.astype(BF16)
    return high, (x - high.astype(F32)).astype(BF16)


def vmem():
    return pl.BlockSpec(memory_space=pltpu.VMEM)


def whole(shape):
    return pl.BlockSpec(shape, lambda i: (0,) * len(shape))


def smem():
    return pl.BlockSpec(memory_space=pltpu.SMEM)


def near_memory(x):
    return pltpu.with_memory_space_constraint(x, pltpu.VMEM)


def hbm(shape, kind):
    return pltpu.HBM(shape, kind)


def call(body, outs, specs, scratch=(), args=()):
    given, ins, made, back = [], [], [], []
    for spec, x in zip(specs, args):
        if spec is FROM_HBM or spec is BY_HAND:
            x = pltpu.with_memory_space_constraint(x, pltpu.HBM)
            spec = whole(x.shape) if spec is FROM_HBM else pl.BlockSpec(memory_space=pl.ANY)
        elif spec.memory_space == pltpu.VMEM and x.dtype != jnp.int32:
            x = near_memory(x)
        given.append(x)
        ins.append(spec)
    for o in outs:
        if isinstance(o, tuple) and len(o) == 3:
            made.append(hbm(*o[:2]))
            back.append(pl.BlockSpec(memory_space=pl.ANY))
        elif isinstance(o, tuple):
            made.append(pltpu.VMEM(*o))
            back.append(vmem())
        else:
            made.append(o)
            back.append(whole(o.shape))
    return pl.pallas_call(
        body,
        out_shape=made,
        grid=(1,),
        in_specs=ins,
        out_specs=back,
        scratch_shapes=list(scratch),
        compiler_params=pltpu.CompilerParams(vmem_limit_bytes=28 << 20),
    )(*given)


def halo_body(send_ref, features_ref, out_ref):
    node = lax.broadcasted_iota(jnp.int32, (NODE_DEV, N_DOM), 0)
    own = features_ref[...]
    for k in range(HALO_PEER):
        hit = jnp.where(node == send_ref[k : k + 1, :], 1.0, 0.0).astype(BF16)
        out_ref[:, k, :] = lax.dot_general(hit, own, TN, preferred_element_type=F32).astype(BF16)


def counts_body(features_ref, w_ref, nbr_ref, halo_count_ref, own_sum_ref, pre_ref, own_buf, w_buf, halo_buf, count_buf, sum_buf, pre_buf, sems):
    copy = pltpu.make_async_copy
    fetch_own = copy(features_ref, own_buf, sems.at[0])
    fetch_w = copy(w_ref.at[0], w_buf, sems.at[1])
    fetch_own.start()
    fetch_w.start()
    rows = 32
    lanes = lax.broadcasted_iota(jnp.int32, (rows, NODE_DEV), 1)

    def chunk(step, _):
        at = pl.ds(pl.multiple_of(step * rows, rows), rows)
        for r in range(RELS):
            index = nbr_ref[at, r * FAN : (r + 1) * FAN]
            place = index & (NODE_DEV - 1)
            code = jnp.where(index < NODE_DEV, 1.0, CODE)
            total = jnp.zeros((rows, NODE_DEV), F32)
            for k in range(FAN):
                hit = lanes == place[:, k : k + 1]
                total = total + jnp.where(hit, code[:, k : k + 1], 0.0)
            halo = jnp.floor(total * (1.0 / CODE))
            halo_buf[r, at, :] = halo.astype(BF16)
            count_buf[r, at, :] = (total - CODE * halo).astype(BF16)
        return 0

    lax.fori_loop(0, NODE_DEV // rows, chunk, 0)
    leave = [copy(halo_buf, halo_count_ref, sems.at[2])]
    leave[0].start()
    fetch_own.wait()
    own = own_buf[...]
    for r in range(RELS):
        sum_buf[r] = dot(count_buf[r], own)
        leave.append(copy(sum_buf.at[r], own_sum_ref.at[r], sems.at[3 + r]))
        leave[-1].start()
    fetch_w.wait()
    pre_buf[...] = dot(own, w_buf[...])
    leave.append(copy(pre_buf, pre_ref, sems.at[5]))
    leave[-1].start()
    for one in leave:
        one.wait()


def layer_body(neg_ids_ref, count_ref, halo_ref, own_sum_ref, pre_ref, w_ref, means_ref, embed_ref, picked_ref):
    halo = halo_ref[...]
    preact = pre_ref[...]
    for r in range(RELS):
        total = own_sum_ref[r] + dot(count_ref[r], halo)
        mean = (total * (1.0 / FAN)).astype(BF16)
        means_ref[r] = mean
        preact = preact + dot(mean, w_ref[r + 1])
    embed = preact.astype(BF16)
    embed_ref[...] = embed
    picked = dot(chosen_rows(neg_ids_ref), embed)[:NEG_DEV]
    picked_ref[...] = jnp.broadcast_to(picked[None], (CHIPS, NEG_DEV, H)).astype(BF16)


def soft_parts(x):
    small = jnp.exp(-jnp.abs(x))
    bottom = 1.0 / (1.0 + small)
    sigmoid = jnp.where(x >= 0, bottom, small * bottom)
    log_one = jnp.where(small < 1e-3, small * (1.0 - 0.5 * small), jnp.log(1.0 + small))
    return sigmoid, jnp.maximum(x, 0.0) + log_one


def largest(x):
    return jnp.max(jnp.max(jnp.abs(x), axis=0, keepdims=True), axis=1, keepdims=True)


def notes_of(values):
    lane = lax.broadcasted_iota(jnp.int32, (NEG_DEV, 128), 1)
    note = jnp.zeros((NEG_DEV, 128), F32)
    for place, value in enumerate(values):
        note = jnp.where(lane == place, value, note)
    return note


def positive_body(count_ref, embed_ref, ends_ref, features_ref, means_ref, grad_ref, note_ref, sources_ref, spread_ref, pairs_ref, sigmoid_ref, softplus_ref, own_buf, mean_buf, sems):
    fetch_own = pltpu.make_async_copy(features_ref, own_buf, sems.at[0])
    fetch_means = pltpu.make_async_copy(means_ref, mean_buf, sems.at[1])
    fetch_own.start()
    fetch_means.start()
    embed = embed_ref[...]
    scores = lax.dot_general(embed, embed, NT, preferred_element_type=F32)
    sigmoid, softplus = soft_parts(-scores)
    sigmoid_ref[...] = sigmoid
    softplus_ref[...] = softplus
    pairs_ref[...] = jnp.zeros((NODE_DEV, NODE_DEV), F32)
    node = lax.broadcasted_iota(jnp.int32, (NODE_DEV, TILE), 0)
    tiles = count_ref[0]

    def group(step, _):
        sources, targets = [], []
        for j in range(GROUP):
            t = step * GROUP + j
            source = jnp.where(t < tiles, ends_ref[t, 0:1, :], -1)
            sources.append(jnp.where(node == source, 1.0, 0.0).astype(BF16))
            targets.append(jnp.where(node == ends_ref[t, 1:2, :], 1.0, 0.0).astype(BF16))
        pairs_ref[...] += lax.dot_general(
            jnp.concatenate(sources, axis=1), jnp.concatenate(targets, axis=1), NT, preferred_element_type=F32
        )
        return 0

    lax.fori_loop(0, (tiles + (GROUP - 1)) // GROUP, group, 0)
    pairs = pairs_ref[...]
    sources = jnp.sum(pairs, axis=1, keepdims=True)
    sources_ref[...] = jnp.broadcast_to(sources, (NODE_DEV, 128))
    high, low = split_two(embed.astype(F32) * sources)
    spread_ref[:, 0:H] = high
    spread_ref[:, H:] = low
    loss = jnp.sum(jnp.sum(pairs * softplus_ref[...], axis=0, keepdims=True), axis=1, keepdims=True)
    high, low = split_two(-((pairs + pairs.T) * sigmoid_ref[...]))
    base = dot(high, embed) + dot(low, embed)
    grad_ref[...] = base
    fetch_own.wait()
    fetch_means.wait()
    widest = largest(own_buf[...].astype(F32))
    for r in range(RELS):
        widest = jnp.maximum(widest, largest(mean_buf[r].astype(F32)))
    count = tiles.astype(F32)
    reach = largest(embed.astype(F32)) * count * (TILE / NEG)
    known = widest * NODE_DEV * largest(base)
    note_ref[...] = notes_of((loss, count, 0.0, known, widest * TILE * count, NEG_DEV * widest, reach))


def scored(embed, rows, sources, spread):
    scores = lax.dot_general(embed, rows, NT, preferred_element_type=F32)
    sigmoid, softplus = soft_parts(scores)
    per_source = jnp.sum(softplus, axis=1, keepdims=True)
    loss = jnp.sum(per_source * sources, axis=0, keepdims=True) * (1.0 / NEG)
    weight = (sigmoid * (1.0 / NEG)).astype(BF16)
    parts = lax.dot_general(weight, spread, TN, preferred_element_type=F32)
    return weight, loss, parts[:, :H] + parts[:, H:]


def near_body(embed_ref, rows_ref, spread_ref, sources_ref, note_in_ref, weight_ref, part_ref, note_ref):
    rows = rows_ref[...]
    weight, loss, part = scored(embed_ref[...], rows, sources_ref[:, 0:1], spread_ref[...])
    weight_ref[...] = weight
    part_ref[...] = part.astype(part_ref.dtype)
    note = note_in_ref[...]
    lane = lax.broadcasted_iota(jnp.int32, note.shape, 1)
    tallest = largest(rows.astype(F32))
    note = jnp.where(lane == 0, note + loss, note)
    note_ref[...] = jnp.where(lane == 2, jnp.maximum(note, note[:, 3:4] + note[:, 4:5] * tallest), note)


def rest_body(near_weight_ref, near_rows_ref, weight_ref, rows_ref, sources_ref, base_ref, grad_ref):
    total = dot(near_weight_ref[...], near_rows_ref[...]) + dot(weight_ref[...], rows_ref[...])
    grad_ref[...] = base_ref[...] + sources_ref[:, 0:1] * total


def merge_body(part_ref, arrived_ref, own_note_ref, other_note_ref, send_ref):
    note = own_note_ref[...] + other_note_ref[...]
    first = note.astype(BF16).astype(F32)
    second = (note - first).astype(BF16).astype(F32)
    third = (note - first) - second
    lane = lax.broadcasted_iota(jnp.int32, note.shape, 1)
    note = jnp.where(lane == 3, pltpu.roll(second, 3, 1), jnp.where(lane == 4, pltpu.roll(third, 4, 1), first))
    send_ref[:, :, H:] = jnp.broadcast_to(note[None], (CHIPS, NEG_DEV, 128)).astype(BF16)
    total = part_ref[...] + arrived_ref[...].astype(F32)
    send_ref[:, :, 0:H] = total.reshape(CHIPS, NEG_DEV, H).astype(BF16)


def chosen_rows(neg_ids_ref):
    row = lax.broadcasted_iota(jnp.int32, (16, NODE_DEV), 0)
    lane = lax.broadcasted_iota(jnp.int32, (16, NODE_DEV), 1)
    chosen = jnp.zeros((16, NODE_DEV), F32)
    for i in range(NEG_DEV):
        chosen = jnp.where((row == i) & (lane == neg_ids_ref[i]), 1.0, chosen)
    return chosen.astype(BF16)


def half_at(core):
    return pl.ds(pl.multiple_of(core * HALF, HALF), HALF)


def known_body(neg_ids_ref, core_ref, grad_ref, features_ref, means_ref, own_ref, other_ref, chosen_ref):
    node = lax.broadcasted_iota(jnp.int32, (NODE_DEV, H), 0)
    grad = grad_ref[...]
    for i in range(NEG_DEV):
        grad = jnp.where(node == neg_ids_ref[i], 0.0, grad)
    pre = grad.astype(BF16)
    picks = chosen_rows(neg_ids_ref)
    swapped = core_ref[0] == 1
    for r, rows in enumerate((features_ref[...], means_ref[0], means_ref[1])):
        at = pl.ds(r * H, H)
        both = lax.dot_general(rows, pre, TN, preferred_element_type=F32)
        first, second = both[:, :HALF], both[:, HALF:]
        own_ref[at, :] = jnp.where(swapped, second, first)
        other_ref[at, :] = jnp.where(swapped, first, second)
        chosen_ref[:, at] = dot(picks, rows).astype(BF16)


def outer_body(neg_ids_ref, core_ref, arrived_ref, grad_ref, total_ref, own_ref, other_ref, note_ref, row_ref):
    total = jnp.sum(arrived_ref[...].astype(F32), axis=0)
    note_ref[...] = total[:, H:]
    total_ref[...] = total[:, :H]
    row_ref[...] = jnp.zeros((16, H), F32)
    firsts = []
    for i in range(NEG_DEV):
        first = i
        for j in reversed(range(i)):
            first = jnp.where(neg_ids_ref[j] == neg_ids_ref[i], j, first)
        firsts.append(first)
        row = grad_ref[pl.ds(neg_ids_ref[i], 1), :]
        row_ref[i : i + 1, :] = row if i == 0 else jnp.where(first == i, row, 0.0)
    for i, first in enumerate(firsts):
        row_ref[pl.ds(first, 1), :] += total_ref[i : i + 1, :]
    own_ref[...] = row_ref[:, half_at(core_ref[0])].astype(BF16)
    other_ref[...] = row_ref[:, half_at(1 - core_ref[0])].astype(BF16)


def pre_body(neg_ids_ref, total_ref, grad_ref, pre_ref, sum_ref):
    sum_ref[...] = grad_ref[...]
    for i in range(NEG_DEV):
        sum_ref[pl.ds(neg_ids_ref[i], 1), :] += total_ref[i : i + 1, :]
    pre_ref[...] = sum_ref[...].astype(BF16)


def update_body(known_ref, own_chosen_ref, other_chosen_ref, own_row_ref, other_row_ref, note_ref, out_ref, factor_ref):
    chosen = jnp.concatenate([own_chosen_ref[...], other_chosen_ref[...]], axis=0)
    rows = jnp.concatenate([own_row_ref[...], other_row_ref[...]], axis=0)
    extra = lax.dot_general(chosen, rows, TN, preferred_element_type=F32)
    known, wide, part = (note_ref[0:1, i : i + 1] for i in (2, 5, 6))
    bound = known + wide * part + TINY
    out_ref[...] = (known_ref[...] + extra) * (SPAN / bound)
    factor_ref[...] = jnp.broadcast_to(bound / SPAN / (note_ref[0:1, 1:2] * TILE), (8, HALF))


def first_half_body(core_ref, half_ref, factor_ref, note_ref, weight_ref, loss_ref):
    note = note_ref[0:1, :]
    loss_ref[...] = (note[:, 0:1] + note[:, 3:4] + note[:, 4:5]) / (note[:, 1:2] * TILE)
    weight_ref[...] = (half_ref[...] * factor_ref[0:1, :]).reshape(RELS + 1, H, HALF)


def second_half_body(core_ref, half_ref, factor_ref, note_ref, begun_ref, weight_ref):
    weight_ref[...] = (half_ref[...] * factor_ref[0:1, :]).reshape(RELS + 1, H, HALF)


def halves(body, which, extra, alias):
    whole_weight = jax.ShapeDtypeStruct((RELS + 1, H, H), F32)
    block = pl.BlockSpec((RELS + 1, H, HALF), lambda r, core: (0, 0, which(core[0])))
    scalar = pl.BlockSpec((1, 1), lambda r, core: (0, 0))
    return pl.pallas_call(
        body,
        out_shape=[whole_weight, jax.ShapeDtypeStruct((1, 1), F32)][: 1 + extra],
        grid_spec=pltpu.PrefetchScalarGridSpec(
            num_scalar_prefetch=1,
            grid=(1,),
            in_specs=[vmem(), vmem(), vmem()] + [pl.BlockSpec(memory_space=pl.ANY)] * len(alias),
            out_specs=[block, scalar][: 1 + extra],
        ),
        input_output_aliases=alias,
        compiler_params=pltpu.CompilerParams(vmem_limit_bytes=28 << 20),
    )


def on_device(features, weights, halo_send, nbr_index, tile_count, edge_ends, neg_ids):
    square = (NODE_DEV, H)
    tall = ((RELS + 1) * H, HALF)
    core = lax.axis_index(NEAR).astype(jnp.int32).reshape(1)
    core, halo_send = lax.optimization_barrier((core, halo_send))
    (outgoing,) = call(halo_body, [((N_DOM, HALO_PEER, H), BF16)], [FROM_HBM, FROM_HBM], (), (halo_send[0].T, features))
    incoming = swap(outgoing, DOM)
    neighbours = nbr_index.reshape(NODE_DEV, RELS * FAN)
    two = (RELS, *square)
    halo_count, own_sum, pre = call(
        counts_body,
        [(two, BF16, BY_HAND), (two, F32, BY_HAND), (square, F32, BY_HAND)],
        [BY_HAND, BY_HAND, vmem()],
        [pltpu.VMEM(square, BF16)] * 2 + [pltpu.VMEM(two, BF16)] * 2 + [pltpu.VMEM(two, F32), pltpu.VMEM(square, F32), pltpu.SemaphoreType.DMA((6,))],
        (features, weights, neighbours),
    )
    means, embed, picked = call(
        layer_body,
        [hbm(two, BF16), (square, BF16), hbm((CHIPS, NEG_DEV, H), BF16)],
        [smem(), FROM_HBM, vmem(), FROM_HBM, FROM_HBM, vmem()],
        (),
        (neg_ids, halo_count, incoming.reshape(512, H), own_sum, pre, weights),
    )
    near_rows = swap(picked, FAR).reshape(square)
    base, note, sources, spread = call(
        positive_body,
        [hbm(square, F32), ((8, 128), F32), ((NODE_DEV, 128), F32), ((NODE_DEV, 2 * H), BF16)],
        [smem(), vmem(), FROM_HBM, BY_HAND, BY_HAND],
        [pltpu.VMEM(square, F32)] * 3 + [pltpu.VMEM(square, BF16), pltpu.VMEM(two, BF16), pltpu.SemaphoreType.DMA((2,))],
        (tile_count, embed, edge_ends, features, means),
    )
    near_rows, note = lax.optimization_barrier((near_rows, note))
    other_rows = core_swap(near_rows)
    near_weight, near_part, note = call(
        near_body,
        [(square, BF16), (square, F32), ((8, 128), F32)],
        [vmem()] * 5,
        (),
        (embed, near_rows, spread, sources, note),
    )
    weight, other_part, note = call(
        near_body,
        [(square, BF16), (square, BF16), ((8, 128), F32)],
        [vmem()] * 5,
        (),
        (embed, other_rows, spread, sources, note),
    )
    other_note = core_swap(note)
    part_arrived = core_swap(other_part)
    (grad,) = call(
        rest_body,
        [(square, F32)],
        [vmem()] * 5 + [FROM_HBM],
        (),
        (near_weight, near_rows, weight, other_rows, sources, base),
    )
    part_arrived, grad = lax.optimization_barrier((part_arrived, grad))
    (outgoing_grad,) = call(
        merge_body,
        [((CHIPS, NEG_DEV, H + 128), BF16)],
        [vmem()] * 4,
        (),
        (near_part, part_arrived, note, other_note),
    )
    outgoing_grad, grad = lax.optimization_barrier((outgoing_grad, grad))
    arrived = swap(outgoing_grad, FAR)
    known_own, known_other, chosen = call(
        known_body,
        [(tall, F32), (tall, F32), ((16, (RELS + 1) * H), BF16)],
        [smem(), smem(), vmem(), FROM_HBM, FROM_HBM],
        (),
        (neg_ids, core, grad, features, means),
    )
    other_chosen = core_swap(chosen)
    known = known_own + core_swap(known_other)
    arrived, known, other_chosen = lax.optimization_barrier((arrived, known, other_chosen))
    total, own_row, send_row, note = call(
        outer_body,
        [((NEG_DEV, H), F32), ((16, HALF), BF16), ((16, HALF), BF16), ((NEG_DEV, 128), F32)],
        [smem(), smem(), vmem(), vmem()],
        [pltpu.VMEM((16, H), F32)],
        (neg_ids, core, arrived, grad),
    )
    other_row = core_swap(send_row)
    (pre_grad,) = call(
        pre_body,
        [hbm(square, BF16)],
        [smem(), vmem(), vmem()],
        [pltpu.VMEM(square, F32)],
        (neg_ids, total, grad),
    )
    partial, factor = call(
        update_body,
        [(tall, F32), ((8, HALF), F32)],
        [vmem()] * 6,
        (),
        (known, chosen, other_chosen, own_row, other_row, note),
    )
    chunks = (CHIPS, 24, HALF)
    sums = swap(partial.astype(F16).reshape(chunks), FAR)
    mine = jnp.sum(sums.astype(F32), axis=0).astype(F16)
    half = swap(jnp.broadcast_to(mine, chunks), FAR).reshape(tall)
    other_half = core_swap(half).astype(F32)
    half = half.astype(F32)
    close = near_memory(factor), near_memory(note)
    begun, mean_loss = halves(first_half_body, lambda c: c, 1, {})(core, near_memory(half), *close)
    (begun, other_half) = lax.optimization_barrier((begun, other_half))
    (weight_grad,) = halves(second_half_body, lambda c: 1 - c, 0, {4: 0})(core, near_memory(other_half), *close, begun)
    return weight_grad, mean_loss.reshape(()), pre_grad


def solution(mesh):
    torus = Mesh(mesh.devices.reshape(4, 4, 4, 2), DOM)
    in_specs = (
        P(DOM, None),
        P(),
        P(DOM, None, None),
        P(DOM, None, None),
        P(DOM),
        P(DOM, None, None),
        P(DOM),
    )
    out_specs = (P(), P(), P(DOM, None))
    return jax.shard_map(on_device, mesh=torus, in_specs=in_specs, out_specs=out_specs, check_vma=False)
```

```python
import jax
import jax.numpy as jnp
from jax import lax
from jax.experimental import pallas as pl
from jax.experimental.pallas import tpu as pltpu
from jax.sharding import Mesh
from jax.sharding import PartitionSpec as P

DOM = ("dom_0", "dom_1", "dom_2", "dom_3")
FAR = ("dom_0", "dom_1", "dom_2")
NEAR = ("dom_3",)
H = 512
RELS = 2
FAN = 8
TILE = 256
NODE_DEV = 512
NEG = 1024
NEG_DEV = 8
N_DOM = 128
HALO_PEER = 4
CHIPS = 64
GROUP = 4
HALF = 256
F32 = jnp.float32
BF16 = jnp.bfloat16
F16 = jnp.float16
SPAN = 60000.0
TINY = 1e-30
CODE = 32.0
NT = (((1,), (1,)), ((), ()))
TN = (((0,), (0,)), ((), ()))
FROM_HBM = "hbm"
BY_HAND = "by_hand"


def swap(x, axes):
    return lax.all_to_all(x, axes, split_axis=0, concat_axis=0, tiled=True)


def core_swap(x):
    return lax.ppermute(x, "dom_3", [(0, 1), (1, 0)])


def dot(a, b):
    return jnp.dot(a, b, preferred_element_type=F32)


def split_two(x):
    high = x.astype(BF16)
    return high, (x - high.astype(F32)).astype(BF16)


def vmem():
    return pl.BlockSpec(memory_space=pltpu.VMEM)


def whole(shape):
    return pl.BlockSpec(shape, lambda i: (0,) * len(shape))


def smem():
    return pl.BlockSpec(memory_space=pltpu.SMEM)


def near_memory(x):
    return pltpu.with_memory_space_constraint(x, pltpu.VMEM)


def hbm(shape, kind):
    return pltpu.HBM(shape, kind)


def call(body, outs, specs, scratch=(), args=()):
    given, ins, made, back = [], [], [], []
    for spec, x in zip(specs, args):
        if spec is FROM_HBM or spec is BY_HAND:
            x = pltpu.with_memory_space_constraint(x, pltpu.HBM)
            spec = whole(x.shape) if spec is FROM_HBM else pl.BlockSpec(memory_space=pl.ANY)
        elif spec.memory_space == pltpu.VMEM and x.dtype != jnp.int32:
            x = near_memory(x)
        given.append(x)
        ins.append(spec)
    for o in outs:
        if isinstance(o, tuple) and len(o) == 3:
            made.append(hbm(*o[:2]))
            back.append(pl.BlockSpec(memory_space=pl.ANY))
        elif isinstance(o, tuple):
            made.append(pltpu.VMEM(*o))
            back.append(vmem())
        else:
            made.append(o)
            back.append(whole(o.shape))
    return pl.pallas_call(
        body,
        out_shape=made,
        grid=(1,),
        in_specs=ins,
        out_specs=back,
        scratch_shapes=list(scratch),
        compiler_params=pltpu.CompilerParams(vmem_limit_bytes=28 << 20),
    )(*given)


def halo_body(send_ref, features_ref, out_ref):
    node = lax.broadcasted_iota(jnp.int32, (NODE_DEV, N_DOM), 0)
    own = features_ref[...]
    for k in range(HALO_PEER):
        hit = jnp.where(node == send_ref[k : k + 1, :], 1.0, 0.0).astype(BF16)
        out_ref[:, k, :] = lax.dot_general(hit, own, TN, preferred_element_type=F32).astype(BF16)


def counts_body(tiles_ref, features_ref, w_ref, nbr_ref, halo_count_ref, own_sum_ref, pre_ref, own_buf, w_buf, halo_buf, count_buf, sum_buf, pre_buf, sems):
    copy = pltpu.make_async_copy
    fetch_own = copy(features_ref, own_buf, sems.at[0])
    fetch_w = copy(w_ref.at[0], w_buf, sems.at[1])
    fetch_own.start()
    fetch_w.start()
    rows = 32
    lanes = lax.broadcasted_iota(jnp.int32, (rows, NODE_DEV), 1)

    def chunk(step, _):
        at = pl.ds(pl.multiple_of(step * rows, rows), rows)
        for r in range(RELS):
            index = nbr_ref[at, r * FAN : (r + 1) * FAN]
            place = index & (NODE_DEV - 1)
            code = jnp.where(index < NODE_DEV, 1.0, CODE)
            total = jnp.zeros((rows, NODE_DEV), F32)
            for k in range(FAN):
                hit = lanes == place[:, k : k + 1]
                total = total + jnp.where(hit, code[:, k : k + 1], 0.0)
            halo = jnp.floor(total * (1.0 / CODE))
            halo_buf[r, at, :] = halo.astype(BF16)
            count_buf[r, at, :] = (total - CODE * halo).astype(BF16)
        return 0

    lax.fori_loop(0, NODE_DEV // rows, chunk, 0)
    leave = [copy(halo_buf, halo_count_ref, sems.at[2])]
    leave[0].start()
    fetch_own.wait()
    own = own_buf[...]
    for r in range(RELS):
        sum_buf[r] = dot(count_buf[r], own)
        leave.append(copy(sum_buf.at[r], own_sum_ref.at[r], sems.at[3 + r]))
        leave[-1].start()
    fetch_w.wait()
    pre_buf[...] = dot(own, w_buf[...])
    leave.append(copy(pre_buf, pre_ref, sems.at[5]))
    leave[-1].start()
    for one in leave:
        one.wait()


def layer_body(neg_ids_ref, count_ref, halo_ref, own_sum_ref, pre_ref, w_ref, means_ref, embed_ref, picked_ref):
    halo = halo_ref[...]
    preact = pre_ref[...]
    for r in range(RELS):
        total = own_sum_ref[r] + dot(count_ref[r], halo)
        mean = (total * (1.0 / FAN)).astype(BF16)
        means_ref[r] = mean
        preact = preact + dot(mean, w_ref[r + 1])
    embed = preact.astype(BF16)
    embed_ref[...] = embed
    picked = dot(chosen_rows(neg_ids_ref), embed)[:NEG_DEV]
    picked_ref[...] = jnp.broadcast_to(picked[None], (CHIPS, NEG_DEV, H)).astype(BF16)


def soft_parts(x):
    small = jnp.exp(-jnp.abs(x))
    bottom = 1.0 / (1.0 + small)
    sigmoid = jnp.where(x >= 0, bottom, small * bottom)
    log_one = jnp.where(small < 1e-3, small * (1.0 - 0.5 * small), jnp.log(1.0 + small))
    return sigmoid, jnp.maximum(x, 0.0) + log_one


def largest(x):
    return jnp.max(jnp.max(jnp.abs(x), axis=0, keepdims=True), axis=1, keepdims=True)


def notes_of(values):
    lane = lax.broadcasted_iota(jnp.int32, (NEG_DEV, 128), 1)
    note = jnp.zeros((NEG_DEV, 128), F32)
    for place, value in enumerate(values):
        note = jnp.where(lane == place, value, note)
    return note


def positive_body(count_ref, embed_ref, ends_ref, features_ref, means_ref, grad_ref, note_ref, sources_ref, spread_ref, pairs_ref, sigmoid_ref, softplus_ref, own_buf, mean_buf, sems):
    fetch_own = pltpu.make_async_copy(features_ref, own_buf, sems.at[0])
    fetch_means = pltpu.make_async_copy(means_ref, mean_buf, sems.at[1])
    fetch_own.start()
    fetch_means.start()
    embed = embed_ref[...]
    scores = lax.dot_general(embed, embed, NT, preferred_element_type=F32)
    sigmoid, softplus = soft_parts(-scores)
    sigmoid_ref[...] = sigmoid
    softplus_ref[...] = softplus
    pairs_ref[...] = jnp.zeros((NODE_DEV, NODE_DEV), F32)
    node = lax.broadcasted_iota(jnp.int32, (NODE_DEV, TILE), 0)
    tiles = count_ref[0]

    def group(step, _):
        sources, targets = [], []
        for j in range(GROUP):
            t = step * GROUP + j
            source = jnp.where(t < tiles, ends_ref[t, 0:1, :], -1)
            sources.append(jnp.where(node == source, 1.0, 0.0).astype(BF16))
            targets.append(jnp.where(node == ends_ref[t, 1:2, :], 1.0, 0.0).astype(BF16))
        pairs_ref[...] += lax.dot_general(
            jnp.concatenate(sources, axis=1), jnp.concatenate(targets, axis=1), NT, preferred_element_type=F32
        )
        return 0

    lax.fori_loop(0, (tiles + (GROUP - 1)) // GROUP, group, 0)
    pairs = pairs_ref[...]
    sources = jnp.sum(pairs, axis=1, keepdims=True)
    sources_ref[...] = jnp.broadcast_to(sources, (NODE_DEV, 128))
    high, low = split_two(embed.astype(F32) * sources)
    spread_ref[:, 0:H] = high
    spread_ref[:, H:] = low
    loss = jnp.sum(jnp.sum(pairs * softplus_ref[...], axis=0, keepdims=True), axis=1, keepdims=True)
    high, low = split_two(-((pairs + pairs.T) * sigmoid_ref[...]))
    base = dot(high, embed) + dot(low, embed)
    grad_ref[...] = base
    fetch_own.wait()
    fetch_means.wait()
    widest = largest(own_buf[...].astype(F32))
    for r in range(RELS):
        widest = jnp.maximum(widest, largest(mean_buf[r].astype(F32)))
    count = tiles.astype(F32)
    reach = largest(embed.astype(F32)) * count * (TILE / NEG)
    known = widest * NODE_DEV * largest(base)
    note_ref[...] = notes_of((loss, count, 0.0, known, widest * TILE * count, NEG_DEV * widest, reach))


def scored(embed, rows, sources, spread):
    scores = lax.dot_general(embed, rows, NT, preferred_element_type=F32)
    sigmoid, softplus = soft_parts(scores)
    per_source = jnp.sum(softplus, axis=1, keepdims=True)
    loss = jnp.sum(per_source * sources, axis=0, keepdims=True) * (1.0 / NEG)
    weight = (sigmoid * (1.0 / NEG)).astype(BF16)
    parts = lax.dot_general(weight, spread, TN, preferred_element_type=F32)
    return weight, loss, parts[:, :H] + parts[:, H:]


def near_body(embed_ref, rows_ref, spread_ref, sources_ref, note_in_ref, weight_ref, part_ref, note_ref):
    rows = rows_ref[...]
    weight, loss, part = scored(embed_ref[...], rows, sources_ref[:, 0:1], spread_ref[...])
    weight_ref[...] = weight
    part_ref[...] = part.astype(part_ref.dtype)
    note = note_in_ref[...]
    lane = lax.broadcasted_iota(jnp.int32, note.shape, 1)
    tallest = largest(rows.astype(F32))
    note = jnp.where(lane == 0, note + loss, note)
    note_ref[...] = jnp.where(lane == 2, jnp.maximum(note, note[:, 3:4] + note[:, 4:5] * tallest), note)


def rest_body(near_weight_ref, near_rows_ref, weight_ref, rows_ref, sources_ref, base_ref, grad_ref):
    total = dot(near_weight_ref[...], near_rows_ref[...]) + dot(weight_ref[...], rows_ref[...])
    grad_ref[...] = base_ref[...] + sources_ref[:, 0:1] * total


def merge_body(part_ref, arrived_ref, own_note_ref, other_note_ref, send_ref):
    note = own_note_ref[...] + other_note_ref[...]
    first = note.astype(BF16).astype(F32)
    second = (note - first).astype(BF16).astype(F32)
    third = (note - first) - second
    lane = lax.broadcasted_iota(jnp.int32, note.shape, 1)
    note = jnp.where(lane == 3, pltpu.roll(second, 3, 1), jnp.where(lane == 4, pltpu.roll(third, 4, 1), first))
    send_ref[:, :, H:] = jnp.broadcast_to(note[None], (CHIPS, NEG_DEV, 128)).astype(BF16)
    total = part_ref[...] + arrived_ref[...].astype(F32)
    send_ref[:, :, 0:H] = total.reshape(CHIPS, NEG_DEV, H).astype(BF16)


def chosen_rows(neg_ids_ref):
    row = lax.broadcasted_iota(jnp.int32, (16, NODE_DEV), 0)
    lane = lax.broadcasted_iota(jnp.int32, (16, NODE_DEV), 1)
    chosen = jnp.zeros((16, NODE_DEV), F32)
    for i in range(NEG_DEV):
        chosen = jnp.where((row == i) & (lane == neg_ids_ref[i]), 1.0, chosen)
    return chosen.astype(BF16)


def half_at(core):
    return pl.ds(pl.multiple_of(core * HALF, HALF), HALF)


def known_body(neg_ids_ref, core_ref, grad_ref, features_ref, means_ref, own_ref, other_ref, chosen_ref):
    node = lax.broadcasted_iota(jnp.int32, (NODE_DEV, H), 0)
    grad = grad_ref[...]
    for i in range(NEG_DEV):
        grad = jnp.where(node == neg_ids_ref[i], 0.0, grad)
    pre = grad.astype(BF16)
    picks = chosen_rows(neg_ids_ref)
    swapped = core_ref[0] == 1
    for r, rows in enumerate((features_ref[...], means_ref[0], means_ref[1])):
        at = pl.ds(r * H, H)
        both = lax.dot_general(rows, pre, TN, preferred_element_type=F32)
        first, second = both[:, :HALF], both[:, HALF:]
        own_ref[at, :] = jnp.where(swapped, second, first)
        other_ref[at, :] = jnp.where(swapped, first, second)
        chosen_ref[:, at] = dot(picks, rows).astype(BF16)


def outer_body(neg_ids_ref, core_ref, arrived_ref, grad_ref, total_ref, own_ref, other_ref, note_ref, row_ref):
    total = jnp.sum(arrived_ref[...].astype(F32), axis=0)
    note_ref[...] = total[:, H:]
    total_ref[...] = total[:, :H]
    row_ref[...] = jnp.zeros((16, H), F32)
    firsts = []
    for i in range(NEG_DEV):
        first = i
        for j in reversed(range(i)):
            first = jnp.where(neg_ids_ref[j] == neg_ids_ref[i], j, first)
        firsts.append(first)
        row = grad_ref[pl.ds(neg_ids_ref[i], 1), :]
        row_ref[i : i + 1, :] = row if i == 0 else jnp.where(first == i, row, 0.0)
    for i, first in enumerate(firsts):
        row_ref[pl.ds(first, 1), :] += total_ref[i : i + 1, :]
    own_ref[...] = row_ref[:, half_at(core_ref[0])].astype(BF16)
    other_ref[...] = row_ref[:, half_at(1 - core_ref[0])].astype(BF16)


def pre_body(neg_ids_ref, total_ref, grad_ref, pre_ref, sum_ref):
    sum_ref[...] = grad_ref[...]
    for i in range(NEG_DEV):
        sum_ref[pl.ds(neg_ids_ref[i], 1), :] += total_ref[i : i + 1, :]
    pre_ref[...] = sum_ref[...].astype(BF16)


def update_body(known_ref, own_chosen_ref, other_chosen_ref, own_row_ref, other_row_ref, note_ref, out_ref, factor_ref):
    chosen = jnp.concatenate([own_chosen_ref[...], other_chosen_ref[...]], axis=0)
    rows = jnp.concatenate([own_row_ref[...], other_row_ref[...]], axis=0)
    extra = lax.dot_general(chosen, rows, TN, preferred_element_type=F32)
    known, wide, part = (note_ref[0:1, i : i + 1] for i in (2, 5, 6))
    bound = known + wide * part + TINY
    out_ref[...] = (known_ref[...] + extra) * (SPAN / bound)
    factor_ref[...] = jnp.broadcast_to(bound / SPAN / (note_ref[0:1, 1:2] * TILE), (8, HALF))


def first_half_body(core_ref, half_ref, factor_ref, note_ref, weight_ref, loss_ref):
    note = note_ref[0:1, :]
    loss_ref[...] = (note[:, 0:1] + note[:, 3:4] + note[:, 4:5]) / (note[:, 1:2] * TILE)
    weight_ref[...] = (half_ref[...] * factor_ref[0:1, :]).reshape(RELS + 1, H, HALF)


def second_half_body(core_ref, half_ref, factor_ref, note_ref, begun_ref, weight_ref):
    weight_ref[...] = (half_ref[...] * factor_ref[0:1, :]).reshape(RELS + 1, H, HALF)


def halves(body, which, extra, alias):
    whole_weight = jax.ShapeDtypeStruct((RELS + 1, H, H), F32)
    block = pl.BlockSpec((RELS + 1, H, HALF), lambda r, core: (0, 0, which(core[0])))
    scalar = pl.BlockSpec((1, 1), lambda r, core: (0, 0))
    return pl.pallas_call(
        body,
        out_shape=[whole_weight, jax.ShapeDtypeStruct((1, 1), F32)][: 1 + extra],
        grid_spec=pltpu.PrefetchScalarGridSpec(
            num_scalar_prefetch=1,
            grid=(1,),
            in_specs=[vmem(), vmem(), vmem()] + [pl.BlockSpec(memory_space=pl.ANY)] * len(alias),
            out_specs=[block, scalar][: 1 + extra],
        ),
        input_output_aliases=alias,
        compiler_params=pltpu.CompilerParams(vmem_limit_bytes=28 << 20),
    )


def on_device(features, weights, halo_send, nbr_index, tile_count, edge_ends, neg_ids):
    square = (NODE_DEV, H)
    tall = ((RELS + 1) * H, HALF)
    core = lax.axis_index(NEAR).astype(jnp.int32).reshape(1)
    core, halo_send = lax.optimization_barrier((core, halo_send))
    (outgoing,) = call(halo_body, [((N_DOM, HALO_PEER, H), BF16)], [FROM_HBM, FROM_HBM], (), (halo_send[0].T, features))
    incoming = swap(outgoing, DOM)
    neighbours = nbr_index.reshape(NODE_DEV, RELS * FAN)
    two = (RELS, *square)
    halo_count, own_sum, pre = call(
        counts_body,
        [(two, BF16, BY_HAND), (two, F32, BY_HAND), (square, F32, BY_HAND)],
        [smem(), BY_HAND, BY_HAND, vmem()],
        [pltpu.VMEM(square, BF16)] * 2 + [pltpu.VMEM(two, BF16)] * 2 + [pltpu.VMEM(two, F32), pltpu.VMEM(square, F32), pltpu.SemaphoreType.DMA((6,))],
        (tile_count, features, weights, neighbours),
    )
    means, embed, picked = call(
        layer_body,
        [hbm(two, BF16), (square, BF16), hbm((CHIPS, NEG_DEV, H), BF16)],
        [smem(), FROM_HBM, vmem(), FROM_HBM, FROM_HBM, vmem()],
        (),
        (neg_ids, halo_count, incoming.reshape(512, H), own_sum, pre, weights),
    )
    near_rows = swap(picked, FAR).reshape(square)
    base, note, sources, spread = call(
        positive_body,
        [hbm(square, F32), ((8, 128), F32), ((NODE_DEV, 128), F32), ((NODE_DEV, 2 * H), BF16)],
        [smem(), vmem(), FROM_HBM, BY_HAND, BY_HAND],
        [pltpu.VMEM(square, F32)] * 3 + [pltpu.VMEM(square, BF16), pltpu.VMEM(two, BF16), pltpu.SemaphoreType.DMA((2,))],
        (tile_count, embed, edge_ends, features, means),
    )
    near_rows, note = lax.optimization_barrier((near_rows, note))
    other_rows = core_swap(near_rows)
    near_weight, near_part, note = call(
        near_body,
        [(square, BF16), (square, F32), ((8, 128), F32)],
        [vmem()] * 5,
        (),
        (embed, near_rows, spread, sources, note),
    )
    weight, other_part, note = call(
        near_body,
        [(square, BF16), (square, BF16), ((8, 128), F32)],
        [vmem()] * 5,
        (),
        (embed, other_rows, spread, sources, note),
    )
    other_note = core_swap(note)
    part_arrived = core_swap(other_part)
    (grad,) = call(
        rest_body,
        [(square, F32)],
        [vmem()] * 5 + [FROM_HBM],
        (),
        (near_weight, near_rows, weight, other_rows, sources, base),
    )
    part_arrived, grad = lax.optimization_barrier((part_arrived, grad))
    (outgoing_grad,) = call(
        merge_body,
        [((CHIPS, NEG_DEV, H + 128), BF16)],
        [vmem()] * 4,
        (),
        (near_part, part_arrived, note, other_note),
    )
    outgoing_grad, grad = lax.optimization_barrier((outgoing_grad, grad))
    arrived = swap(outgoing_grad, FAR)
    known_own, known_other, chosen = call(
        known_body,
        [(tall, F32), (tall, F32), ((16, (RELS + 1) * H), BF16)],
        [smem(), smem(), vmem(), FROM_HBM, FROM_HBM],
        (),
        (neg_ids, core, grad, features, means),
    )
    other_chosen = core_swap(chosen)
    known = known_own + core_swap(known_other)
    arrived, known, other_chosen = lax.optimization_barrier((arrived, known, other_chosen))
    total, own_row, send_row, note = call(
        outer_body,
        [((NEG_DEV, H), F32), ((16, HALF), BF16), ((16, HALF), BF16), ((NEG_DEV, 128), F32)],
        [smem(), smem(), vmem(), vmem()],
        [pltpu.VMEM((16, H), F32)],
        (neg_ids, core, arrived, grad),
    )
    other_row = core_swap(send_row)
    (pre_grad,) = call(
        pre_body,
        [hbm(square, BF16)],
        [smem(), vmem(), vmem()],
        [pltpu.VMEM(square, F32)],
        (neg_ids, total, grad),
    )
    partial, factor = call(
        update_body,
        [(tall, F32), ((8, HALF), F32)],
        [vmem()] * 6,
        (),
        (known, chosen, other_chosen, own_row, other_row, note),
    )
    chunks = (CHIPS, 24, HALF)
    sums = swap(partial.astype(F16).reshape(chunks), FAR)
    mine = jnp.sum(sums.astype(F32), axis=0).astype(F16)
    half = swap(jnp.broadcast_to(mine, chunks), FAR).reshape(tall)
    other_half = core_swap(half).astype(F32)
    half = half.astype(F32)
    close = near_memory(factor), near_memory(note)
    begun, mean_loss = halves(first_half_body, lambda c: c, 1, {})(core, near_memory(half), *close)
    (begun, other_half) = lax.optimization_barrier((begun, other_half))
    (weight_grad,) = halves(second_half_body, lambda c: 1 - c, 0, {4: 0})(core, near_memory(other_half), *close, begun)
    return weight_grad, mean_loss.reshape(()), pre_grad


def solution(mesh):
    torus = Mesh(mesh.devices.reshape(4, 4, 4, 2), DOM)
    in_specs = (
        P(DOM, None),
        P(),
        P(DOM, None, None),
        P(DOM, None, None),
        P(DOM),
        P(DOM, None, None),
        P(DOM),
    )
    out_specs = (P(), P(), P(DOM, None))
    return jax.shard_map(on_device, mesh=torus, in_specs=in_specs, out_specs=out_specs, check_vma=False)
```

```python
import jax
import jax.numpy as jnp
from jax import lax
from jax.experimental import pallas as pl
from jax.experimental.pallas import tpu as pltpu
from jax.sharding import Mesh
from jax.sharding import PartitionSpec as P

DOM = ("dom_0", "dom_1", "dom_2", "dom_3")
FAR = ("dom_0", "dom_1", "dom_2")
NEAR = ("dom_3",)
H = 512
RELS = 2
FAN = 8
TILE = 256
NODE_DEV = 512
NEG = 1024
NEG_DEV = 8
N_DOM = 128
HALO_PEER = 4
CHIPS = 64
GROUP = 4
HALF = 256
F32 = jnp.float32
BF16 = jnp.bfloat16
F16 = jnp.float16
SPAN = 60000.0
TINY = 1e-30
CODE = 32.0
NT = (((1,), (1,)), ((), ()))
TN = (((0,), (0,)), ((), ()))
FROM_HBM = "hbm"
BY_HAND = "by_hand"


def swap(x, axes):
    return lax.all_to_all(x, axes, split_axis=0, concat_axis=0, tiled=True)


def core_swap(x):
    return lax.ppermute(x, "dom_3", [(0, 1), (1, 0)])


def dot(a, b):
    return jnp.dot(a, b, preferred_element_type=F32)


def split_two(x):
    high = x.astype(BF16)
    return high, (x - high.astype(F32)).astype(BF16)


def vmem():
    return pl.BlockSpec(memory_space=pltpu.VMEM)


def whole(shape):
    return pl.BlockSpec(shape, lambda i: (0,) * len(shape))


def smem():
    return pl.BlockSpec(memory_space=pltpu.SMEM)


def near_memory(x):
    return pltpu.with_memory_space_constraint(x, pltpu.VMEM)


def hbm(shape, kind):
    return pltpu.HBM(shape, kind)


def call(body, outs, specs, scratch=(), args=()):
    given, ins, made, back = [], [], [], []
    for spec, x in zip(specs, args):
        if spec is FROM_HBM or spec is BY_HAND:
            x = pltpu.with_memory_space_constraint(x, pltpu.HBM)
            spec = whole(x.shape) if spec is FROM_HBM else pl.BlockSpec(memory_space=pl.ANY)
        elif spec.memory_space == pltpu.VMEM and x.dtype != jnp.int32:
            x = near_memory(x)
        given.append(x)
        ins.append(spec)
    for o in outs:
        if isinstance(o, tuple) and len(o) == 3:
            made.append(hbm(*o[:2]))
            back.append(pl.BlockSpec(memory_space=pl.ANY))
        elif isinstance(o, tuple):
            made.append(pltpu.VMEM(*o))
            back.append(vmem())
        else:
            made.append(o)
            back.append(whole(o.shape))
    return pl.pallas_call(
        body,
        out_shape=made,
        grid=(1,),
        in_specs=ins,
        out_specs=back,
        scratch_shapes=list(scratch),
        compiler_params=pltpu.CompilerParams(vmem_limit_bytes=28 << 20),
    )(*given)


def halo_body(send_ref, features_ref, out_ref):
    node = lax.broadcasted_iota(jnp.int32, (NODE_DEV, N_DOM), 0)
    own = features_ref[...]
    for k in range(HALO_PEER):
        hit = jnp.where(node == send_ref[k : k + 1, :], 1.0, 0.0).astype(BF16)
        out_ref[:, k, :] = lax.dot_general(hit, own, TN, preferred_element_type=F32).astype(BF16)


def counts_body(features_ref, w_ref, nbr_ref, halo_count_ref, own_sum_ref, pre_ref, own_buf, w_buf, halo_buf, count_buf, sum_buf, pre_buf, sems):
    copy = pltpu.make_async_copy
    fetch_own = copy(features_ref, own_buf, sems.at[0])
    fetch_w = copy(w_ref.at[0], w_buf, sems.at[1])
    fetch_own.start()
    fetch_w.start()
    rows = 32
    lanes = lax.broadcasted_iota(jnp.int32, (rows, NODE_DEV), 1)

    def chunk(step, _):
        at = pl.ds(pl.multiple_of(step * rows, rows), rows)
        for r in range(RELS):
            index = nbr_ref[at, r * FAN : (r + 1) * FAN]
            place = index & (NODE_DEV - 1)
            code = jnp.where(index < NODE_DEV, 1.0, CODE)
            total = jnp.zeros((rows, NODE_DEV), F32)
            for k in range(FAN):
                hit = lanes == place[:, k : k + 1]
                total = total + jnp.where(hit, code[:, k : k + 1], 0.0)
            halo = jnp.floor(total * (1.0 / CODE))
            halo_buf[r, at, :] = halo.astype(BF16)
            count_buf[r, at, :] = (total - CODE * halo).astype(BF16)
        return 0

    lax.fori_loop(0, NODE_DEV // rows, chunk, 0)
    leave = [copy(halo_buf, halo_count_ref, sems.at[2])]
    leave[0].start()
    fetch_own.wait()
    own = own_buf[...]
    for r in range(RELS):
        sum_buf[r] = dot(count_buf[r], own)
        leave.append(copy(sum_buf.at[r], own_sum_ref.at[r], sems.at[3 + r]))
        leave[-1].start()
    fetch_w.wait()
    pre_buf[...] = dot(own, w_buf[...])
    leave.append(copy(pre_buf, pre_ref, sems.at[5]))
    leave[-1].start()
    for one in leave:
        one.wait()


def layer_body(neg_ids_ref, count_ref, halo_ref, own_sum_ref, pre_ref, w_ref, means_ref, embed_ref, picked_ref):
    halo = halo_ref[...]
    preact = pre_ref[...]
    for r in range(RELS):
        total = own_sum_ref[r] + dot(count_ref[r], halo)
        mean = (total * (1.0 / FAN)).astype(BF16)
        means_ref[r] = mean
        preact = preact + dot(mean, w_ref[r + 1])
    embed = preact.astype(BF16)
    embed_ref[...] = embed
    picked = dot(chosen_rows(neg_ids_ref), embed)[:NEG_DEV]
    picked_ref[...] = jnp.broadcast_to(picked[None], (CHIPS, NEG_DEV, H)).astype(BF16)


def soft_parts(x):
    small = jnp.exp(-jnp.abs(x))
    bottom = 1.0 / (1.0 + small)
    sigmoid = jnp.where(x >= 0, bottom, small * bottom)
    log_one = jnp.where(small < 1e-3, small * (1.0 - 0.5 * small), jnp.log(1.0 + small))
    return sigmoid, jnp.maximum(x, 0.0) + log_one


def largest(x):
    return jnp.max(jnp.max(jnp.abs(x), axis=0, keepdims=True), axis=1, keepdims=True)


def notes_of(values):
    lane = lax.broadcasted_iota(jnp.int32, (NEG_DEV, 128), 1)
    note = jnp.zeros((NEG_DEV, 128), F32)
    for place, value in enumerate(values):
        note = jnp.where(lane == place, value, note)
    return note


def positive_body(count_ref, embed_ref, ends_ref, features_ref, means_ref, grad_ref, note_ref, sources_ref, spread_ref, pairs_ref, sigmoid_ref, softplus_ref, own_buf, mean_buf, sems):
    fetch_own = pltpu.make_async_copy(features_ref, own_buf, sems.at[0])
    fetch_means = pltpu.make_async_copy(means_ref, mean_buf, sems.at[1])
    fetch_own.start()
    fetch_means.start()
    embed = embed_ref[...]
    scores = lax.dot_general(embed, embed, NT, preferred_element_type=F32)
    sigmoid, softplus = soft_parts(-scores)
    sigmoid_ref[...] = sigmoid
    softplus_ref[...] = softplus
    pairs_ref[...] = jnp.zeros((NODE_DEV, NODE_DEV), F32)
    node = lax.broadcasted_iota(jnp.int32, (NODE_DEV, TILE), 0)
    tiles = count_ref[0]

    def group(step, _):
        sources, targets = [], []
        for j in range(GROUP):
            t = step * GROUP + j
            source = jnp.where(t < tiles, ends_ref[t, 0:1, :], -1)
            sources.append(jnp.where(node == source, 1.0, 0.0).astype(BF16))
            targets.append(jnp.where(node == ends_ref[t, 1:2, :], 1.0, 0.0).astype(BF16))
        pairs_ref[...] += lax.dot_general(
            jnp.concatenate(sources, axis=1), jnp.concatenate(targets, axis=1), NT, preferred_element_type=F32
        )
        return 0

    lax.fori_loop(0, (tiles + (GROUP - 1)) // GROUP, group, 0)
    pairs = pairs_ref[...]
    sources = jnp.sum(pairs, axis=1, keepdims=True)
    sources_ref[...] = jnp.broadcast_to(sources, (NODE_DEV, 128))
    high, low = split_two(embed.astype(F32) * sources)
    spread_ref[:, 0:H] = high
    spread_ref[:, H:] = low
    loss = jnp.sum(jnp.sum(pairs * softplus_ref[...], axis=0, keepdims=True), axis=1, keepdims=True)
    high, low = split_two(-((pairs + pairs.T) * sigmoid_ref[...]))
    base = dot(high, embed) + dot(low, embed)
    grad_ref[...] = base
    fetch_own.wait()
    fetch_means.wait()
    widest = largest(own_buf[...].astype(F32))
    for r in range(RELS):
        widest = jnp.maximum(widest, largest(mean_buf[r].astype(F32)))
    count = tiles.astype(F32)
    reach = largest(embed.astype(F32)) * count * (TILE / NEG)
    known = widest * NODE_DEV * largest(base)
    note_ref[...] = notes_of((loss, count, 0.0, known, widest * TILE * count, NEG_DEV * widest, reach))


def scored(embed, rows, sources, spread):
    scores = lax.dot_general(embed, rows, NT, preferred_element_type=F32)
    sigmoid, softplus = soft_parts(scores)
    per_source = jnp.sum(softplus, axis=1, keepdims=True)
    loss = jnp.sum(per_source * sources, axis=0, keepdims=True) * (1.0 / NEG)
    weight = (sigmoid * (1.0 / NEG)).astype(BF16)
    parts = lax.dot_general(weight, spread, TN, preferred_element_type=F32)
    return weight, loss, parts[:, :H] + parts[:, H:]


def near_body(embed_ref, rows_ref, spread_ref, sources_ref, note_in_ref, weight_ref, part_ref, note_ref):
    rows = rows_ref[...]
    weight, loss, part = scored(embed_ref[...], rows, sources_ref[:, 0:1], spread_ref[...])
    weight_ref[...] = weight
    part_ref[...] = part.astype(part_ref.dtype)
    note = note_in_ref[...]
    lane = lax.broadcasted_iota(jnp.int32, note.shape, 1)
    tallest = largest(rows.astype(F32))
    note = jnp.where(lane == 0, note + loss, note)
    note_ref[...] = jnp.where(lane == 2, jnp.maximum(note, note[:, 3:4] + note[:, 4:5] * tallest), note)


def rest_body(near_weight_ref, near_rows_ref, weight_ref, rows_ref, sources_ref, base_ref, grad_ref):
    total = dot(near_weight_ref[...], near_rows_ref[...]) + dot(weight_ref[...], rows_ref[...])
    grad_ref[...] = base_ref[...] + sources_ref[:, 0:1] * total


def merge_body(part_ref, arrived_ref, own_note_ref, other_note_ref, send_ref):
    note = own_note_ref[...] + other_note_ref[...]
    first = note.astype(BF16).astype(F32)
    second = (note - first).astype(BF16).astype(F32)
    third = (note - first) - second
    lane = lax.broadcasted_iota(jnp.int32, note.shape, 1)
    note = jnp.where(lane == 3, pltpu.roll(second, 3, 1), jnp.where(lane == 4, pltpu.roll(third, 4, 1), first))
    send_ref[:, :, H:] = jnp.broadcast_to(note[None], (CHIPS, NEG_DEV, 128)).astype(BF16)
    total = part_ref[...] + arrived_ref[...].astype(F32)
    send_ref[:, :, 0:H] = total.reshape(CHIPS, NEG_DEV, H).astype(BF16)


def chosen_rows(neg_ids_ref):
    row = lax.broadcasted_iota(jnp.int32, (16, NODE_DEV), 0)
    lane = lax.broadcasted_iota(jnp.int32, (16, NODE_DEV), 1)
    chosen = jnp.zeros((16, NODE_DEV), F32)
    for i in range(NEG_DEV):
        chosen = jnp.where((row == i) & (lane == neg_ids_ref[i]), 1.0, chosen)
    return chosen.astype(BF16)


def half_at(core):
    return pl.ds(pl.multiple_of(core * HALF, HALF), HALF)


def known_body(neg_ids_ref, core_ref, grad_ref, features_ref, means_ref, own_ref, other_ref, chosen_ref):
    node = lax.broadcasted_iota(jnp.int32, (NODE_DEV, H), 0)
    grad = grad_ref[...]
    for i in range(NEG_DEV):
        grad = jnp.where(node == neg_ids_ref[i], 0.0, grad)
    pre = grad.astype(BF16)
    picks = chosen_rows(neg_ids_ref)
    swapped = core_ref[0] == 1
    for r, rows in enumerate((features_ref[...], means_ref[0], means_ref[1])):
        at = pl.ds(r * H, H)
        both = lax.dot_general(rows, pre, TN, preferred_element_type=F32)
        first, second = both[:, :HALF], both[:, HALF:]
        own_ref[at, :] = jnp.where(swapped, second, first)
        other_ref[at, :] = jnp.where(swapped, first, second)
        chosen_ref[:, at] = dot(picks, rows).astype(BF16)


def outer_body(neg_ids_ref, core_ref, arrived_ref, grad_ref, total_ref, own_ref, other_ref, note_ref, row_ref):
    total = jnp.sum(arrived_ref[...].astype(F32), axis=0)
    note_ref[...] = total[:, H:]
    total_ref[...] = total[:, :H]
    row_ref[...] = jnp.zeros((16, H), F32)
    firsts = []
    for i in range(NEG_DEV):
        first = i
        for j in reversed(range(i)):
            first = jnp.where(neg_ids_ref[j] == neg_ids_ref[i], j, first)
        firsts.append(first)
        row = grad_ref[pl.ds(neg_ids_ref[i], 1), :]
        row_ref[i : i + 1, :] = row if i == 0 else jnp.where(first == i, row, 0.0)
    for i, first in enumerate(firsts):
        row_ref[pl.ds(first, 1), :] += total_ref[i : i + 1, :]
    own_ref[...] = row_ref[:, half_at(core_ref[0])].astype(BF16)
    other_ref[...] = row_ref[:, half_at(1 - core_ref[0])].astype(BF16)


def pre_body(neg_ids_ref, total_ref, grad_ref, pre_ref, sum_ref, round_ref, sems):
    sum_ref[...] = grad_ref[...]
    for i in range(NEG_DEV):
        sum_ref[pl.ds(neg_ids_ref[i], 1), :] += total_ref[i : i + 1, :]
    leave = []
    for part in range(4):
        at = pl.ds(part * N_DOM, N_DOM)
        round_ref[at, :] = sum_ref[at, :].astype(BF16)
        leave.append(pltpu.make_async_copy(round_ref.at[at], pre_ref.at[at], sems.at[part]))
        leave[part].start()
    for one in leave:
        one.wait()


def update_body(known_ref, own_chosen_ref, other_chosen_ref, own_row_ref, other_row_ref, note_ref, out_ref, factor_ref):
    chosen = jnp.concatenate([own_chosen_ref[...], other_chosen_ref[...]], axis=0)
    rows = jnp.concatenate([own_row_ref[...], other_row_ref[...]], axis=0)
    extra = lax.dot_general(chosen, rows, TN, preferred_element_type=F32)
    known, wide, part = (note_ref[0:1, i : i + 1] for i in (2, 5, 6))
    bound = known + wide * part + TINY
    out_ref[...] = (known_ref[...] + extra) * (SPAN / bound)
    factor_ref[...] = jnp.broadcast_to(bound / SPAN / (note_ref[0:1, 1:2] * TILE), (8, HALF))


def first_half_body(core_ref, half_ref, factor_ref, note_ref, weight_ref, loss_ref):
    note = note_ref[0:1, :]
    loss_ref[...] = (note[:, 0:1] + note[:, 3:4] + note[:, 4:5]) / (note[:, 1:2] * TILE)
    weight_ref[...] = (half_ref[...] * factor_ref[0:1, :]).reshape(RELS + 1, H, HALF)


def second_half_body(core_ref, half_ref, factor_ref, note_ref, begun_ref, weight_ref):
    weight_ref[...] = (half_ref[...] * factor_ref[0:1, :]).reshape(RELS + 1, H, HALF)


def halves(body, which, extra, alias):
    whole_weight = jax.ShapeDtypeStruct((RELS + 1, H, H), F32)
    block = pl.BlockSpec((RELS + 1, H, HALF), lambda r, core: (0, 0, which(core[0])))
    scalar = pl.BlockSpec((1, 1), lambda r, core: (0, 0))
    return pl.pallas_call(
        body,
        out_shape=[whole_weight, jax.ShapeDtypeStruct((1, 1), F32)][: 1 + extra],
        grid_spec=pltpu.PrefetchScalarGridSpec(
            num_scalar_prefetch=1,
            grid=(1,),
            in_specs=[vmem(), vmem(), vmem()] + [pl.BlockSpec(memory_space=pl.ANY)] * len(alias),
            out_specs=[block, scalar][: 1 + extra],
        ),
        input_output_aliases=alias,
        compiler_params=pltpu.CompilerParams(vmem_limit_bytes=28 << 20),
    )


def on_device(features, weights, halo_send, nbr_index, tile_count, edge_ends, neg_ids):
    square = (NODE_DEV, H)
    tall = ((RELS + 1) * H, HALF)
    core = lax.axis_index(NEAR).astype(jnp.int32).reshape(1)
    core, halo_send = lax.optimization_barrier((core, halo_send))
    (outgoing,) = call(halo_body, [((N_DOM, HALO_PEER, H), BF16)], [FROM_HBM, FROM_HBM], (), (halo_send[0].T, features))
    incoming = swap(outgoing, DOM)
    neighbours = nbr_index.reshape(NODE_DEV, RELS * FAN)
    two = (RELS, *square)
    halo_count, own_sum, pre = call(
        counts_body,
        [(two, BF16, BY_HAND), (two, F32, BY_HAND), (square, F32, BY_HAND)],
        [BY_HAND, BY_HAND, vmem()],
        [pltpu.VMEM(square, BF16)] * 2 + [pltpu.VMEM(two, BF16)] * 2 + [pltpu.VMEM(two, F32), pltpu.VMEM(square, F32), pltpu.SemaphoreType.DMA((6,))],
        (features, weights, neighbours),
    )
    means, embed, picked = call(
        layer_body,
        [hbm(two, BF16), (square, BF16), hbm((CHIPS, NEG_DEV, H), BF16)],
        [smem(), FROM_HBM, vmem(), FROM_HBM, FROM_HBM, vmem()],
        (),
        (neg_ids, halo_count, incoming.reshape(512, H), own_sum, pre, weights),
    )
    near_rows = swap(picked, FAR).reshape(square)
    base, note, sources, spread = call(
        positive_body,
        [hbm(square, F32), ((8, 128), F32), ((NODE_DEV, 128), F32), ((NODE_DEV, 2 * H), BF16)],
        [smem(), vmem(), FROM_HBM, BY_HAND, BY_HAND],
        [pltpu.VMEM(square, F32)] * 3 + [pltpu.VMEM(square, BF16), pltpu.VMEM(two, BF16), pltpu.SemaphoreType.DMA((2,))],
        (tile_count, embed, edge_ends, features, means),
    )
    near_rows, note = lax.optimization_barrier((near_rows, note))
    other_rows = core_swap(near_rows)
    near_weight, near_part, note = call(
        near_body,
        [(square, BF16), (square, F32), ((8, 128), F32)],
        [vmem()] * 5,
        (),
        (embed, near_rows, spread, sources, note),
    )
    weight, other_part, note = call(
        near_body,
        [(square, BF16), (square, BF16), ((8, 128), F32)],
        [vmem()] * 5,
        (),
        (embed, other_rows, spread, sources, note),
    )
    other_note = core_swap(note)
    part_arrived = core_swap(other_part)
    (grad,) = call(
        rest_body,
        [(square, F32)],
        [vmem()] * 5 + [FROM_HBM],
        (),
        (near_weight, near_rows, weight, other_rows, sources, base),
    )
    part_arrived, grad = lax.optimization_barrier((part_arrived, grad))
    (outgoing_grad,) = call(
        merge_body,
        [((CHIPS, NEG_DEV, H + 128), BF16)],
        [vmem()] * 4,
        (),
        (near_part, part_arrived, note, other_note),
    )
    outgoing_grad, grad = lax.optimization_barrier((outgoing_grad, grad))
    arrived = swap(outgoing_grad, FAR)
    known_own, known_other, chosen = call(
        known_body,
        [(tall, F32), (tall, F32), ((16, (RELS + 1) * H), BF16)],
        [smem(), smem(), vmem(), FROM_HBM, FROM_HBM],
        (),
        (neg_ids, core, grad, features, means),
    )
    other_chosen = core_swap(chosen)
    known = known_own + core_swap(known_other)
    arrived, known, other_chosen = lax.optimization_barrier((arrived, known, other_chosen))
    total, own_row, send_row, note = call(
        outer_body,
        [((NEG_DEV, H), F32), ((16, HALF), BF16), ((16, HALF), BF16), ((NEG_DEV, 128), F32)],
        [smem(), smem(), vmem(), vmem()],
        [pltpu.VMEM((16, H), F32)],
        (neg_ids, core, arrived, grad),
    )
    other_row = core_swap(send_row)
    (pre_grad,) = call(
        pre_body,
        [(square, BF16, BY_HAND)],
        [smem(), vmem(), vmem()],
        [pltpu.VMEM(square, F32), pltpu.VMEM(square, BF16), pltpu.SemaphoreType.DMA((4,))],
        (neg_ids, total, grad),
    )
    partial, factor = call(
        update_body,
        [(tall, F32), ((8, HALF), F32)],
        [vmem()] * 6,
        (),
        (known, chosen, other_chosen, own_row, other_row, note),
    )
    chunks = (CHIPS, 24, HALF)
    sums = swap(partial.astype(F16).reshape(chunks), FAR)
    mine = jnp.sum(sums.astype(F32), axis=0).astype(F16)
    half = swap(jnp.broadcast_to(mine, chunks), FAR).reshape(tall)
    other_half = core_swap(half).astype(F32)
    half = half.astype(F32)
    close = near_memory(factor), near_memory(note)
    begun, mean_loss = halves(first_half_body, lambda c: c, 1, {})(core, near_memory(half), *close)
    (begun, other_half) = lax.optimization_barrier((begun, other_half))
    (weight_grad,) = halves(second_half_body, lambda c: 1 - c, 0, {4: 0})(core, near_memory(other_half), *close, begun)
    return weight_grad, mean_loss.reshape(()), pre_grad


def solution(mesh):
    torus = Mesh(mesh.devices.reshape(4, 4, 4, 2), DOM)
    in_specs = (
        P(DOM, None),
        P(),
        P(DOM, None, None),
        P(DOM, None, None),
        P(DOM),
        P(DOM, None, None),
        P(DOM),
    )
    out_specs = (P(), P(), P(DOM, None))
    return jax.shard_map(on_device, mesh=torus, in_specs=in_specs, out_specs=out_specs, check_vma=False)
```
